8 devices in a mesh: col: 2 (over z, y), row: 4 (over x, core).
Axes of the slice: x: 2, y: 2, z: 1, core: 2. Of those that a mesh axis runs over, the one named last changes fastest.
Arguments:
- vel_u: float32 [41, 192, 1024], P(None, 'row', 'col')
- vel_v: float32 [41, 192, 1024], P(None, 'row', 'col')
- temperature: float32 [41, 192, 1024], P(None, 'row', 'col')
- salinity: float32 [41, 192, 1024], P(None, 'row', 'col')
- surf_eta: float32 [192, 1024], P('row', 'col')
- trans_u: float32 [192, 1024], P('row', 'col')
- trans_v: float32 [192, 1024], P('row', 'col')
- bottom_depth: float32 [192, 1024], P('row', 'col')
- level_count: int32 [192, 1024], P('row', 'col')
- avg_weights: float32 [30], replicated
Outputs:
- output 1: float32 [192, 1024], P('row', 'col')
- output 2: float32 [192, 1024], P('row', 'col')
- output 3: float32 [192, 1024], P('row', 'col')
- output 4: float32 [41, 192, 1024], P(None, 'row', 'col')
- output 5: float32 [41, 192, 1024], P(None, 'row', 'col')
- output 6: float32 [41, 192, 1024], P(None, 'row', 'col')
- output 7: float32 [41, 192, 1024], P(None, 'row', 'col')
All inputs are finite; a program needn't handle non-finite values.
Results may differ from the reference program's by a relative error of at most 0.001.
Values sent between devices are 32-bit elements.
A program may use at most 1 GiB of HBM per device.

```python
import jax
import jax.numpy as jnp
from jax import lax

LEVELS = 41
SUBCYCLES = 30
GRID_Y = 192
GRID_X = 1024

TIME_STEP = 1.0
GRAVITY = 16.0
BC_GRAVITY = 4.0
EXPAND_T = 0.2
CONTRACT_S = 0.6
CORIO_F0 = 0.4
CORIO_BETA = 0.4
VISC_R = 2.0
DIFF_R = 0.5


def setup_inputs(seed: int = 0) -> dict:
    keys = jax.random.split(jax.random.key(seed), 10)
    shape3 = (LEVELS, GRID_Y, GRID_X)
    shape2 = (GRID_Y, GRID_X)
    north_open = (jnp.arange(GRID_Y) < GRID_Y - 1).astype(jnp.float32)[:, None]
    vel_u = 0.3 * jax.random.normal(keys[0], shape3, jnp.float32)
    vel_v = 0.3 * jax.random.normal(keys[1], shape3, jnp.float32) * north_open
    temperature = jax.random.normal(keys[2], shape3, jnp.float32)
    salinity = 0.5 * jax.random.normal(keys[3], shape3, jnp.float32)
    surf_eta = 0.1 * jax.random.normal(keys[4], shape2, jnp.float32)
    trans_u = 0.3 * jax.random.normal(keys[5], shape2, jnp.float32)
    trans_v = 0.3 * jax.random.normal(keys[6], shape2, jnp.float32) * north_open
    bottom_depth = jax.random.uniform(keys[7], shape2, jnp.float32, 0.5, 1.5)
    level_count = jax.random.randint(keys[8], shape2, 1, LEVELS + 1, dtype=jnp.int32)
    level_count = level_count.at[0, 0].set(1).at[0, 1].set(LEVELS)
    ramp = (jnp.arange(SUBCYCLES) + 1.0) / SUBCYCLES
    raw_weights = ramp * jax.random.uniform(keys[9], (SUBCYCLES,), jnp.float32, 0.5, 1.5)
    avg_weights = raw_weights / jnp.sum(raw_weights)
    return {'vel_u': vel_u, 'vel_v': vel_v, 'temperature': temperature, 'salinity': salinity, 'surf_eta': surf_eta, 'trans_u': trans_u, 'trans_v': trans_v, 'bottom_depth': bottom_depth, 'level_count': level_count, 'avg_weights': avg_weights}


def pad_halo(field):
    wrapped = jnp.concatenate([field[..., -1:], field, field[..., :1]], axis=-1)
    ghost = jnp.zeros_like(wrapped[..., :1, :])
    return jnp.concatenate([ghost, wrapped, ghost], axis=-2)


def shifted(padded, step_y, step_x):
    n_rows = padded.shape[-2] - 2
    n_cols = padded.shape[-1] - 2
    return padded[..., 1 + step_y:1 + step_y + n_rows, 1 + step_x:1 + step_x + n_cols]


def tri_solve(right_side, active, strength):
    link = strength * active[1:]
    zero_row = jnp.zeros_like(right_side[:1])
    low_links = jnp.concatenate([zero_row, link], axis=0)
    up_links = jnp.concatenate([link, zero_row], axis=0)

    def down(carry, level):
        ratio_prev, value_prev = carry
        low_link, up_link, target = level
        denominator = 1.0 + low_link + up_link + low_link * ratio_prev
        ratio = -up_link / denominator
        value = (target + low_link * value_prev) / denominator
        return (ratio, value), (ratio, value)

    start = (jnp.zeros_like(right_side[0]), jnp.zeros_like(right_side[0]))
    _, (ratios, values) = lax.scan(down, start, (low_links, up_links, right_side))

    def back(below, level):
        ratio, value = level
        solved = value - ratio * below
        return solved, solved

    _, solved_all = lax.scan(back, jnp.zeros_like(right_side[0]), (ratios, values), reverse=True)
    return solved_all


def ocean_columns(u_pad, v_pad, temperature_pad, salinity_pad, count_pad, depth_pad, coriolis_u, coriolis_v):
    n_levels = u_pad.shape[0]
    count_mid = shifted(count_pad, 0, 0)
    levels_u = jnp.minimum(count_mid, shifted(count_pad, 0, 1))
    levels_uw = jnp.minimum(shifted(count_pad, 0, -1), count_mid)
    levels_v = jnp.minimum(count_mid, shifted(count_pad, 1, 0))
    levels_vs = jnp.minimum(shifted(count_pad, -1, 0), count_mid)
    level_index = jnp.arange(n_levels)[:, None, None]
    mask_mid = (level_index < count_mid).astype(jnp.float32)
    mask_u = (level_index < levels_u).astype(jnp.float32)
    mask_uw = (level_index < levels_uw).astype(jnp.float32)
    mask_v = (level_index < levels_v).astype(jnp.float32)
    mask_vs = (level_index < levels_vs).astype(jnp.float32)
    u_mid = shifted(u_pad, 0, 0)
    v_mid = shifted(v_pad, 0, 0)
    u_west = shifted(u_pad, 0, -1)
    v_south = shifted(v_pad, -1, 0)
    v_at_u = 0.25 * (v_mid + shifted(v_pad, 0, 1) + v_south + shifted(v_pad, -1, 1))
    u_at_v = 0.25 * (u_mid + u_west + shifted(u_pad, 1, 0) + shifted(u_pad, 1, -1))
    inertia_u = 0.5 * (u_mid * (shifted(u_pad, 0, 1) - u_west) + v_at_u * (shifted(u_pad, 1, 0) - shifted(u_pad, -1, 0)))
    inertia_v = 0.5 * (u_at_v * (shifted(v_pad, 0, 1) - shifted(v_pad, 0, -1)) + v_mid * (shifted(v_pad, 1, 0) - v_south))
    density = CONTRACT_S * salinity_pad - EXPAND_T * temperature_pad
    pressure = (BC_GRAVITY / n_levels) * (jnp.cumsum(density, axis=0) - 0.5 * density)
    pressure_mid = shifted(pressure, 0, 0)
    u_star = u_mid + TIME_STEP * (coriolis_u * v_at_u - inertia_u - shifted(pressure, 0, 1) + pressure_mid)
    v_star = v_mid + TIME_STEP * (-coriolis_v * u_at_v - inertia_v - shifted(pressure, 1, 0) + pressure_mid)
    u_visc = tri_solve(u_star, mask_u, VISC_R)
    v_visc = tri_solve(v_star, mask_v, VISC_R)
    count_u = jnp.maximum(jnp.sum(mask_u, axis=0), 1.0)
    count_v = jnp.maximum(jnp.sum(mask_v, axis=0), 1.0)
    depth_mid = shifted(depth_pad, 0, 0)
    depth_u = 0.5 * (depth_mid + shifted(depth_pad, 0, 1))
    depth_v = 0.5 * (depth_mid + shifted(depth_pad, 1, 0))
    force_u = depth_u * jnp.sum(mask_u * (u_visc - u_mid), axis=0) / count_u / TIME_STEP
    force_v = depth_v * jnp.sum(mask_v * (v_visc - v_mid), axis=0) / count_v / TIME_STEP
    shear_u = u_visc - jnp.sum(mask_u * u_visc, axis=0) / count_u
    shear_v = v_visc - jnp.sum(mask_v * v_visc, axis=0) / count_v
    wet_u = (levels_u > 0).astype(jnp.float32)
    wet_v = (levels_v > 0).astype(jnp.float32)

    def advect(tracer_pad):
        tracer_mid = shifted(tracer_pad, 0, 0)
        flux_east = mask_u * u_mid * (tracer_mid + shifted(tracer_pad, 0, 1))
        flux_west = mask_uw * u_west * (shifted(tracer_pad, 0, -1) + tracer_mid)
        flux_north = mask_v * v_mid * (tracer_mid + shifted(tracer_pad, 1, 0))
        flux_south = mask_vs * v_south * (shifted(tracer_pad, -1, 0) + tracer_mid)
        return tracer_mid - 0.5 * TIME_STEP * (flux_east - flux_west + flux_north - flux_south)

    temperature_new = tri_solve(advect(temperature_pad), mask_mid, DIFF_R)
    salinity_new = tri_solve(advect(salinity_pad), mask_mid, DIFF_R)
    return (shear_u, shear_v, mask_u, mask_v, depth_u, depth_v, wet_u, wet_v, force_u, force_v, temperature_new, salinity_new)


def fast_update(stack_pad, force_u, force_v, depth_u, depth_v, wet_u, wet_v, coriolis_u, coriolis_v, dt_fast):
    eta_pad = stack_pad[0]
    trans_u_pad = stack_pad[1]
    trans_v_pad = stack_pad[2]
    eta_ext = eta_pad[1:, 1:] - dt_fast * (trans_u_pad[1:, 1:] - trans_u_pad[1:, :-1] + trans_v_pad[1:, 1:] - trans_v_pad[:-1, 1:])
    eta_new = eta_ext[:-1, :-1]
    trans_u_old = shifted(trans_u_pad, 0, 0)
    trans_v_old = shifted(trans_v_pad, 0, 0)
    v_at_u = 0.25 * (trans_v_old + shifted(trans_v_pad, 0, 1) + shifted(trans_v_pad, -1, 0) + shifted(trans_v_pad, -1, 1))
    u_at_v = 0.25 * (trans_u_old + shifted(trans_u_pad, 0, -1) + shifted(trans_u_pad, 1, 0) + shifted(trans_u_pad, 1, -1))
    trans_u_new = wet_u * (trans_u_old + dt_fast * (coriolis_u * v_at_u + force_u - GRAVITY * depth_u * (eta_ext[:-1, 1:] - eta_new)))
    trans_v_new = wet_v * (trans_v_old + dt_fast * (force_v - coriolis_v * u_at_v - GRAVITY * depth_v * (eta_ext[1:, :-1] - eta_new)))
    return eta_new, trans_u_new, trans_v_new


def reference(vel_u, vel_v, temperature, salinity, surf_eta, trans_u, trans_v, bottom_depth, level_count, avg_weights):
    n_rows = surf_eta.shape[0]
    dt_fast = TIME_STEP / avg_weights.shape[0]
    row_pos = jnp.arange(n_rows).astype(jnp.float32)[:, None]
    coriolis_u = CORIO_F0 + CORIO_BETA * ((row_pos + 0.5) / n_rows - 0.5)
    coriolis_v = CORIO_F0 + CORIO_BETA * ((row_pos + 1.0) / n_rows - 0.5)
    columns = ocean_columns(pad_halo(vel_u), pad_halo(vel_v), pad_halo(temperature), pad_halo(salinity), pad_halo(level_count), pad_halo(bottom_depth), coriolis_u, coriolis_v)
    shear_u, shear_v, mask_u, mask_v, depth_u, depth_v, wet_u, wet_v, force_u, force_v, temperature_new, salinity_new = columns

    def subcycle(carry, weight):
        eta_old, trans_u_old, trans_v_old, acc_u, acc_v = carry
        stack_pad = pad_halo(jnp.stack([eta_old, trans_u_old, trans_v_old]))
        eta_new, trans_u_new, trans_v_new = fast_update(stack_pad, force_u, force_v, depth_u, depth_v, wet_u, wet_v, coriolis_u, coriolis_v, dt_fast)
        return (eta_new, trans_u_new, trans_v_new, acc_u + weight * trans_u_new, acc_v + weight * trans_v_new), None

    zero_field = jnp.zeros_like(surf_eta)
    final, _ = lax.scan(subcycle, (surf_eta, trans_u, trans_v, zero_field, zero_field), avg_weights)
    eta_fin, trans_u_fin, trans_v_fin, bar_u, bar_v = final
    vel_u_new = mask_u * (shear_u + bar_u / depth_u)
    vel_v_new = mask_v * (shear_v + bar_v / depth_v)
    return (eta_fin, trans_u_fin, trans_v_fin, vel_u_new, vel_v_new, temperature_new, salinity_new)
```

```python
import functools

import jax
import jax.numpy as jnp
from jax import lax
from jax.experimental import pallas as pl
from jax.experimental.pallas import tpu as pltpu
from jax.sharding import PartitionSpec as P

TIME_STEP = 1.0
GRAVITY = 16.0
BC_GRAVITY = 4.0
EXPAND_T = 0.2
CONTRACT_S = 0.6
CORIO_F0 = 0.4
CORIO_BETA = 0.4
VISC_R = 2.0
DIFF_R = 0.5

LEV = 41
ROWS = 48
SUB = 8
COLS = 512
LANES = 128
STRIPS = COLS // LANES
TILES = ROWS // SUB
PITCH = 56
REACH = 32
EXT = ROWS + 2 * REACH
EXT_TILES = EXT // SUB
PAGE = EXT + 16
MESH = pl.DeviceIdType.MESH
F32 = jnp.float32
VMEM_LIMIT = 62 * 1024 * 1024


def tables(strength):
    inner, last, ratio = [], [], 0.0
    for level in range(LEV):
        low = strength if level else 0.0
        pivot = 1.0 + low + strength - low * ratio
        inner.append(pivot)
        last.append(1.0 + low - low * ratio)
        ratio = strength / pivot
    return inner, last


def lane_index():
    return lax.broadcasted_iota(jnp.int32, (SUB, LANES), 1)


def west_of(strips, edge, at_last):
    mixed = [jnp.where(at_last, edge if c == 0 else strips[c - 1], strips[c]) for c in range(len(strips))]
    return [pltpu.roll(x, 1, 1) for x in mixed]


def east_of(strips, edge, at_first):
    n = len(strips)
    mixed = [jnp.where(at_first, edge if c == n - 1 else strips[c + 1], strips[c]) for c in range(n)]
    return [pltpu.roll(x, LANES - 1, 1) for x in mixed]


def places(n_row):
    row = lax.axis_index('row')
    col = lax.axis_index('col')
    other = 1 - col
    has_north = row < n_row - 1
    has_south = row > 0
    return dict(
        row=row, has_north=has_north, has_south=has_south,
        side={'col': other, 'row': row},
        north={'col': col, 'row': row + 1}, south={'col': col, 'row': row - 1},
        north_side={'col': other, 'row': row + 1}, south_side={'col': other, 'row': row - 1})


def meet(at):
    barrier = pltpu.get_barrier_semaphore()
    pl.semaphore_signal(barrier, inc=1, device_id=at['side'], device_id_type=MESH)

    @pl.when(at['has_north'])
    def _():
        pl.semaphore_signal(barrier, inc=1, device_id=at['north'], device_id_type=MESH)
        pl.semaphore_signal(barrier, inc=1, device_id=at['north_side'], device_id_type=MESH)

    @pl.when(at['has_south'])
    def _():
        pl.semaphore_signal(barrier, inc=1, device_id=at['south'], device_id_type=MESH)
        pl.semaphore_signal(barrier, inc=1, device_id=at['south_side'], device_id_type=MESH)

    return barrier


def await_meet(barrier, at):
    pl.semaphore_wait(barrier, 1 + 2 * at['has_north'].astype(jnp.int32) + 2 * at['has_south'].astype(jnp.int32))


def remote(src, dst, send, recv, where):
    return pltpu.make_async_remote_copy(src_ref=src, dst_ref=dst, send_sem=send, recv_sem=recv, device_id=where, device_id_type=MESH)


def halo_kernel(n_row, u, v, t, s, eta, tu, tv, depth, count,
                north_rows, south_rows, side_cols, own_cols, counts, wide_north, wide_south, wide_side,
                edge, fold, zero, load_sem, zero_sem, send_sem, recv_sem):
    at = places(n_row)
    fields = (u, v, t, s)
    loads = []
    for f in range(4):
        for e in range(2):
            copy = pltpu.make_async_copy(fields[f].at[:, :, pl.ds(e * (COLS - LANES), LANES)], edge.at[f, e], load_sem.at[f, e])
            copy.start()
            loads.append(copy)
    barrier = meet(at)
    lane = lane_index()
    fast = (eta, tu, tv, depth)
    low_half = lax.broadcasted_iota(jnp.int32, (ROWS, LANES), 1) < LANES // 2
    for f in range(4):
        fold[f] = jnp.where(low_half, fast[f][:, :LANES], fast[f][:, COLS - LANES:])
    for c in range(STRIPS):
        counts[c, SUB:SUB + ROWS, :] = count[:, c * LANES:(c + 1) * LANES].astype(F32)

    @pl.when(jnp.logical_not(at['has_north']))
    def _():
        zero[...] = jnp.zeros_like(zero)
        counts[:, SUB + ROWS:, :] = jnp.zeros((STRIPS, SUB, LANES), F32)
        side_cols[:, SUB + ROWS:, :] = jnp.zeros((4, SUB, LANES), F32)
        wide_north[...] = jnp.zeros_like(wide_north)
        wide_side[:, REACH + ROWS:, :] = jnp.zeros((4, REACH, LANES), F32)
        for f in range(4):
            pltpu.make_async_copy(zero, north_rows.at[f], zero_sem.at[f]).start()

    @pl.when(jnp.logical_not(at['has_south']))
    def _():
        zero[...] = jnp.zeros_like(zero)
        counts[:, :SUB, :] = jnp.zeros((STRIPS, SUB, LANES), F32)
        side_cols[:, :SUB, :] = jnp.zeros((4, SUB, LANES), F32)
        wide_south[...] = jnp.zeros_like(wide_south)
        wide_side[:, :REACH, :] = jnp.zeros((4, REACH, LANES), F32)
        for f in range(4):
            pltpu.make_async_copy(zero, south_rows.at[f], zero_sem.at[f]).start()

    await_meet(barrier, at)
    slot = iter(range(64))
    go_north, go_south, go_side = [], [], []

    def send(bucket, src, dst, where):
        i = next(slot)
        bucket.append(remote(src, dst, send_sem.at[i], recv_sem.at[i], at[where]))

    for f in range(4):
        send(go_north, fields[f].at[:, pl.ds(ROWS - 1, 1), :], south_rows.at[f], 'north')
        send(go_south, fields[f].at[:, pl.ds(0, 1), :], north_rows.at[f], 'south')
    send(go_north, counts.at[:, pl.ds(ROWS, SUB), :], counts.at[:, pl.ds(0, SUB), :], 'north')
    send(go_south, counts.at[:, pl.ds(SUB, SUB), :], counts.at[:, pl.ds(SUB + ROWS, SUB), :], 'south')
    for f in range(4):
        send(go_north, fast[f].at[pl.ds(ROWS - REACH, REACH), :], wide_south.at[f], 'north')
        send(go_south, fast[f].at[pl.ds(0, REACH), :], wide_north.at[f], 'south')
    send(go_side, fold, wide_side.at[:, pl.ds(REACH, ROWS), :], 'side')
    send(go_north, fold.at[:, pl.ds(ROWS - REACH, REACH), :], wide_side.at[:, pl.ds(0, REACH), :], 'north_side')
    send(go_south, fold.at[:, pl.ds(0, REACH), :], wide_side.at[:, pl.ds(REACH + ROWS, REACH), :], 'south_side')

    @pl.when(at['has_north'])
    def _():
        for copy in go_north:
            copy.start()

    @pl.when(at['has_south'])
    def _():
        for copy in go_south:
            copy.start()

    for copy in go_side:
        copy.start()

    half = lane >> 1
    at_first = lane == 0
    for f in range(4):
        loads[2 * f].wait()
        loads[2 * f + 1].wait()

        def pack(tile, _):
            rows = pl.ds(pl.multiple_of(SUB * tile, SUB), SUB)
            packed = jnp.zeros((SUB, LANES), F32)
            for k in range(LEV + 1 if f == 0 else LEV):
                if k < LEV:
                    first, last = edge[f, 0, k, rows, :], edge[f, 1, k, rows, :]
                else:
                    shifted = pl.ds(pl.multiple_of(SUB * tile + SUB, SUB), SUB)
                    first, last = counts[0, shifted, :], counts[STRIPS - 1, shifted, :]
                both = pltpu.roll(jnp.where(at_first, first, last), 2 * k + 1, 1)
                packed = jnp.where(half == k, both, packed)
            own_cols[f, rows, :] = packed
            return 0

        lax.fori_loop(0, TILES, pack, 0)
        send(go_side, own_cols.at[f], side_cols.at[f, pl.ds(SUB, ROWS), :], 'side')
        go_side[-1].start()
    late_south, late_north = [], []
    send(late_south, own_cols.at[0, pl.ds(0, SUB), :], side_cols.at[0, pl.ds(SUB + ROWS, SUB), :], 'south_side')
    send(late_north, own_cols.at[1, pl.ds(ROWS - SUB, SUB), :], side_cols.at[1, pl.ds(0, SUB), :], 'north_side')

    @pl.when(at['has_north'])
    def _():
        late_north[0].start()

    @pl.when(at['has_south'])
    def _():
        late_south[0].start()

    for copy in go_side:
        copy.wait()

    @pl.when(at['has_north'])
    def _():
        for copy in go_north + late_north:
            copy.wait_send()
        for copy in go_south + late_south:
            copy.wait_recv()

    @pl.when(at['has_south'])
    def _():
        for copy in go_south + late_south:
            copy.wait_send()
        for copy in go_north + late_north:
            copy.wait_recv()

    @pl.when(jnp.logical_not(at['has_north']))
    def _():
        for f in range(4):
            pltpu.make_async_copy(zero, north_rows.at[f], zero_sem.at[f]).wait()

    @pl.when(jnp.logical_not(at['has_south']))
    def _():
        for f in range(4):
            pltpu.make_async_copy(zero, south_rows.at[f], zero_sem.at[f]).wait()


def force_kernel(n_row, force, wide_north, wide_south, wide_side, fold, send_sem, recv_sem):
    at = places(n_row)
    barrier = meet(at)
    low_half = lax.broadcasted_iota(jnp.int32, (ROWS, LANES), 1) < LANES // 2
    for f in range(2):
        fold[f] = jnp.where(low_half, force[f, :, :LANES], force[f, :, COLS - LANES:])

    @pl.when(jnp.logical_not(at['has_north']))
    def _():
        wide_north[...] = jnp.zeros_like(wide_north)
        wide_side[:, REACH + ROWS:, :] = jnp.zeros((2, REACH, LANES), F32)

    @pl.when(jnp.logical_not(at['has_south']))
    def _():
        wide_south[...] = jnp.zeros_like(wide_south)
        wide_side[:, :REACH, :] = jnp.zeros((2, REACH, LANES), F32)

    await_meet(barrier, at)

    def copy_of(i, src, dst, where):
        return remote(src, dst, send_sem.at[i], recv_sem.at[i], at[where])

    go_north = [copy_of(0, force.at[:, pl.ds(ROWS - REACH, REACH), :], wide_south, 'north'),
                copy_of(1, fold.at[:, pl.ds(ROWS - REACH, REACH), :], wide_side.at[:, pl.ds(0, REACH), :], 'north_side')]
    go_south = [copy_of(2, force.at[:, pl.ds(0, REACH), :], wide_north, 'south'),
                copy_of(3, fold.at[:, pl.ds(0, REACH), :], wide_side.at[:, pl.ds(REACH + ROWS, REACH), :], 'south_side')]
    go_side = copy_of(4, fold, wide_side.at[:, pl.ds(REACH, ROWS), :], 'side')

    @pl.when(at['has_north'])
    def _():
        for copy in go_north:
            copy.start()

    @pl.when(at['has_south'])
    def _():
        for copy in go_south:
            copy.start()

    go_side.start()
    go_side.wait()

    @pl.when(at['has_north'])
    def _():
        for copy in go_north:
            copy.wait_send()
        for copy in go_south:
            copy.wait_recv()

    @pl.when(at['has_south'])
    def _():
        for copy in go_south:
            copy.wait_send()
        for copy in go_north:
            copy.wait_recv()


def strip_copies(tile, fields, strips, sem):
    rows = pl.ds(pl.multiple_of(SUB * tile, SUB), SUB)
    return [pltpu.make_async_copy(fields[f].at[:, rows, pl.ds(LANES * c, LANES)], strips[f].at[c, pl.ds(1, LEV), rows, :], sem.at[tile, f, c])
            for f in range(len(fields)) for c in range(STRIPS)]


def border_copies(north_rows, south_rows, strips, sem):
    copies = []
    for f in range(len(strips)):
        for c in range(STRIPS):
            lanes = pl.ds(LANES * c, LANES)
            copies.append(pltpu.make_async_copy(north_rows.at[f, :, :, lanes], strips[f].at[c, pl.ds(1, LEV), pl.ds(ROWS, 1), :], sem.at[0, f, c]))
            copies.append(pltpu.make_async_copy(south_rows.at[f, :, :, lanes], strips[f].at[c, pl.ds(0, LEV), pl.ds(PITCH - 1, 1), :], sem.at[1, f, c]))
    return copies


def level_rows(tile, c, k, offset=0):
    return pl.ds(SUB * tile + (c * (LEV + 1) * PITCH + PITCH * (k + 1) + offset), SUB)


def face_counts(counts_flat, side_cols, tile, at_first):
    rows = SUB * tile + SUB
    mid = [counts_flat[pl.ds(rows + c * 64, SUB), :] for c in range(STRIPS)]
    north = [counts_flat[pl.ds(rows + c * 64 + 1, SUB), :] for c in range(STRIPS)]
    edge = pltpu.roll(side_cols[0, pl.ds(rows, SUB), :], LANES - 1 - 2 * LEV, 1)
    east = east_of(mid, edge, at_first)
    return mid, [jnp.minimum(a, b) for a, b in zip(mid, east)], [jnp.minimum(a, b) for a, b in zip(mid, north)]


def momentum_kernel(n_row, u, v, t, s, north_rows, south_rows, side_cols, counts,
                    wu_out, wv_out, force, level_mean,
                    u_s, v_s, t_s, s_s, p_s, b_s, wu, wv, load_sem, border_sem, store_sem):
    row = lax.axis_index('row')
    fields, strips = (u, v, t, s), (u_s, v_s, t_s, s_s)
    borders = border_copies(north_rows, south_rows, strips, border_sem)
    for copy in strip_copies(TILES - 1, fields, strips, load_sem):
        copy.start()
    for copy in borders:
        copy.start()
    for tile in range(TILES - 2, -1, -1):
        for copy in strip_copies(tile, fields, strips, load_sem):
            copy.start()
    for copy in strip_copies(TILES - 1, fields, strips, load_sem):
        copy.wait()
    for copy in borders:
        copy.wait()
    lane = lane_index()
    at_first, at_last = lane == 0, lane == LANES - 1
    rows_total = (LEV + 1) * PITCH * STRIPS
    uf, vf, tf, sf, pf, bf = [ref.reshape(rows_total, LANES) for ref in (u_s, v_s, t_s, s_s, p_s, b_s)]
    counts_flat = counts.reshape(STRIPS * 64, LANES)
    half_scale = 0.5 * BC_GRAVITY / LEV
    pivot, _ = tables(VISC_R)
    four = range(STRIPS)

    def density(sal, tem):
        return (half_scale * CONTRACT_S) * sal - (half_scale * EXPAND_T) * tem

    acc = [jnp.zeros((SUB, LANES), F32)] * STRIPS
    side_u = side_cols[0, pl.ds(SUB + ROWS, SUB), :]
    for k in range(LEV):
        edge = pltpu.roll(side_u, LANES - 1 - 2 * k, 1)
        uu = [uf[level_rows(TILES, c, k), :] for c in four]
        uw = west_of(uu, edge, at_last)
        for c in four:
            at = level_rows(TILES, c, k)
            bf[at, :] = uu[c] + uw[c]
            rho = density(sf[at, :], tf[at, :])
            pf[at, :] = acc[c] + rho
            acc[c] = (acc[c] + rho) + rho

    def tile_step(step, _):
        tile = TILES - 1 - step

        @pl.when(tile > 0)
        def _():
            for copy in strip_copies(tile - 1, fields, strips, load_sem):
                copy.wait()

        mid_count, nu, nv = face_counts(counts_flat, side_cols, tile, at_first)
        row_pos = (row * ROWS + SUB * tile + lax.broadcasted_iota(jnp.int32, (SUB, LANES), 0)).astype(F32)
        fu = 0.25 * (CORIO_F0 + CORIO_BETA * ((row_pos + 0.5) / (ROWS * n_row) - 0.5))
        fv = 0.25 * (CORIO_F0 + CORIO_BETA * ((row_pos + 1.0) / (ROWS * n_row) - 0.5))
        mid_rows = pl.ds(SUB * tile + SUB, SUB)
        side_u = side_cols[0, mid_rows, :]
        side_v = side_cols[1, mid_rows, :]
        side_a = side_v + side_cols[1, pl.ds(SUB * tile + 7, SUB), :]
        side_r = density(side_cols[3, mid_rows, :], side_cols[2, mid_rows, :])
        zero = jnp.zeros((SUB, LANES), F32)
        acc = [zero] * STRIPS
        acc_e = zero
        xu, xv = [zero] * STRIPS, [zero] * STRIPS
        sum_du, sum_dv, sum_su, sum_sv = [zero] * STRIPS, [zero] * STRIPS, [zero] * STRIPS, [zero] * STRIPS
        for k in range(LEV):
            turn = LANES - 1 - 2 * k
            here = [level_rows(tile, c, k) for c in four]
            up = [level_rows(tile, c, k, 1) for c in four]
            below = [level_rows(tile, c, k, -1) for c in four]
            uu = [uf[here[c], :] for c in four]
            vv = [vf[here[c], :] for c in four]
            v_south = [vf[below[c], :] for c in four]
            edge_u = pltpu.roll(side_u, turn, 1)
            edge_v = pltpu.roll(side_v, turn, 1)
            u_west = west_of(uu, edge_u, at_last)
            u_east = east_of(uu, edge_u, at_first)
            v_west = west_of(vv, edge_v, at_last)
            v_east = east_of(vv, edge_v, at_first)
            pair_v = [vv[c] + v_south[c] for c in four]
            pair_ve = east_of(pair_v, pltpu.roll(side_a, turn, 1), at_first)
            rho_e = pltpu.roll(side_r, turn, 1)
            p_edge = acc_e + rho_e
            acc_e = p_edge + rho_e
            pp = []
            for c in four:
                rho = density(sf[here[c], :], tf[here[c], :])
                pp.append(acc[c] + rho)
                acc[c] = pp[c] + rho
                pf[here[c], :] = pp[c]
            p_east = east_of(pp, p_edge, at_first)
            for c in four:
                pair_u = uu[c] + u_west[c]
                bf[here[c], :] = pair_u
                v4 = pair_v[c] + pair_ve[c]
                u4 = pair_u + bf[up[c], :]
                du = v4 * (fu - 0.125 * (uf[up[c], :] - uf[below[c], :])) - 0.5 * uu[c] * (u_east[c] - u_west[c]) + (pp[c] - p_east[c])
                dv = (pp[c] - pf[up[c], :]) - u4 * (fv + 0.125 * (v_east[c] - v_west[c])) - 0.5 * vv[c] * (vf[up[c], :] - v_south[c])
                us, vs = uu[c] + du, vv[c] + dv
                on_u, on_v = nu[c] > k, nv[c] > k
                sum_du[c] += jnp.where(on_u, du, 0.0)
                sum_dv[c] += jnp.where(on_v, dv, 0.0)
                sum_su[c] += jnp.where(on_u, us, 0.0)
                sum_sv[c] += jnp.where(on_v, vs, 0.0)
                xu[c] = us * (1.0 / pivot[k]) + xu[c] * (VISC_R / pivot[k])
                xv[c] = vs * (1.0 / pivot[k]) + xv[c] * (VISC_R / pivot[k])
                wu[tile, k, c] = xu[c]
                wv[tile, k, c] = xv[c]
        out_rows = pl.ds(pl.multiple_of(SUB * tile, SUB), SUB)
        for c in four:
            lanes = pl.ds(LANES * c, LANES)
            inv_u = 1.0 / jnp.maximum(nu[c], 1.0)
            inv_v = 1.0 / jnp.maximum(nv[c], 1.0)
            force[0, out_rows, lanes] = sum_du[c] * inv_u
            force[1, out_rows, lanes] = sum_dv[c] * inv_v
            level_mean[0, out_rows, lanes] = sum_su[c] * inv_u
            level_mean[1, out_rows, lanes] = sum_sv[c] * inv_v
        pltpu.make_async_copy(wu.at[tile], wu_out.at[tile], store_sem.at[0, tile]).start()
        pltpu.make_async_copy(wv.at[tile], wv_out.at[tile], store_sem.at[1, tile]).start()
        return 0

    lax.fori_loop(0, TILES, tile_step, 0)
    for tile in range(TILES):
        pltpu.make_async_copy(wu.at[tile], wu_out.at[tile], store_sem.at[0, tile]).wait()
        pltpu.make_async_copy(wv.at[tile], wv_out.at[tile], store_sem.at[1, tile]).wait()


def tracer_kernel(u, v, t, s, north_rows, south_rows, side_cols, own_cols, counts,
                  t_out, s_out,
                  u_s, v_s, t_s, s_s, ft_s, fs_s, wt, ws, t_new, s_new, load_sem, border_sem, store_sem):
    fields, strips = (u, v, t, s), (u_s, v_s, t_s, s_s)
    borders = border_copies(north_rows, south_rows, strips, border_sem)
    for copy in strip_copies(0, fields, strips, load_sem):
        copy.start()
    for copy in borders:
        copy.start()
    for tile in range(1, TILES):
        for copy in strip_copies(tile, fields, strips, load_sem):
            copy.start()
    for copy in strip_copies(0, fields, strips, load_sem):
        copy.wait()
    for copy in borders:
        copy.wait()
    lane = lane_index()
    at_first, at_last = lane == 0, lane == LANES - 1
    even = (lane & 1) == 0
    half = (lane >> 1).astype(F32)
    rows_total = (LEV + 1) * PITCH * STRIPS
    uf, vf, tf, sf, ftf, fsf = [ref.reshape(rows_total, LANES) for ref in (u_s, v_s, t_s, s_s, ft_s, fs_s)]
    counts_flat = counts.reshape(STRIPS * 64, LANES)
    pivot, final = tables(DIFF_R)
    four = range(STRIPS)
    scale = 0.5 * TIME_STEP

    south_count = [jnp.minimum(counts_flat[pl.ds(c * 64, SUB), :], counts_flat[pl.ds(c * 64 + 1, SUB), :]) for c in four]
    for k in range(LEV):
        for c in four:
            here, up = level_rows(-1, c, k), level_rows(-1, c, k, 1)
            hv = jnp.where(south_count[c] > k, scale * vf[here, :], 0.0)
            ftf[here, :] = hv * (tf[here, :] + tf[up, :])
            fsf[here, :] = hv * (sf[here, :] + sf[up, :])

    def tile_step(tile, _):
        @pl.when(tile < TILES - 1)
        def _():
            for copy in strip_copies(tile + 1, fields, strips, load_sem):
                copy.wait()

        mid, nu, nv = face_counts(counts_flat, side_cols, tile, at_first)
        mid_rows = pl.ds(SUB * tile + SUB, SUB)
        own_rows = pl.ds(SUB * tile, SUB)
        side_u = side_cols[0, mid_rows, :]
        west_count = jnp.minimum(side_u[:, 2 * LEV:2 * LEV + 1], mid[0][:, 0:1])
        west_half = jnp.where(half < west_count, scale * side_u, 0.0)
        side_t, side_s = side_cols[2, mid_rows, :], side_cols[3, mid_rows, :]
        mix_t = jnp.where(even, west_half * (side_t + pltpu.roll(own_cols[2, own_rows, :], LANES - 1, 1)), side_t)
        mix_s = jnp.where(even, west_half * (side_s + pltpu.roll(own_cols[3, own_rows, :], LANES - 1, 1)), side_s)
        zero = jnp.zeros((SUB, LANES), F32)
        xt, xs = [zero] * STRIPS, [zero] * STRIPS
        for k in range(LEV):
            turn = LANES - 1 - 2 * k
            here = [level_rows(tile, c, k) for c in four]
            up = [level_rows(tile, c, k, 1) for c in four]
            below = [level_rows(tile, c, k, -1) for c in four]
            hu = [jnp.where(nu[c] > k, scale * uf[here[c], :], 0.0) for c in four]
            hv = [jnp.where(nv[c] > k, scale * vf[here[c], :], 0.0) for c in four]
            if k < LEV - 1:
                inverse = [jnp.where(mid[c] > k + 1, 1.0 / pivot[k], 1.0 / final[k]) for c in four]
            else:
                inverse = [1.0 / final[k]] * STRIPS

            def advance(flat, flux, mix, x, w):
                q = [flat[here[c], :] for c in four]
                edge = pltpu.roll(mix, turn, 1)
                q_east = east_of(q, edge, at_first)
                flux_e = [hu[c] * (q[c] + q_east[c]) for c in four]
                flux_w = west_of(flux_e, edge, at_last)
                for c in four:
                    flux_n = hv[c] * (q[c] + flat[up[c], :])
                    flux[here[c], :] = flux_n
                    new = q[c] - ((flux_e[c] - flux_w[c]) + (flux_n - flux[below[c], :]))
                    x[c] = (new + DIFF_R * x[c]) * inverse[c]
                    w[k, c] = x[c]

            advance(tf, ftf, mix_t, xt, wt)
            advance(sf, fsf, mix_s, xs, ws)
        bt, bs = [zero] * STRIPS, [zero] * STRIPS
        out_rows = pl.ds(pl.multiple_of(SUB * tile, SUB), SUB)
        for k in range(LEV - 1, -1, -1):
            for c in four:
                here = level_rows(tile, c, k)
                lanes = pl.ds(LANES * c, LANES)
                on = mid[c] > k
                yt = wt[k, c] + (DIFF_R / pivot[k]) * bt[c]
                ys = ws[k, c] + (DIFF_R / pivot[k]) * bs[c]
                t_new[k, out_rows, lanes] = jnp.where(on, yt, tf[here, :])
                s_new[k, out_rows, lanes] = jnp.where(on, ys, sf[here, :])
                bt[c] = jnp.where(on, yt, 0.0)
                bs[c] = jnp.where(on, ys, 0.0)
        pltpu.make_async_copy(t_new.at[:, out_rows, :], t_out.at[:, out_rows, :], store_sem.at[0, tile]).start()
        pltpu.make_async_copy(s_new.at[:, out_rows, :], s_out.at[:, out_rows, :], store_sem.at[1, tile]).start()
        return 0

    lax.fori_loop(0, TILES, tile_step, 0)
    for tile in range(TILES):
        rows = pl.ds(SUB * tile, SUB)
        pltpu.make_async_copy(t_new.at[:, rows, :], t_out.at[:, rows, :], store_sem.at[0, tile]).wait()
        pltpu.make_async_copy(s_new.at[:, rows, :], s_out.at[:, rows, :], store_sem.at[1, tile]).wait()


def fast_kernel(n_row, n_sub, weights, wu_in, wv_in, eta, tu, tv, depth, wide_north, wide_south, wide_side,
                force, force_north, force_south, force_side, level_mean, counts, side_cols,
                eta_out, tu_out, tv_out, u_out, v_out,
                e_s, u_s, v_s, b_s, d_s, cu_s, cv_s, bu_s, bv_s, fu_s, fv_s, bar_u, bar_v, wu, wv, u_new, v_new, load_sem, store_sem):
    row = lax.axis_index('row')
    for tile in range(TILES):
        pltpu.make_async_copy(wu_in.at[tile], wu.at[tile], load_sem.at[0, tile]).start()
        pltpu.make_async_copy(wv_in.at[tile], wv.at[tile], load_sem.at[1, tile]).start()
    lane = lane_index()
    at_first, at_last = lane == 0, lane == LANES - 1
    five = range(STRIPS + 1)
    dt_fast = TIME_STEP / n_sub
    total = ROWS * n_row
    zero = jnp.zeros((SUB, LANES), F32)

    def page(tile, c, offset=0):
        return pl.ds(c * PAGE + SUB + SUB * tile + offset, SUB)

    def gather(f, own, north, south, side, tile, c):
        if c == STRIPS:
            return side[f, SUB * tile:SUB * tile + SUB, :]
        lanes = slice(c * LANES, (c + 1) * LANES)
        if tile < REACH // SUB:
            return south[f, SUB * tile:SUB * tile + SUB, lanes]
        if tile < (REACH + ROWS) // SUB:
            return own[SUB * tile - REACH:SUB * tile - REACH + SUB, lanes]
        start = SUB * tile - REACH - ROWS
        return north[f, start:start + SUB, lanes]

    for ref in (e_s, u_s, v_s, b_s, d_s):
        for c in five:
            ref[page(-1, c), :] = zero
            ref[page(EXT_TILES, c), :] = zero
    for tile in range(EXT_TILES):
        for c in five:
            at = page(tile, c)
            e_s[at, :] = gather(0, eta, wide_north, wide_south, wide_side, tile, c)
            u_s[at, :] = gather(1, tu, wide_north, wide_south, wide_side, tile, c)
            v_s[at, :] = gather(2, tv, wide_north, wide_south, wide_side, tile, c)
            d_s[at, :] = gather(3, depth, wide_north, wide_south, wide_side, tile, c)
            bu_s[at, :] = gather(0, force.at[0], force_north, force_south, force_side, tile, c)
            bv_s[at, :] = gather(1, force.at[1], force_north, force_south, force_side, tile, c)
    for tile in range(EXT_TILES):
        place = row * ROWS + (SUB * tile - REACH) + lax.broadcasted_iota(jnp.int32, (SUB, LANES), 0)
        inside = jnp.logical_and(place >= 0, place < total)
        inside_v = jnp.logical_and(place >= 0, place < total - 1)
        row_pos = place.astype(F32)
        fu = (0.25 * dt_fast) * (CORIO_F0 + CORIO_BETA * ((row_pos + 0.5) / total - 0.5))
        fv = (0.25 * dt_fast) * (CORIO_F0 + CORIO_BETA * ((row_pos + 1.0) / total - 0.5))
        fu_s[SUB * tile:SUB * tile + SUB, :] = jnp.where(inside, fu, 0.0)
        fv_s[SUB * tile:SUB * tile + SUB, :] = jnp.where(inside_v, fv, 0.0)
        deep = [d_s[page(tile, c), :] for c in five]
        deep_e = east_of(deep, deep[0], at_first)
        for c in five:
            at = page(tile, c)
            hu = jnp.where(inside, 0.5 * (deep[c] + deep_e[c]), 0.0)
            hv = jnp.where(inside_v, 0.5 * (deep[c] + d_s[page(tile, c, 1), :]), 0.0)
            cu_s[at, :] = (dt_fast * GRAVITY) * hu
            cv_s[at, :] = (dt_fast * GRAVITY) * hv
            bu_s[at, :] = (dt_fast / TIME_STEP) * hu * bu_s[at, :]
            bv_s[at, :] = (dt_fast / TIME_STEP) * hv * bv_s[at, :]
    bar_u[...] = jnp.zeros_like(bar_u)
    bar_v[...] = jnp.zeros_like(bar_v)

    def subcycle(n, low, high):
        weight = weights[n]
        for tile in range(high - 1, low - 1, -1):
            uu = [u_s[page(tile, c), :] for c in five]
            vv = [v_s[page(tile, c), :] for c in five]
            v_south = [v_s[page(tile, c, -1), :] for c in five]
            u_west = west_of(uu, uu[-1], at_last)
            ee = []
            for c in five:
                at = page(tile, c)
                new = e_s[at, :] - dt_fast * ((uu[c] - u_west[c]) + (vv[c] - v_south[c]))
                e_s[at, :] = new
                ee.append(new)
                b_s[at, :] = uu[c] + u_west[c]
            pair_v = [vv[c] + v_south[c] for c in five]
            pair_ve = east_of(pair_v, pair_v[0], at_first)
            e_east = east_of(ee, ee[0], at_first)
            fu = fu_s[SUB * tile:SUB * tile + SUB, :]
            fv = fv_s[SUB * tile:SUB * tile + SUB, :]
            for c in five:
                at, up = page(tile, c), page(tile, c, 1)
                u_next = uu[c] + ((fu * (pair_v[c] + pair_ve[c]) + bu_s[at, :]) - cu_s[at, :] * (e_east[c] - ee[c]))
                v_next = vv[c] + ((bv_s[at, :] - fv * ((uu[c] + u_west[c]) + b_s[up, :])) - cv_s[at, :] * (e_s[up, :] - ee[c]))
                u_s[at, :] = u_next
                v_s[at, :] = v_next
                if c < STRIPS and REACH // SUB <= tile < (REACH + ROWS) // SUB:
                    own = tile - REACH // SUB
                    bar_u[own, c] += weight * u_next
                    bar_v[own, c] += weight * v_next

    def wall_row():
        for tile in range(EXT_TILES):
            place = row * ROWS + (SUB * tile - REACH) + lax.broadcasted_iota(jnp.int32, (SUB, LANES), 0)
            wet = jnp.logical_and(place >= 0, place < total - 1)
            for c in five:
                at = page(tile, c)
                v_s[at, :] = jnp.where(wet, v_s[at, :], 0.0)
                if c < STRIPS and REACH // SUB <= tile < (REACH + ROWS) // SUB:
                    own = tile - REACH // SUB
                    bar_v[own, c] = jnp.where(wet, bar_v[own, c], 0.0)

    n = 0
    while n < n_sub:
        spread = -(-(n_sub - n) // SUB)
        stop = n_sub - SUB * (spread - 1)
        low, high = REACH // SUB - spread, (REACH + ROWS) // SUB + spread

        def some(i, _, low=low, high=high, first=(n == 0)):
            subcycle(i, low, high)
            if first:
                pl.when(i == 0)(wall_row)
            return 0

        lax.fori_loop(n, stop, some, 0)
        n = stop

    counts_flat = counts.reshape(STRIPS * 64, LANES)
    pivot, final = tables(VISC_R)
    four = range(STRIPS)
    for tile in range(TILES):
        for c in four:
            at = page(tile + REACH // SUB, c)
            rows, lanes = pl.ds(SUB * tile, SUB), pl.ds(LANES * c, LANES)
            eta_out[rows, lanes] = e_s[at, :]
            tu_out[rows, lanes] = u_s[at, :]
            tv_out[rows, lanes] = v_s[at, :]

    def tile_step(tile, _):
        pltpu.make_async_copy(wu_in.at[tile], wu.at[tile], load_sem.at[0, tile]).wait()
        pltpu.make_async_copy(wv_in.at[tile], wv.at[tile], load_sem.at[1, tile]).wait()
        mid, nu, nv = face_counts(counts_flat, side_cols, tile, at_first)
        out_rows = pl.ds(pl.multiple_of(SUB * tile, SUB), SUB)
        add_u, add_v = [], []
        for c in four:
            at = pl.ds(c * PAGE + SUB + REACH + SUB * tile, SUB)
            lanes = pl.ds(LANES * c, LANES)
            deep_u = cu_s[at, :] * (1.0 / (dt_fast * GRAVITY))
            deep_v = cv_s[at, :] * (1.0 / (dt_fast * GRAVITY))
            deep_v = jnp.where(nv[c] > 0, deep_v, 1.0)
            add_u.append(bar_u[tile, c] / deep_u - level_mean[0, out_rows, lanes])
            add_v.append(bar_v[tile, c] / deep_v - level_mean[1, out_rows, lanes])
        xu, xv = [zero] * STRIPS, [zero] * STRIPS
        for k in range(LEV - 1, -1, -1):
            ratio, bottom = VISC_R / pivot[k], pivot[k] / final[k]
            for c in four:
                lanes = pl.ds(LANES * c, LANES)

                def solve(w, x, n, add, out):
                    value = w[tile, k, c]
                    last = value * bottom
                    if k < LEV - 1:
                        x[c] = jnp.where(n[c] > k + 1, value + ratio * x[c], last)
                    else:
                        x[c] = last
                    out[k, out_rows, lanes] = jnp.where(n[c] > k, x[c] + add[c], 0.0)

                solve(wu, xu, nu, add_u, u_new)
                solve(wv, xv, nv, add_v, v_new)
        pltpu.make_async_copy(u_new.at[:, out_rows, :], u_out.at[:, out_rows, :], store_sem.at[0, tile]).start()
        pltpu.make_async_copy(v_new.at[:, out_rows, :], v_out.at[:, out_rows, :], store_sem.at[1, tile]).start()
        return 0

    lax.fori_loop(0, TILES, tile_step, 0)
    for tile in range(TILES):
        rows = pl.ds(SUB * tile, SUB)
        pltpu.make_async_copy(u_new.at[:, rows, :], u_out.at[:, rows, :], store_sem.at[0, tile]).wait()
        pltpu.make_async_copy(v_new.at[:, rows, :], v_out.at[:, rows, :], store_sem.at[1, tile]).wait()


def solution(mesh):
    n_row = mesh.shape['row']
    hbm = pl.BlockSpec(memory_space=pltpu.HBM)
    vmem = pl.BlockSpec(memory_space=pltpu.VMEM)
    smem = pl.BlockSpec(memory_space=pltpu.SMEM)
    dma = pltpu.SemaphoreType.DMA
    strip = pltpu.VMEM((STRIPS, LEV + 1, PITCH, LANES), F32)
    whole = pltpu.VMEM((LEV, ROWS, COLS), F32)
    column = pltpu.VMEM((TILES, LEV, STRIPS, SUB, LANES), F32)
    one = pltpu.VMEM((LEV, STRIPS, SUB, LANES), F32)
    extended = pltpu.VMEM(((STRIPS + 1) * PAGE, LANES), F32)

    def shape(*dims):
        return jax.ShapeDtypeStruct(dims, F32)

    def call(body, ins, outs, shapes, scratch, **params):
        return pl.pallas_call(body, out_shape=shapes, in_specs=ins, out_specs=outs, scratch_shapes=scratch,
                              compiler_params=pltpu.CompilerParams(vmem_limit_bytes=VMEM_LIMIT, **params))

    def step(vel_u, vel_v, temp, salt, eta, tu, tv, depth, count, weights):
        n_sub = weights.shape[0]
        north_rows, south_rows, side_cols, own_cols, counts, wide_north, wide_south, wide_side = call(
            functools.partial(halo_kernel, n_row), [hbm] * 4 + [vmem] * 5, [hbm] * 2 + [vmem] * 6,
            [shape(4, LEV, 1, COLS)] * 2 + [shape(4, ROWS + 16, LANES), shape(4, ROWS, LANES), shape(STRIPS, ROWS + 16, LANES),
                                            shape(4, REACH, COLS), shape(4, REACH, COLS), shape(4, EXT, LANES)],
            [pltpu.VMEM((4, 2, LEV, ROWS, LANES), F32), pltpu.VMEM((4, ROWS, LANES), F32), pltpu.VMEM((LEV, 1, COLS), F32),
             dma((4, 2)), dma((4,)), dma((32,)), dma((32,))],
            collective_id=0, has_side_effects=True)(vel_u, vel_v, temp, salt, eta, tu, tv, depth, count)
        wu, wv, force, level_mean = call(
            functools.partial(momentum_kernel, n_row), [hbm] * 6 + [vmem] * 2, [hbm] * 2 + [vmem] * 2,
            [shape(TILES, LEV, STRIPS, SUB, LANES)] * 2 + [shape(2, ROWS, COLS)] * 2,
            [strip] * 6 + [column] * 2 + [dma((TILES, 4, STRIPS)), dma((2, 4, STRIPS)), dma((2, TILES))],
        )(vel_u, vel_v, temp, salt, north_rows, south_rows, side_cols, counts)
        force_north, force_south, force_side = call(
            functools.partial(force_kernel, n_row), [vmem], [vmem] * 3,
            [shape(2, REACH, COLS), shape(2, REACH, COLS), shape(2, EXT, LANES)],
            [pltpu.VMEM((2, ROWS, LANES), F32), dma((5,)), dma((5,))],
            collective_id=1, has_side_effects=True)(force)
        temp_new, salt_new = call(
            tracer_kernel, [hbm] * 6 + [vmem] * 3, [hbm] * 2,
            [shape(LEV, ROWS, COLS)] * 2,
            [strip] * 6 + [one] * 2 + [whole] * 2 + [dma((TILES, 4, STRIPS)), dma((2, 4, STRIPS)), dma((2, TILES))],
        )(vel_u, vel_v, temp, salt, north_rows, south_rows, side_cols, own_cols, counts)
        eta_new, tu_new, tv_new, u_new, v_new = call(
            functools.partial(fast_kernel, n_row, n_sub), [smem] + [hbm] * 2 + [vmem] * 14, [vmem] * 3 + [hbm] * 2,
            [shape(ROWS, COLS)] * 3 + [shape(LEV, ROWS, COLS)] * 2,
            [extended] * 9 + [pltpu.VMEM((EXT, LANES), F32)] * 2 + [pltpu.VMEM((TILES, STRIPS, SUB, LANES), F32)] * 2
            + [column] * 2 + [whole] * 2 + [dma((2, TILES)), dma((2, TILES))],
        )(weights, wu, wv, eta, tu, tv, depth, wide_north, wide_south, wide_side,
          force, force_north, force_south, force_side, level_mean, counts, side_cols)
        return eta_new, tu_new, tv_new, u_new, v_new, temp_new, salt_new

    cube = P(None, 'row', 'col')
    flat = P('row', 'col')
    return jax.shard_map(step, mesh=mesh, in_specs=(cube, cube, cube, cube, flat, flat, flat, flat, flat, P()),
                         out_specs=(flat, flat, flat, cube, cube, cube, cube), check_vma=False)
```

```python
import functools

import jax
import jax.numpy as jnp
from jax import lax
from jax.experimental import pallas as pl
from jax.experimental.pallas import tpu as pltpu
from jax.sharding import PartitionSpec as P

TIME_STEP = 1.0
GRAVITY = 16.0
BC_GRAVITY = 4.0
EXPAND_T = 0.2
CONTRACT_S = 0.6
CORIO_F0 = 0.4
CORIO_BETA = 0.4
VISC_R = 2.0
DIFF_R = 0.5

LEV = 41
ROWS = 48
SUB = 8
COLS = 512
LANES = 128
STRIPS = COLS // LANES
TILES = ROWS // SUB
PITCH = 56
REACH = 32
EXT = ROWS + 2 * REACH
EXT_TILES = EXT // SUB
PAGE = EXT + 16
MESH = pl.DeviceIdType.MESH
F32 = jnp.float32
VMEM_LIMIT = 62 * 1024 * 1024


def tables(strength):
    inner, last, ratio = [], [], 0.0
    for level in range(LEV):
        low = strength if level else 0.0
        pivot = 1.0 + low + strength - low * ratio
        inner.append(pivot)
        last.append(1.0 + low - low * ratio)
        ratio = strength / pivot
    return inner, last


def lane_index():
    return lax.broadcasted_iota(jnp.int32, (SUB, LANES), 1)


def west_of(strips, edge, at_last):
    mixed = [jnp.where(at_last, edge if c == 0 else strips[c - 1], strips[c]) for c in range(len(strips))]
    return [pltpu.roll(x, 1, 1) for x in mixed]


def east_of(strips, edge, at_first):
    n = len(strips)
    mixed = [jnp.where(at_first, edge if c == n - 1 else strips[c + 1], strips[c]) for c in range(n)]
    return [pltpu.roll(x, LANES - 1, 1) for x in mixed]


def places(n_row):
    row = lax.axis_index('row')
    col = lax.axis_index('col')
    other = 1 - col
    has_north = row < n_row - 1
    has_south = row > 0
    return dict(
        row=row, has_north=has_north, has_south=has_south,
        side={'col': other, 'row': row},
        north={'col': col, 'row': row + 1}, south={'col': col, 'row': row - 1},
        north_side={'col': other, 'row': row + 1}, south_side={'col': other, 'row': row - 1})


def meet(at):
    barrier = pltpu.get_barrier_semaphore()
    pl.semaphore_signal(barrier, inc=1, device_id=at['side'], device_id_type=MESH)

    @pl.when(at['has_north'])
    def _():
        pl.semaphore_signal(barrier, inc=1, device_id=at['north'], device_id_type=MESH)
        pl.semaphore_signal(barrier, inc=1, device_id=at['north_side'], device_id_type=MESH)

    @pl.when(at['has_south'])
    def _():
        pl.semaphore_signal(barrier, inc=1, device_id=at['south'], device_id_type=MESH)
        pl.semaphore_signal(barrier, inc=1, device_id=at['south_side'], device_id_type=MESH)

    return barrier


def await_meet(barrier, at):
    pl.semaphore_wait(barrier, 1 + 2 * at['has_north'].astype(jnp.int32) + 2 * at['has_south'].astype(jnp.int32))


def remote(src, dst, send, recv, where):
    return pltpu.make_async_remote_copy(src_ref=src, dst_ref=dst, send_sem=send, recv_sem=recv, device_id=where, device_id_type=MESH)


def halo_kernel(n_row, u, v, t, s, eta, tu, tv, depth, count,
                north_rows, south_rows, side_cols, own_cols, counts, wide_north, wide_south, wide_side,
                edge, fold, zero, load_sem, zero_sem, send_sem, recv_sem):
    at = places(n_row)
    fields = (u, v, t, s)
    loads = []
    for f in range(4):
        for e in range(2):
            copy = pltpu.make_async_copy(fields[f].at[:, :, pl.ds(e * (COLS - LANES), LANES)], edge.at[f, e], load_sem.at[f, e])
            copy.start()
            loads.append(copy)
    barrier = meet(at)
    lane = lane_index()
    fast = (eta, tu, tv, depth)
    low_half = lax.broadcasted_iota(jnp.int32, (ROWS, LANES), 1) < LANES // 2
    for f in range(4):
        fold[f] = jnp.where(low_half, fast[f][:, :LANES], fast[f][:, COLS - LANES:])
    for c in range(STRIPS):
        counts[c, SUB:SUB + ROWS, :] = count[:, c * LANES:(c + 1) * LANES].astype(F32)

    @pl.when(jnp.logical_not(at['has_north']))
    def _():
        zero[...] = jnp.zeros_like(zero)
        counts[:, SUB + ROWS:, :] = jnp.zeros((STRIPS, SUB, LANES), F32)
        side_cols[:, SUB + ROWS:, :] = jnp.zeros((4, SUB, LANES), F32)
        wide_north[...] = jnp.zeros_like(wide_north)
        wide_side[:, REACH + ROWS:, :] = jnp.zeros((4, REACH, LANES), F32)
        for f in range(4):
            pltpu.make_async_copy(zero, north_rows.at[f], zero_sem.at[f]).start()

    @pl.when(jnp.logical_not(at['has_south']))
    def _():
        zero[...] = jnp.zeros_like(zero)
        counts[:, :SUB, :] = jnp.zeros((STRIPS, SUB, LANES), F32)
        side_cols[:, :SUB, :] = jnp.zeros((4, SUB, LANES), F32)
        wide_south[...] = jnp.zeros_like(wide_south)
        wide_side[:, :REACH, :] = jnp.zeros((4, REACH, LANES), F32)
        for f in range(4):
            pltpu.make_async_copy(zero, south_rows.at[f], zero_sem.at[f]).start()

    await_meet(barrier, at)
    slot = iter(range(64))
    go_north, go_south, go_side = [], [], []

    def send(bucket, src, dst, where):
        i = next(slot)
        bucket.append(remote(src, dst, send_sem.at[i], recv_sem.at[i], at[where]))

    for f in range(4):
        send(go_north, fields[f].at[:, pl.ds(ROWS - 1, 1), :], south_rows.at[f], 'north')
        send(go_south, fields[f].at[:, pl.ds(0, 1), :], north_rows.at[f], 'south')
    send(go_north, counts.at[:, pl.ds(ROWS, SUB), :], counts.at[:, pl.ds(0, SUB), :], 'north')
    send(go_south, counts.at[:, pl.ds(SUB, SUB), :], counts.at[:, pl.ds(SUB + ROWS, SUB), :], 'south')
    for f in range(4):
        send(go_north, fast[f].at[pl.ds(ROWS - REACH, REACH), :], wide_south.at[f], 'north')
        send(go_south, fast[f].at[pl.ds(0, REACH), :], wide_north.at[f], 'south')
    send(go_side, fold, wide_side.at[:, pl.ds(REACH, ROWS), :], 'side')
    send(go_north, fold.at[:, pl.ds(ROWS - REACH, REACH), :], wide_side.at[:, pl.ds(0, REACH), :], 'north_side')
    send(go_south, fold.at[:, pl.ds(0, REACH), :], wide_side.at[:, pl.ds(REACH + ROWS, REACH), :], 'south_side')

    @pl.when(at['has_north'])
    def _():
        for copy in go_north:
            copy.start()

    @pl.when(at['has_south'])
    def _():
        for copy in go_south:
            copy.start()

    for copy in go_side:
        copy.start()

    half = lane >> 1
    at_first = lane == 0
    for f in range(4):
        loads[2 * f].wait()
        loads[2 * f + 1].wait()

        def pack(tile, _):
            rows = pl.ds(pl.multiple_of(SUB * tile, SUB), SUB)
            packed = jnp.zeros((SUB, LANES), F32)
            for k in range(LEV + 1 if f == 0 else LEV):
                if k < LEV:
                    first, last = edge[f, 0, k, rows, :], edge[f, 1, k, rows, :]
                else:
                    shifted = pl.ds(pl.multiple_of(SUB * tile + SUB, SUB), SUB)
                    first, last = counts[0, shifted, :], counts[STRIPS - 1, shifted, :]
                both = pltpu.roll(jnp.where(at_first, first, last), 2 * k + 1, 1)
                packed = jnp.where(half == k, both, packed)
            own_cols[f, rows, :] = packed
            return 0

        lax.fori_loop(0, TILES, pack, 0)
        send(go_side, own_cols.at[f], side_cols.at[f, pl.ds(SUB, ROWS), :], 'side')
        go_side[-1].start()
    late_south, late_north = [], []
    send(late_south, own_cols.at[0, pl.ds(0, SUB), :], side_cols.at[0, pl.ds(SUB + ROWS, SUB), :], 'south_side')
    send(late_north, own_cols.at[1, pl.ds(ROWS - SUB, SUB), :], side_cols.at[1, pl.ds(0, SUB), :], 'north_side')

    @pl.when(at['has_north'])
    def _():
        late_north[0].start()

    @pl.when(at['has_south'])
    def _():
        late_south[0].start()

    for copy in go_side:
        copy.wait()

    @pl.when(at['has_north'])
    def _():
        for copy in go_north + late_north:
            copy.wait_send()
        for copy in go_south + late_south:
            copy.wait_recv()

    @pl.when(at['has_south'])
    def _():
        for copy in go_south + late_south:
            copy.wait_send()
        for copy in go_north + late_north:
            copy.wait_recv()

    @pl.when(jnp.logical_not(at['has_north']))
    def _():
        for f in range(4):
            pltpu.make_async_copy(zero, north_rows.at[f], zero_sem.at[f]).wait()

    @pl.when(jnp.logical_not(at['has_south']))
    def _():
        for f in range(4):
            pltpu.make_async_copy(zero, south_rows.at[f], zero_sem.at[f]).wait()


def force_kernel(n_row, force, wide_north, wide_south, wide_side, fold, send_sem, recv_sem):
    at = places(n_row)
    barrier = meet(at)
    low_half = lax.broadcasted_iota(jnp.int32, (ROWS, LANES), 1) < LANES // 2
    for f in range(2):
        fold[f] = jnp.where(low_half, force[f, :, :LANES], force[f, :, COLS - LANES:])

    @pl.when(jnp.logical_not(at['has_north']))
    def _():
        wide_north[...] = jnp.zeros_like(wide_north)
        wide_side[:, REACH + ROWS:, :] = jnp.zeros((2, REACH, LANES), F32)

    @pl.when(jnp.logical_not(at['has_south']))
    def _():
        wide_south[...] = jnp.zeros_like(wide_south)
        wide_side[:, :REACH, :] = jnp.zeros((2, REACH, LANES), F32)

    await_meet(barrier, at)

    def copy_of(i, src, dst, where):
        return remote(src, dst, send_sem.at[i], recv_sem.at[i], at[where])

    go_north = [copy_of(0, force.at[:, pl.ds(ROWS - REACH, REACH), :], wide_south, 'north'),
                copy_of(1, fold.at[:, pl.ds(ROWS - REACH, REACH), :], wide_side.at[:, pl.ds(0, REACH), :], 'north_side')]
    go_south = [copy_of(2, force.at[:, pl.ds(0, REACH), :], wide_north, 'south'),
                copy_of(3, fold.at[:, pl.ds(0, REACH), :], wide_side.at[:, pl.ds(REACH + ROWS, REACH), :], 'south_side')]
    go_side = copy_of(4, fold, wide_side.at[:, pl.ds(REACH, ROWS), :], 'side')

    @pl.when(at['has_north'])
    def _():
        for copy in go_north:
            copy.start()

    @pl.when(at['has_south'])
    def _():
        for copy in go_south:
            copy.start()

    go_side.start()
    go_side.wait()

    @pl.when(at['has_north'])
    def _():
        for copy in go_north:
            copy.wait_send()
        for copy in go_south:
            copy.wait_recv()

    @pl.when(at['has_south'])
    def _():
        for copy in go_south:
            copy.wait_send()
        for copy in go_north:
            copy.wait_recv()


def strip_copies(tile, fields, strips, sem):
    rows = pl.ds(pl.multiple_of(SUB * tile, SUB), SUB)
    return [pltpu.make_async_copy(fields[f].at[:, rows, pl.ds(LANES * c, LANES)], strips[f].at[c, pl.ds(1, LEV), rows, :], sem.at[tile, f, c])
            for f in range(len(fields)) for c in range(STRIPS)]


def border_copies(north_rows, south_rows, strips, sem):
    copies = []
    for f in range(len(strips)):
        for c in range(STRIPS):
            lanes = pl.ds(LANES * c, LANES)
            copies.append(pltpu.make_async_copy(north_rows.at[f, :, :, lanes], strips[f].at[c, pl.ds(1, LEV), pl.ds(ROWS, 1), :], sem.at[0, f, c]))
            copies.append(pltpu.make_async_copy(south_rows.at[f, :, :, lanes], strips[f].at[c, pl.ds(0, LEV), pl.ds(PITCH - 1, 1), :], sem.at[1, f, c]))
    return copies


def level_rows(tile, c, k, offset=0):
    return pl.ds(SUB * tile + (c * (LEV + 1) * PITCH + PITCH * (k + 1) + offset), SUB)


def face_counts(counts_flat, side_cols, tile, at_first):
    rows = SUB * tile + SUB
    mid = [counts_flat[pl.ds(rows + c * 64, SUB), :] for c in range(STRIPS)]
    north = [counts_flat[pl.ds(rows + c * 64 + 1, SUB), :] for c in range(STRIPS)]
    edge = pltpu.roll(side_cols[0, pl.ds(rows, SUB), :], LANES - 1 - 2 * LEV, 1)
    east = east_of(mid, edge, at_first)
    return mid, [jnp.minimum(a, b) for a, b in zip(mid, east)], [jnp.minimum(a, b) for a, b in zip(mid, north)]


def unpack(packed, edges, rows):
    for k in range(LEV):
        for f, side in enumerate(packed):
            edges[f, k, rows, :] = pltpu.roll(side, LANES - 1 - 2 * k, 1)


def momentum_kernel(n_row, u, v, t, s, north_rows, south_rows, side_cols, counts,
                    wu_out, wv_out, force, level_mean,
                    u_s, v_s, t_s, s_s, p_s, b_s, edges, wu, wv, load_sem, border_sem, store_sem):
    row = lax.axis_index('row')
    fields, strips = (u, v, t, s), (u_s, v_s, t_s, s_s)
    borders = border_copies(north_rows, south_rows, strips, border_sem)
    for copy in strip_copies(TILES - 1, fields, strips, load_sem):
        copy.start()
    for copy in borders:
        copy.start()
    for tile in range(TILES - 2, -1, -1):
        for copy in strip_copies(tile, fields, strips, load_sem):
            copy.start()
    rows_total = (LEV + 1) * PITCH * STRIPS
    uf, vf, tf, sf, pf, bf = [ref.reshape(rows_total, LANES) for ref in (u_s, v_s, t_s, s_s, p_s, b_s)]
    counts_flat = counts.reshape(STRIPS * 64, LANES)
    half_scale = 0.5 * BC_GRAVITY / LEV
    pivot, _ = tables(VISC_R)
    four = range(STRIPS)

    def density(sal, tem):
        return (half_scale * CONTRACT_S) * sal - (half_scale * EXPAND_T) * tem

    def spread(tile, _):
        rows = pl.ds(pl.multiple_of(SUB * tile, SUB), SUB)
        mid_rows = pl.ds(SUB * tile + SUB, SUB)
        side_v = side_cols[1, mid_rows, :]
        packed = (side_cols[0, mid_rows, :], side_v, side_v + side_cols[1, pl.ds(SUB * tile + SUB - 1, SUB), :],
                  density(side_cols[3, mid_rows, :], side_cols[2, mid_rows, :]))
        unpack(packed, edges, rows)
        return 0

    lax.fori_loop(0, TILES + 1, spread, 0)
    lane = lane_index()
    at_first, at_last = lane == 0, lane == LANES - 1
    for copy in strip_copies(TILES - 1, fields, strips, load_sem):
        copy.wait()
    for copy in borders:
        copy.wait()
    acc = [jnp.zeros((SUB, LANES), F32)] * STRIPS
    for k in range(LEV):
        edge = edges[0, k, pl.ds(ROWS, SUB), :]
        uu = [uf[level_rows(TILES, c, k), :] for c in four]
        uw = west_of(uu, edge, at_last)
        for c in four:
            at = level_rows(TILES, c, k)
            bf[at, :] = uu[c] + uw[c]
            rho = density(sf[at, :], tf[at, :])
            pf[at, :] = acc[c] + rho
            acc[c] = (acc[c] + rho) + rho

    def tile_step(step, _):
        tile = TILES - 1 - step

        @pl.when(tile > 0)
        def _():
            for copy in strip_copies(tile - 1, fields, strips, load_sem):
                copy.wait()

        mid_count, nu, nv = face_counts(counts_flat, side_cols, tile, at_first)
        row_pos = (row * ROWS + SUB * tile + lax.broadcasted_iota(jnp.int32, (SUB, LANES), 0)).astype(F32)
        fu = 0.25 * (CORIO_F0 + CORIO_BETA * ((row_pos + 0.5) / (ROWS * n_row) - 0.5))
        fv = 0.25 * (CORIO_F0 + CORIO_BETA * ((row_pos + 1.0) / (ROWS * n_row) - 0.5))
        out_rows = pl.ds(pl.multiple_of(SUB * tile, SUB), SUB)
        zero = jnp.zeros((SUB, LANES), F32)
        acc = [zero] * STRIPS
        acc_e = zero
        xu, xv = [zero] * STRIPS, [zero] * STRIPS
        sum_du, sum_dv, sum_su, sum_sv = [zero] * STRIPS, [zero] * STRIPS, [zero] * STRIPS, [zero] * STRIPS
        for k in range(LEV):
            here = [level_rows(tile, c, k) for c in four]
            up = [level_rows(tile, c, k, 1) for c in four]
            below = [level_rows(tile, c, k, -1) for c in four]
            uu = [uf[here[c], :] for c in four]
            vv = [vf[here[c], :] for c in four]
            v_south = [vf[below[c], :] for c in four]
            edge_u = edges[0, k, out_rows, :]
            edge_v = edges[1, k, out_rows, :]
            u_west = west_of(uu, edge_u, at_last)
            u_east = east_of(uu, edge_u, at_first)
            v_west = west_of(vv, edge_v, at_last)
            v_east = east_of(vv, edge_v, at_first)
            pair_v = [vv[c] + v_south[c] for c in four]
            pair_ve = east_of(pair_v, edges[2, k, out_rows, :], at_first)
            rho_e = edges[3, k, out_rows, :]
            p_edge = acc_e + rho_e
            acc_e = p_edge + rho_e
            pp = []
            for c in four:
                rho = density(sf[here[c], :], tf[here[c], :])
                pp.append(acc[c] + rho)
                acc[c] = pp[c] + rho
                pf[here[c], :] = pp[c]
            p_east = east_of(pp, p_edge, at_first)
            for c in four:
                pair_u = uu[c] + u_west[c]
                bf[here[c], :] = pair_u
                v4 = pair_v[c] + pair_ve[c]
                u4 = pair_u + bf[up[c], :]
                du = v4 * (fu - 0.125 * (uf[up[c], :] - uf[below[c], :])) - 0.5 * uu[c] * (u_east[c] - u_west[c]) + (pp[c] - p_east[c])
                dv = (pp[c] - pf[up[c], :]) - u4 * (fv + 0.125 * (v_east[c] - v_west[c])) - 0.5 * vv[c] * (vf[up[c], :] - v_south[c])
                us, vs = uu[c] + du, vv[c] + dv
                on_u, on_v = nu[c] > k, nv[c] > k
                sum_du[c] += jnp.where(on_u, du, 0.0)
                sum_dv[c] += jnp.where(on_v, dv, 0.0)
                sum_su[c] += jnp.where(on_u, us, 0.0)
                sum_sv[c] += jnp.where(on_v, vs, 0.0)
                xu[c] = us * (1.0 / pivot[k]) + xu[c] * (VISC_R / pivot[k])
                xv[c] = vs * (1.0 / pivot[k]) + xv[c] * (VISC_R / pivot[k])
                wu[tile, k, c] = xu[c]
                wv[tile, k, c] = xv[c]
        for c in four:
            lanes = pl.ds(LANES * c, LANES)
            inv_u = 1.0 / jnp.maximum(nu[c], 1.0)
            inv_v = 1.0 / jnp.maximum(nv[c], 1.0)
            force[0, out_rows, lanes] = sum_du[c] * inv_u
            force[1, out_rows, lanes] = sum_dv[c] * inv_v
            level_mean[0, out_rows, lanes] = sum_su[c] * inv_u
            level_mean[1, out_rows, lanes] = sum_sv[c] * inv_v
        pltpu.make_async_copy(wu.at[tile], wu_out.at[tile], store_sem.at[0, tile]).start()
        pltpu.make_async_copy(wv.at[tile], wv_out.at[tile], store_sem.at[1, tile]).start()
        return 0

    lax.fori_loop(0, TILES, tile_step, 0)
    for tile in range(TILES):
        pltpu.make_async_copy(wu.at[tile], wu_out.at[tile], store_sem.at[0, tile]).wait()
        pltpu.make_async_copy(wv.at[tile], wv_out.at[tile], store_sem.at[1, tile]).wait()


def tracer_kernel(u, v, t, s, north_rows, south_rows, side_cols, counts,
                  t_out, s_out,
                  u_s, v_s, t_s, s_s, ft_s, fs_s, edges, wt, ws, t_new, s_new, load_sem, border_sem, store_sem):
    fields, strips = (u, v, t, s), (u_s, v_s, t_s, s_s)
    borders = border_copies(north_rows, south_rows, strips, border_sem)
    for copy in strip_copies(0, fields, strips, load_sem):
        copy.start()
    for copy in borders:
        copy.start()
    for tile in range(1, TILES):
        for copy in strip_copies(tile, fields, strips, load_sem):
            copy.start()
    lane = lane_index()
    at_first, at_last = lane == 0, lane == LANES - 1
    half = (lane >> 1).astype(F32)
    rows_total = (LEV + 1) * PITCH * STRIPS
    uf, vf, tf, sf, ftf, fsf = [ref.reshape(rows_total, LANES) for ref in (u_s, v_s, t_s, s_s, ft_s, fs_s)]
    counts_flat = counts.reshape(STRIPS * 64, LANES)
    pivot, final = tables(DIFF_R)
    four = range(STRIPS)
    scale = 0.5 * TIME_STEP

    def spread(tile, _):
        rows = pl.ds(pl.multiple_of(SUB * tile, SUB), SUB)
        mid_rows = pl.ds(SUB * tile + SUB, SUB)
        side_u = side_cols[0, mid_rows, :]
        west_count = jnp.minimum(side_u[:, 2 * LEV:2 * LEV + 1], counts[0, mid_rows, :][:, 0:1])
        west_half = jnp.where(half < west_count, scale * side_u, 0.0)
        packed = (side_cols[2, mid_rows, :], side_cols[3, mid_rows, :], west_half)
        unpack(packed, edges, rows)
        return 0

    lax.fori_loop(0, TILES, spread, 0)
    for copy in strip_copies(0, fields, strips, load_sem):
        copy.wait()
    for copy in borders:
        copy.wait()
    south_count = [jnp.minimum(counts_flat[pl.ds(c * 64, SUB), :], counts_flat[pl.ds(c * 64 + 1, SUB), :]) for c in four]
    for k in range(LEV):
        for c in four:
            here, up = level_rows(-1, c, k), level_rows(-1, c, k, 1)
            hv = jnp.where(south_count[c] > k, scale * vf[here, :], 0.0)
            ftf[here, :] = hv * (tf[here, :] + tf[up, :])
            fsf[here, :] = hv * (sf[here, :] + sf[up, :])

    def tile_step(tile, _):
        @pl.when(tile < TILES - 1)
        def _():
            for copy in strip_copies(tile + 1, fields, strips, load_sem):
                copy.wait()

        mid, nu, nv = face_counts(counts_flat, side_cols, tile, at_first)
        out_rows = pl.ds(pl.multiple_of(SUB * tile, SUB), SUB)
        zero = jnp.zeros((SUB, LANES), F32)
        xt, xs = [zero] * STRIPS, [zero] * STRIPS
        for k in range(LEV):
            here = [level_rows(tile, c, k) for c in four]
            up = [level_rows(tile, c, k, 1) for c in four]
            below = [level_rows(tile, c, k, -1) for c in four]
            hu = [jnp.where(nu[c] > k, scale * uf[here[c], :], 0.0) for c in four]
            hv = [jnp.where(nv[c] > k, scale * vf[here[c], :], 0.0) for c in four]
            hw = west_of(hu, edges[2, k, out_rows, :], at_last)
            if k < LEV - 1:
                inverse = [jnp.where(mid[c] > k + 1, 1.0 / pivot[k], 1.0 / final[k]) for c in four]
            else:
                inverse = [1.0 / final[k]] * STRIPS

            def advance(flat, flux, which, x, w):
                q = [flat[here[c], :] for c in four]
                edge = edges[which, k, out_rows, :]
                q_east = east_of(q, edge, at_first)
                q_west = west_of(q, edge, at_last)
                flux_e = [hu[c] * (q[c] + q_east[c]) for c in four]
                flux_w = [hw[c] * (q[c] + q_west[c]) for c in four]
                for c in four:
                    flux_n = hv[c] * (q[c] + flat[up[c], :])
                    flux[here[c], :] = flux_n
                    new = q[c] - ((flux_e[c] - flux_w[c]) + (flux_n - flux[below[c], :]))
                    x[c] = (new + DIFF_R * x[c]) * inverse[c]
                    w[k, c] = x[c]

            advance(tf, ftf, 0, xt, wt)
            advance(sf, fsf, 1, xs, ws)
        bt, bs = [zero] * STRIPS, [zero] * STRIPS
        for k in range(LEV - 1, -1, -1):
            for c in four:
                here = level_rows(tile, c, k)
                lanes = pl.ds(LANES * c, LANES)
                on = mid[c] > k
                yt = wt[k, c] + (DIFF_R / pivot[k]) * bt[c]
                ys = ws[k, c] + (DIFF_R / pivot[k]) * bs[c]
                t_new[k, out_rows, lanes] = jnp.where(on, yt, tf[here, :])
                s_new[k, out_rows, lanes] = jnp.where(on, ys, sf[here, :])
                bt[c] = jnp.where(on, yt, 0.0)
                bs[c] = jnp.where(on, ys, 0.0)
        pltpu.make_async_copy(t_new.at[:, out_rows, :], t_out.at[:, out_rows, :], store_sem.at[0, tile]).start()
        pltpu.make_async_copy(s_new.at[:, out_rows, :], s_out.at[:, out_rows, :], store_sem.at[1, tile]).start()
        return 0

    lax.fori_loop(0, TILES, tile_step, 0)
    for tile in range(TILES):
        rows = pl.ds(SUB * tile, SUB)
        pltpu.make_async_copy(t_new.at[:, rows, :], t_out.at[:, rows, :], store_sem.at[0, tile]).wait()
        pltpu.make_async_copy(s_new.at[:, rows, :], s_out.at[:, rows, :], store_sem.at[1, tile]).wait()


def fast_kernel(n_row, n_sub, weights, wu_in, wv_in, eta, tu, tv, depth, wide_north, wide_south, wide_side,
                force, force_north, force_south, force_side, level_mean, counts, side_cols,
                eta_out, tu_out, tv_out, u_out, v_out,
                e_s, u_s, v_s, b_s, d_s, cu_s, cv_s, bu_s, bv_s, fu_s, fv_s, bar_u, bar_v, wu, wv, u_new, v_new, load_sem, store_sem):
    row = lax.axis_index('row')
    for tile in range(TILES):
        pltpu.make_async_copy(wu_in.at[tile], wu.at[tile], load_sem.at[0, tile]).start()
        pltpu.make_async_copy(wv_in.at[tile], wv.at[tile], load_sem.at[1, tile]).start()
    lane = lane_index()
    at_first, at_last = lane == 0, lane == LANES - 1
    five = range(STRIPS + 1)
    dt_fast = TIME_STEP / n_sub
    total = ROWS * n_row
    zero = jnp.zeros((SUB, LANES), F32)

    def page(tile, c, offset=0):
        return pl.ds(c * PAGE + SUB + SUB * tile + offset, SUB)

    def gather(f, own, north, south, side, tile, c):
        if c == STRIPS:
            return side[f, SUB * tile:SUB * tile + SUB, :]
        lanes = slice(c * LANES, (c + 1) * LANES)
        if tile < REACH // SUB:
            return south[f, SUB * tile:SUB * tile + SUB, lanes]
        if tile < (REACH + ROWS) // SUB:
            return own[SUB * tile - REACH:SUB * tile - REACH + SUB, lanes]
        start = SUB * tile - REACH - ROWS
        return north[f, start:start + SUB, lanes]

    for ref in (e_s, u_s, v_s, b_s, d_s):
        for c in five:
            ref[page(-1, c), :] = zero
            ref[page(EXT_TILES, c), :] = zero
    for tile in range(EXT_TILES):
        for c in five:
            at = page(tile, c)
            e_s[at, :] = gather(0, eta, wide_north, wide_south, wide_side, tile, c)
            u_s[at, :] = gather(1, tu, wide_north, wide_south, wide_side, tile, c)
            v_s[at, :] = gather(2, tv, wide_north, wide_south, wide_side, tile, c)
            d_s[at, :] = gather(3, depth, wide_north, wide_south, wide_side, tile, c)
            bu_s[at, :] = gather(0, force.at[0], force_north, force_south, force_side, tile, c)
            bv_s[at, :] = gather(1, force.at[1], force_north, force_south, force_side, tile, c)
    for tile in range(EXT_TILES):
        place = row * ROWS + (SUB * tile - REACH) + lax.broadcasted_iota(jnp.int32, (SUB, LANES), 0)
        inside = jnp.logical_and(place >= 0, place < total)
        inside_v = jnp.logical_and(place >= 0, place < total - 1)
        row_pos = place.astype(F32)
        fu = (0.25 * dt_fast) * (CORIO_F0 + CORIO_BETA * ((row_pos + 0.5) / total - 0.5))
        fv = (0.25 * dt_fast) * (CORIO_F0 + CORIO_BETA * ((row_pos + 1.0) / total - 0.5))
        fu_s[SUB * tile:SUB * tile + SUB, :] = jnp.where(inside, fu, 0.0)
        fv_s[SUB * tile:SUB * tile + SUB, :] = jnp.where(inside_v, fv, 0.0)
        deep = [d_s[page(tile, c), :] for c in five]
        deep_e = east_of(deep, deep[0], at_first)
        for c in five:
            at = page(tile, c)
            hu = jnp.where(inside, 0.5 * (deep[c] + deep_e[c]), 0.0)
            hv = jnp.where(inside_v, 0.5 * (deep[c] + d_s[page(tile, c, 1), :]), 0.0)
            cu_s[at, :] = (dt_fast * GRAVITY) * hu
            cv_s[at, :] = (dt_fast * GRAVITY) * hv
            bu_s[at, :] = (dt_fast / TIME_STEP) * hu * bu_s[at, :]
            bv_s[at, :] = (dt_fast / TIME_STEP) * hv * bv_s[at, :]
    bar_u[...] = jnp.zeros_like(bar_u)
    bar_v[...] = jnp.zeros_like(bar_v)

    def subcycle(n, low, high):
        weight = weights[n]
        for tile in range(high - 1, low - 1, -1):
            uu = [u_s[page(tile, c), :] for c in five]
            vv = [v_s[page(tile, c), :] for c in five]
            v_south = [v_s[page(tile, c, -1), :] for c in five]
            u_west = west_of(uu, uu[-1], at_last)
            ee = []
            for c in five:
                at = page(tile, c)
                new = e_s[at, :] - dt_fast * ((uu[c] - u_west[c]) + (vv[c] - v_south[c]))
                e_s[at, :] = new
                ee.append(new)
                b_s[at, :] = uu[c] + u_west[c]
            pair_v = [vv[c] + v_south[c] for c in five]
            pair_ve = east_of(pair_v, pair_v[0], at_first)
            e_east = east_of(ee, ee[0], at_first)
            fu = fu_s[SUB * tile:SUB * tile + SUB, :]
            fv = fv_s[SUB * tile:SUB * tile + SUB, :]
            for c in five:
                at, up = page(tile, c), page(tile, c, 1)
                u_next = uu[c] + ((fu * (pair_v[c] + pair_ve[c]) + bu_s[at, :]) - cu_s[at, :] * (e_east[c] - ee[c]))
                v_next = vv[c] + ((bv_s[at, :] - fv * ((uu[c] + u_west[c]) + b_s[up, :])) - cv_s[at, :] * (e_s[up, :] - ee[c]))
                u_s[at, :] = u_next
                v_s[at, :] = v_next
                if c < STRIPS and REACH // SUB <= tile < (REACH + ROWS) // SUB:
                    own = tile - REACH // SUB
                    bar_u[own, c] += weight * u_next
                    bar_v[own, c] += weight * v_next

    def wall_row():
        for tile in range(EXT_TILES):
            place = row * ROWS + (SUB * tile - REACH) + lax.broadcasted_iota(jnp.int32, (SUB, LANES), 0)
            wet = jnp.logical_and(place >= 0, place < total - 1)
            for c in five:
                at = page(tile, c)
                v_s[at, :] = jnp.where(wet, v_s[at, :], 0.0)
                if c < STRIPS and REACH // SUB <= tile < (REACH + ROWS) // SUB:
                    own = tile - REACH // SUB
                    bar_v[own, c] = jnp.where(wet, bar_v[own, c], 0.0)

    n = 0
    while n < n_sub:
        spread = -(-(n_sub - n) // SUB)
        stop = n_sub - SUB * (spread - 1)
        low, high = REACH // SUB - spread, (REACH + ROWS) // SUB + spread

        def some(i, _, low=low, high=high, first=(n == 0)):
            subcycle(i, low, high)
            if first:
                pl.when(i == 0)(wall_row)
            return 0

        lax.fori_loop(n, stop, some, 0)
        n = stop

    counts_flat = counts.reshape(STRIPS * 64, LANES)
    pivot, final = tables(VISC_R)
    four = range(STRIPS)
    for tile in range(TILES):
        for c in four:
            at = page(tile + REACH // SUB, c)
            rows, lanes = pl.ds(SUB * tile, SUB), pl.ds(LANES * c, LANES)
            eta_out[rows, lanes] = e_s[at, :]
            tu_out[rows, lanes] = u_s[at, :]
            tv_out[rows, lanes] = v_s[at, :]

    def tile_step(tile, _):
        pltpu.make_async_copy(wu_in.at[tile], wu.at[tile], load_sem.at[0, tile]).wait()
        pltpu.make_async_copy(wv_in.at[tile], wv.at[tile], load_sem.at[1, tile]).wait()
        mid, nu, nv = face_counts(counts_flat, side_cols, tile, at_first)
        out_rows = pl.ds(pl.multiple_of(SUB * tile, SUB), SUB)
        add_u, add_v = [], []
        for c in four:
            at = pl.ds(c * PAGE + SUB + REACH + SUB * tile, SUB)
            lanes = pl.ds(LANES * c, LANES)
            deep_u = cu_s[at, :] * (1.0 / (dt_fast * GRAVITY))
            deep_v = cv_s[at, :] * (1.0 / (dt_fast * GRAVITY))
            deep_v = jnp.where(nv[c] > 0, deep_v, 1.0)
            add_u.append(bar_u[tile, c] / deep_u - level_mean[0, out_rows, lanes])
            add_v.append(bar_v[tile, c] / deep_v - level_mean[1, out_rows, lanes])
        xu, xv = [zero] * STRIPS, [zero] * STRIPS
        for k in range(LEV - 1, -1, -1):
            ratio, bottom = VISC_R / pivot[k], pivot[k] / final[k]
            for c in four:
                lanes = pl.ds(LANES * c, LANES)

                def solve(w, x, n, add, out):
                    value = w[tile, k, c]
                    last = value * bottom
                    if k < LEV - 1:
                        x[c] = jnp.where(n[c] > k + 1, value + ratio * x[c], last)
                    else:
                        x[c] = last
                    out[k, out_rows, lanes] = jnp.where(n[c] > k, x[c] + add[c], 0.0)

                solve(wu, xu, nu, add_u, u_new)
                solve(wv, xv, nv, add_v, v_new)
        pltpu.make_async_copy(u_new.at[:, out_rows, :], u_out.at[:, out_rows, :], store_sem.at[0, tile]).start()
        pltpu.make_async_copy(v_new.at[:, out_rows, :], v_out.at[:, out_rows, :], store_sem.at[1, tile]).start()
        return 0

    lax.fori_loop(0, TILES, tile_step, 0)
    for tile in range(TILES):
        rows = pl.ds(SUB * tile, SUB)
        pltpu.make_async_copy(u_new.at[:, rows, :], u_out.at[:, rows, :], store_sem.at[0, tile]).wait()
        pltpu.make_async_copy(v_new.at[:, rows, :], v_out.at[:, rows, :], store_sem.at[1, tile]).wait()


def solution(mesh):
    n_row = mesh.shape['row']
    hbm = pl.BlockSpec(memory_space=pltpu.HBM)
    vmem = pl.BlockSpec(memory_space=pltpu.VMEM)
    smem = pl.BlockSpec(memory_space=pltpu.SMEM)
    dma = pltpu.SemaphoreType.DMA
    strip = pltpu.VMEM((STRIPS, LEV + 1, PITCH, LANES), F32)
    whole = pltpu.VMEM((LEV, ROWS, COLS), F32)
    column = pltpu.VMEM((TILES, LEV, STRIPS, SUB, LANES), F32)
    one = pltpu.VMEM((LEV, STRIPS, SUB, LANES), F32)
    extended = pltpu.VMEM(((STRIPS + 1) * PAGE, LANES), F32)

    def shape(*dims):
        return jax.ShapeDtypeStruct(dims, F32)

    def call(body, ins, outs, shapes, scratch, **params):
        return pl.pallas_call(body, out_shape=shapes, in_specs=ins, out_specs=outs, scratch_shapes=scratch,
                              compiler_params=pltpu.CompilerParams(vmem_limit_bytes=VMEM_LIMIT, **params))

    def step(vel_u, vel_v, temp, salt, eta, tu, tv, depth, count, weights):
        n_sub = weights.shape[0]
        north_rows, south_rows, side_cols, own_cols, counts, wide_north, wide_south, wide_side = call(
            functools.partial(halo_kernel, n_row), [hbm] * 4 + [vmem] * 5, [hbm] * 2 + [vmem] * 6,
            [shape(4, LEV, 1, COLS)] * 2 + [shape(4, ROWS + 16, LANES), shape(4, ROWS, LANES), shape(STRIPS, ROWS + 16, LANES),
                                            shape(4, REACH, COLS), shape(4, REACH, COLS), shape(4, EXT, LANES)],
            [pltpu.VMEM((4, 2, LEV, ROWS, LANES), F32), pltpu.VMEM((4, ROWS, LANES), F32), pltpu.VMEM((LEV, 1, COLS), F32),
             dma((4, 2)), dma((4,)), dma((32,)), dma((32,))],
            collective_id=0, has_side_effects=True)(vel_u, vel_v, temp, salt, eta, tu, tv, depth, count)
        wu, wv, force, level_mean = call(
            functools.partial(momentum_kernel, n_row), [hbm] * 6 + [vmem] * 2, [hbm] * 2 + [vmem] * 2,
            [shape(TILES, LEV, STRIPS, SUB, LANES)] * 2 + [shape(2, ROWS, COLS)] * 2,
            [strip] * 6 + [pltpu.VMEM((4, LEV, ROWS + SUB, LANES), F32)] + [column] * 2 + [dma((TILES, 4, STRIPS)), dma((2, 4, STRIPS)), dma((2, TILES))],
        )(vel_u, vel_v, temp, salt, north_rows, south_rows, side_cols, counts)
        force_north, force_south, force_side = call(
            functools.partial(force_kernel, n_row), [vmem], [vmem] * 3,
            [shape(2, REACH, COLS), shape(2, REACH, COLS), shape(2, EXT, LANES)],
            [pltpu.VMEM((2, ROWS, LANES), F32), dma((5,)), dma((5,))],
            collective_id=1, has_side_effects=True)(force)
        temp_new, salt_new = call(
            tracer_kernel, [hbm] * 6 + [vmem] * 2, [hbm] * 2,
            [shape(LEV, ROWS, COLS)] * 2,
            [strip] * 6 + [pltpu.VMEM((3, LEV, ROWS, LANES), F32)] + [one] * 2 + [whole] * 2 + [dma((TILES, 4, STRIPS)), dma((2, 4, STRIPS)), dma((2, TILES))],
        )(vel_u, vel_v, temp, salt, north_rows, south_rows, side_cols, counts)
        eta_new, tu_new, tv_new, u_new, v_new = call(
            functools.partial(fast_kernel, n_row, n_sub), [smem] + [hbm] * 2 + [vmem] * 14, [vmem] * 3 + [hbm] * 2,
            [shape(ROWS, COLS)] * 3 + [shape(LEV, ROWS, COLS)] * 2,
            [extended] * 9 + [pltpu.VMEM((EXT, LANES), F32)] * 2 + [pltpu.VMEM((TILES, STRIPS, SUB, LANES), F32)] * 2
            + [column] * 2 + [whole] * 2 + [dma((2, TILES)), dma((2, TILES))],
        )(weights, wu, wv, eta, tu, tv, depth, wide_north, wide_south, wide_side,
          force, force_north, force_south, force_side, level_mean, counts, side_cols)
        return eta_new, tu_new, tv_new, u_new, v_new, temp_new, salt_new

    cube = P(None, 'row', 'col')
    flat = P('row', 'col')
    return jax.shard_map(step, mesh=mesh, in_specs=(cube, cube, cube, cube, flat, flat, flat, flat, flat, P()),
                         out_specs=(flat, flat, flat, cube, cube, cube, cube), check_vma=False)
```

```python
import functools

import jax
import jax.numpy as jnp
from jax import lax
from jax.experimental import pallas as pl
from jax.experimental.pallas import tpu as pltpu
from jax.sharding import PartitionSpec as P

TIME_STEP = 1.0
GRAVITY = 16.0
BC_GRAVITY = 4.0
EXPAND_T = 0.2
CONTRACT_S = 0.6
CORIO_F0 = 0.4
CORIO_BETA = 0.4
VISC_R = 2.0
DIFF_R = 0.5

LEV = 41
ROWS = 48
SUB = 8
COLS = 512
LANES = 128
STRIPS = COLS // LANES
TILES = ROWS // SUB
PITCH = 56
REACH = 32
EXT = ROWS + 2 * REACH
EXT_TILES = EXT // SUB
PAGE = EXT + 16
MESH = pl.DeviceIdType.MESH
F32 = jnp.float32
VMEM_LIMIT = 62 * 1024 * 1024


def tables(strength):
    inner, last, ratio = [], [], 0.0
    for level in range(LEV):
        low = strength if level else 0.0
        pivot = 1.0 + low + strength - low * ratio
        inner.append(pivot)
        last.append(1.0 + low - low * ratio)
        ratio = strength / pivot
    return inner, last


def lane_index():
    return lax.broadcasted_iota(jnp.int32, (SUB, LANES), 1)


def west_of(strips, edge, at_last):
    mixed = [jnp.where(at_last, edge if c == 0 else strips[c - 1], strips[c]) for c in range(len(strips))]
    return [pltpu.roll(x, 1, 1) for x in mixed]


def east_of(strips, edge, at_first):
    n = len(strips)
    mixed = [jnp.where(at_first, edge if c == n - 1 else strips[c + 1], strips[c]) for c in range(n)]
    return [pltpu.roll(x, LANES - 1, 1) for x in mixed]


def places(n_row):
    row = lax.axis_index('row')
    col = lax.axis_index('col')
    other = 1 - col
    has_north = row < n_row - 1
    has_south = row > 0
    return dict(
        row=row, has_north=has_north, has_south=has_south,
        side={'col': other, 'row': row},
        north={'col': col, 'row': row + 1}, south={'col': col, 'row': row - 1},
        north_side={'col': other, 'row': row + 1}, south_side={'col': other, 'row': row - 1})


def meet(at):
    barrier = pltpu.get_barrier_semaphore()
    pl.semaphore_signal(barrier, inc=1, device_id=at['side'], device_id_type=MESH)

    @pl.when(at['has_north'])
    def _():
        pl.semaphore_signal(barrier, inc=1, device_id=at['north'], device_id_type=MESH)
        pl.semaphore_signal(barrier, inc=1, device_id=at['north_side'], device_id_type=MESH)

    @pl.when(at['has_south'])
    def _():
        pl.semaphore_signal(barrier, inc=1, device_id=at['south'], device_id_type=MESH)
        pl.semaphore_signal(barrier, inc=1, device_id=at['south_side'], device_id_type=MESH)

    return barrier


def await_meet(barrier, at):
    pl.semaphore_wait(barrier, 1 + 2 * at['has_north'].astype(jnp.int32) + 2 * at['has_south'].astype(jnp.int32))


def remote(src, dst, send, recv, where):
    return pltpu.make_async_remote_copy(src_ref=src, dst_ref=dst, send_sem=send, recv_sem=recv, device_id=where, device_id_type=MESH)


def level_rows(tile, k, offset=0):
    return pl.ds(SUB * tile + (PITCH * (k + 1) + offset), SUB)


def west_stack(strips, edge, at_last):
    return pltpu.roll(jnp.where(at_last, jnp.concatenate([edge[None], strips[:-1]], axis=0), strips), 1, 2)


def east_stack(strips, edge, at_first):
    return pltpu.roll(jnp.where(at_first, jnp.concatenate([strips[1:], edge[None]], axis=0), strips), LANES - 1, 2)


def face_counts(counts, side_cols, tile):
    rows = SUB * tile + SUB
    mid = counts[:, pl.ds(rows, SUB), :]
    north = counts[:, pl.ds(rows + 1, SUB), :]
    edge = pltpu.roll(side_cols[0, pl.ds(rows, SUB), :], LANES - 1 - 2 * LEV, 1)
    at_first = lax.broadcasted_iota(jnp.int32, mid.shape, 2) == 0
    return mid, jnp.minimum(mid, east_stack(mid, edge, at_first)), jnp.minimum(mid, north)


def unpack(packed, edges, rows):
    for k in range(LEV):
        for f, side in enumerate(packed):
            edges[f, k, rows, :] = pltpu.roll(side, LANES - 1 - 2 * k, 1)


def step_kernel(n_row, u, v, t, s, eta, tu, tv, depth, count,
                wu_out, wv_out, wt_out, ws_out, force, level_mean, side_cols, counts,
                wide_north, wide_south, wide_side, force_north, force_south, force_side,
                u_s, v_s, t_s, s_s, one_s, two_s, edges, wu, wv, wt, ws, own_cols, fold, force_fold,
                load_sem, send_sem, recv_sem, store_sem):
    at = places(n_row)
    fields, strips = (u, v, t, s), (u_s, v_s, t_s, s_s)
    four = range(STRIPS)
    loads = [[pltpu.make_async_copy(fields[f].at[:, :, pl.ds(LANES * c, LANES)], strips[f].at[c, pl.ds(1, LEV), pl.ds(0, ROWS), :], load_sem.at[f, c])
              for c in four] for f in four]
    for c in (0, STRIPS - 1):
        for f in four:
            loads[f][c].start()
    for c in range(1, STRIPS - 1):
        for f in four:
            loads[f][c].start()
    lane = lane_index()
    at_first, at_last = lane == 0, lane == LANES - 1
    zero = jnp.zeros((SUB, LANES), F32)

    def clear_rows():
        def body(k, _):
            for strip in strips:
                for c in four:
                    strip[c, k, pl.ds(ROWS, SUB), :] = zero
            return 0

        lax.fori_loop(0, LEV + 1, body, 0)

    @pl.when(jnp.logical_not(at['has_north']))
    def _():
        clear_rows()
        counts[:, SUB + ROWS:, :] = jnp.zeros((STRIPS, SUB, LANES), F32)
        side_cols[:, SUB + ROWS:, :] = jnp.zeros((STRIPS, SUB, LANES), F32)
        wide_north[...] = jnp.zeros_like(wide_north)
        force_north[...] = jnp.zeros_like(force_north)
        wide_side[:, REACH + ROWS:, :] = jnp.zeros((STRIPS, REACH, LANES), F32)
        force_side[:, REACH + ROWS:, :] = jnp.zeros((2, REACH, LANES), F32)

    @pl.when(jnp.logical_not(at['has_south']))
    def _():
        clear_rows()
        counts[:, :SUB, :] = jnp.zeros((STRIPS, SUB, LANES), F32)
        side_cols[:, :SUB, :] = jnp.zeros((STRIPS, SUB, LANES), F32)
        wide_south[...] = jnp.zeros_like(wide_south)
        force_south[...] = jnp.zeros_like(force_south)
        wide_side[:, :REACH, :] = jnp.zeros((STRIPS, REACH, LANES), F32)
        force_side[:, :REACH, :] = jnp.zeros((2, REACH, LANES), F32)

    for c in four:
        counts[c, SUB:SUB + ROWS, :] = count[:, c * LANES:(c + 1) * LANES].astype(F32)
    barrier = meet(at)
    await_meet(barrier, at)
    slot = iter(range(LANES))

    def plan(bucket, src, dst, where):
        i = next(slot)
        bucket.append(remote(src, dst, send_sem.at[i], recv_sem.at[i], at[where]))

    def start(north, south, side=()):
        @pl.when(at['has_north'])
        def _():
            for copy in north:
                copy.start()

        @pl.when(at['has_south'])
        def _():
            for copy in south:
                copy.start()

        for copy in side:
            copy.start()

    def arrive(north, south, side=()):
        for copy in side:
            copy.wait_recv()

        @pl.when(at['has_north'])
        def _():
            for copy in south:
                copy.wait_recv()

        @pl.when(at['has_south'])
        def _():
            for copy in north:
                copy.wait_recv()

    def leave(north, south, side=()):
        for copy in side:
            copy.wait_send()

        @pl.when(at['has_north'])
        def _():
            for copy in north:
                copy.wait_send()

        @pl.when(at['has_south'])
        def _():
            for copy in south:
                copy.wait_send()

    rows_north, rows_south = [], []
    for f in four:
        for c in four:
            lanes = pl.ds(LANES * c, LANES)
            plan(rows_north, fields[f].at[:, pl.ds(ROWS - 1, 1), lanes], strips[f].at[c, pl.ds(0, LEV), pl.ds(PITCH - 1, 1), :], 'north')
            plan(rows_south, fields[f].at[:, pl.ds(0, 1), lanes], strips[f].at[c, pl.ds(1, LEV), pl.ds(ROWS, 1), :], 'south')
    count_north, count_south = [], []
    plan(count_north, counts.at[:, pl.ds(ROWS, SUB), :], counts.at[:, pl.ds(0, SUB), :], 'north')
    plan(count_south, counts.at[:, pl.ds(SUB, SUB), :], counts.at[:, pl.ds(SUB + ROWS, SUB), :], 'south')
    start(count_north + rows_north, count_south + rows_south)

    half_lane = lane >> 1
    sides, corner_north, corner_south = [], [], []
    for f in four:
        loads[f][0].wait()
        loads[f][STRIPS - 1].wait()

        def pack(tile, _):
            rows = pl.ds(pl.multiple_of(SUB * tile, SUB), SUB)
            packed = zero
            for k in range(LEV + 1 if f == 0 else LEV):
                if k < LEV:
                    first, last = strips[f][0, k + 1, rows, :], strips[f][STRIPS - 1, k + 1, rows, :]
                else:
                    lower = pl.ds(pl.multiple_of(SUB * tile + SUB, SUB), SUB)
                    first, last = counts[0, lower, :], counts[STRIPS - 1, lower, :]
                both = pltpu.roll(jnp.where(at_first, first, last), 2 * k + 1, 1)
                packed = jnp.where(half_lane == k, both, packed)
            own_cols[f, rows, :] = packed
            return 0

        lax.fori_loop(0, TILES, pack, 0)
        plan(sides, own_cols.at[f], side_cols.at[f, pl.ds(SUB, ROWS), :], 'side')
        sides[-1].start()
        if f == 0:
            plan(corner_south, own_cols.at[f, pl.ds(0, SUB), :], side_cols.at[f, pl.ds(SUB + ROWS, SUB), :], 'south_side')
        if f == 1:
            plan(corner_north, own_cols.at[f, pl.ds(ROWS - SUB, SUB), :], side_cols.at[f, pl.ds(0, SUB), :], 'north_side')
    start(corner_north, corner_south)

    fast = (eta, tu, tv, depth)
    low_half = lax.broadcasted_iota(jnp.int32, (ROWS, LANES), 1) < LANES // 2
    for f in four:
        fold[f] = jnp.where(low_half, fast[f][:, :LANES], fast[f][:, COLS - LANES:])
    wide_up, wide_down, wide_across = [], [], []
    for f in four:
        plan(wide_up, fast[f].at[pl.ds(ROWS - REACH, REACH), :], wide_south.at[f], 'north')
        plan(wide_down, fast[f].at[pl.ds(0, REACH), :], wide_north.at[f], 'south')
    plan(wide_up, fold.at[:, pl.ds(ROWS - REACH, REACH), :], wide_side.at[:, pl.ds(0, REACH), :], 'north_side')
    plan(wide_down, fold.at[:, pl.ds(0, REACH), :], wide_side.at[:, pl.ds(REACH + ROWS, REACH), :], 'south_side')
    plan(wide_across, fold, wide_side.at[:, pl.ds(REACH, ROWS), :], 'side')

    half_scale = 0.5 * BC_GRAVITY / LEV
    scale = 0.5 * TIME_STEP
    half = half_lane.astype(F32)

    def density(sal, tem):
        return (half_scale * CONTRACT_S) * sal - (half_scale * EXPAND_T) * tem

    arrive(count_north + corner_north, count_south + corner_south, sides)

    def spread(tile, _):
        rows = pl.ds(pl.multiple_of(SUB * tile, SUB), SUB)
        mid_rows = pl.ds(SUB * tile + SUB, SUB)
        side = [side_cols[f, mid_rows, :] for f in four]
        west_count = jnp.minimum(side[0][:, 2 * LEV:2 * LEV + 1], counts[0, mid_rows, :][:, 0:1])
        unpack((side[0], side[1], side[1] + side_cols[1, pl.ds(SUB * tile + SUB - 1, SUB), :], density(side[3], side[2]),
                side[2], side[3], jnp.where(half < west_count, scale * side[0], 0.0)), edges, rows)
        return 0

    lax.fori_loop(0, TILES + 1, spread, 0)
    for c in range(1, STRIPS - 1):
        for f in four:
            loads[f][c].wait()
    arrive(rows_north, rows_south)
    leave(rows_north, rows_south)
    start(wide_up, wide_down, wide_across)
    flats = [ref.reshape(STRIPS, (LEV + 1) * PITCH, LANES) for ref in (u_s, v_s, t_s, s_s, one_s, two_s)]
    uf, vf, tf, sf, pf, bf = flats
    stack = lax.broadcasted_iota(jnp.int32, (STRIPS, SUB, LANES), 2)
    first_lanes, last_lanes = stack == 0, stack == LANES - 1
    none = jnp.zeros((STRIPS, SUB, LANES), F32)
    pivot, _ = tables(VISC_R)
    acc = none
    for k in range(LEV):
        spot = level_rows(TILES, k)
        uu = uf[:, spot, :]
        bf[:, spot, :] = uu + west_stack(uu, edges[0, k, pl.ds(ROWS, SUB), :], last_lanes)
        rho = density(sf[:, spot, :], tf[:, spot, :])
        pf[:, spot, :] = acc + rho
        acc = (acc + rho) + rho

    def momentum(step, _):
        tile = TILES - 1 - step
        _, nu, nv = face_counts(counts, side_cols, tile)
        row_pos = (at['row'] * ROWS + SUB * tile + lax.broadcasted_iota(jnp.int32, (STRIPS, SUB, LANES), 1)).astype(F32)
        fu = 0.25 * (CORIO_F0 + CORIO_BETA * ((row_pos + 0.5) / (ROWS * n_row) - 0.5))
        fv = 0.25 * (CORIO_F0 + CORIO_BETA * ((row_pos + 1.0) / (ROWS * n_row) - 0.5))
        out_rows = pl.ds(pl.multiple_of(SUB * tile, SUB), SUB)
        acc, acc_e = none, zero
        xu, xv, sum_du, sum_dv, sum_su, sum_sv = (none,) * 6
        for k in range(LEV):
            here, up, below = [level_rows(tile, k, step) for step in (0, 1, -1)]
            uu, vv = uf[:, here, :], vf[:, here, :]
            v_south = vf[:, below, :]
            edge_u, edge_v = edges[0, k, out_rows, :], edges[1, k, out_rows, :]
            u_west = west_stack(uu, edge_u, last_lanes)
            u_east = east_stack(uu, edge_u, first_lanes)
            v_west = west_stack(vv, edge_v, last_lanes)
            v_east = east_stack(vv, edge_v, first_lanes)
            pair_v = vv + v_south
            pair_ve = east_stack(pair_v, edges[2, k, out_rows, :], first_lanes)
            rho_e = edges[3, k, out_rows, :]
            p_edge = acc_e + rho_e
            acc_e = p_edge + rho_e
            rho = density(sf[:, here, :], tf[:, here, :])
            pp = acc + rho
            acc = pp + rho
            pf[:, here, :] = pp
            p_east = east_stack(pp, p_edge, first_lanes)
            pair_u = uu + u_west
            bf[:, here, :] = pair_u
            v4 = pair_v + pair_ve
            u4 = pair_u + bf[:, up, :]
            du = v4 * (fu - 0.125 * (uf[:, up, :] - uf[:, below, :])) - 0.5 * uu * (u_east - u_west) + (pp - p_east)
            dv = (pp - pf[:, up, :]) - u4 * (fv + 0.125 * (v_east - v_west)) - 0.5 * vv * (vf[:, up, :] - v_south)
            us, vs = uu + du, vv + dv
            on_u, on_v = nu > k, nv > k
            sum_du += jnp.where(on_u, du, 0.0)
            sum_dv += jnp.where(on_v, dv, 0.0)
            sum_su += jnp.where(on_u, us, 0.0)
            sum_sv += jnp.where(on_v, vs, 0.0)
            xu = us * (1.0 / pivot[k]) + xu * (VISC_R / pivot[k])
            xv = vs * (1.0 / pivot[k]) + xv * (VISC_R / pivot[k])
            wu[tile, k] = xu
            wv[tile, k] = xv
        inv_u = 1.0 / jnp.maximum(nu, 1.0)
        inv_v = 1.0 / jnp.maximum(nv, 1.0)
        for c in four:
            lanes = pl.ds(LANES * c, LANES)
            force[0, out_rows, lanes] = (sum_du * inv_u)[c]
            force[1, out_rows, lanes] = (sum_dv * inv_v)[c]
            level_mean[0, out_rows, lanes] = (sum_su * inv_u)[c]
            level_mean[1, out_rows, lanes] = (sum_sv * inv_v)[c]
        pltpu.make_async_copy(wu.at[tile], wu_out.at[tile], store_sem.at[0, tile]).start()
        pltpu.make_async_copy(wv.at[tile], wv_out.at[tile], store_sem.at[1, tile]).start()
        return 0

    lax.fori_loop(0, TILES, momentum, 0)

    low_half = lax.broadcasted_iota(jnp.int32, (ROWS, LANES), 1) < LANES // 2
    for f in range(2):
        force_fold[f] = jnp.where(low_half, force[f, :, :LANES], force[f, :, COLS - LANES:])
    force_up, force_down, force_across = [], [], []
    plan(force_up, force.at[:, pl.ds(ROWS - REACH, REACH), :], force_south, 'north')
    plan(force_up, force_fold.at[:, pl.ds(ROWS - REACH, REACH), :], force_side.at[:, pl.ds(0, REACH), :], 'north_side')
    plan(force_down, force.at[:, pl.ds(0, REACH), :], force_north, 'south')
    plan(force_down, force_fold.at[:, pl.ds(0, REACH), :], force_side.at[:, pl.ds(REACH + ROWS, REACH), :], 'south_side')
    plan(force_across, force_fold, force_side.at[:, pl.ds(REACH, ROWS), :], 'side')
    start(force_up, force_down, force_across)

    ftf, fsf = pf, bf
    pivot, final = tables(DIFF_R)

    south_count = jnp.minimum(counts[:, pl.ds(0, SUB), :], counts[:, pl.ds(1, SUB), :])
    for k in range(LEV):
        here, up = level_rows(-1, k), level_rows(-1, k, 1)
        hv = jnp.where(south_count > k, scale * vf[:, here, :], 0.0)
        ftf[:, here, :] = hv * (tf[:, here, :] + tf[:, up, :])
        fsf[:, here, :] = hv * (sf[:, here, :] + sf[:, up, :])

    def tracers(tile, _):
        mid, nu, nv = face_counts(counts, side_cols, tile)
        out_rows = pl.ds(pl.multiple_of(SUB * tile, SUB), SUB)
        xt, xs = none, none
        for k in range(LEV):
            here, up, below = [level_rows(tile, k, step) for step in (0, 1, -1)]
            hu = jnp.where(nu > k, scale * uf[:, here, :], 0.0)
            hv = jnp.where(nv > k, scale * vf[:, here, :], 0.0)
            hw = west_stack(hu, edges[6, k, out_rows, :], last_lanes)
            inverse = jnp.where(mid > k + 1, 1.0 / pivot[k], 1.0 / final[k]) if k < LEV - 1 else 1.0 / final[k]

            def advance(flat, flux, which, x, w):
                q = flat[:, here, :]
                edge = edges[which, k, out_rows, :]
                flux_e = hu * (q + east_stack(q, edge, first_lanes))
                flux_w = hw * (q + west_stack(q, edge, last_lanes))
                flux_n = hv * (q + flat[:, up, :])
                flux[:, here, :] = flux_n
                new = q - ((flux_e - flux_w) + (flux_n - flux[:, below, :]))
                x = (new + DIFF_R * x) * inverse
                w[tile, k] = jnp.where(mid > k, x, new)
                return x

            xt = advance(tf, ftf, 4, xt, wt)
            xs = advance(sf, fsf, 5, xs, ws)
        pltpu.make_async_copy(wt.at[tile], wt_out.at[tile], store_sem.at[2, tile]).start()
        pltpu.make_async_copy(ws.at[tile], ws_out.at[tile], store_sem.at[3, tile]).start()
        return 0

    lax.fori_loop(0, TILES, tracers, 0)
    for tile in range(TILES):
        for i, (src, dst) in enumerate(((wu, wu_out), (wv, wv_out), (wt, wt_out), (ws, ws_out))):
            pltpu.make_async_copy(src.at[tile], dst.at[tile], store_sem.at[i, tile]).wait()
    leave(count_north + corner_north, count_south + corner_south, sides)
    for group in ((wide_up, wide_down, wide_across), (force_up, force_down, force_across)):
        arrive(*group)
        leave(*group)


def fast_kernel(n_row, n_sub, weights, wu_in, wv_in, wt_in, ws_in, eta, tu, tv, depth, wide_north, wide_south, wide_side,
                force, force_north, force_south, force_side, level_mean, counts, side_cols,
                eta_out, tu_out, tv_out, u_out, v_out, t_out, s_out,
                e_s, u_s, v_s, b_s, d_s, cu_s, cv_s, bu_s, bv_s, fu_s, fv_s, bar_u, bar_v, wu, wv, wt, ws, u_new, v_new, t_new, s_new, load_sem, store_sem):
    row = lax.axis_index('row')
    def fetch(tile):
        return [pltpu.make_async_copy(src.at[tile], dst.at[tile], load_sem.at[i, tile])
                for i, (src, dst) in enumerate(((wt_in, wt), (ws_in, ws), (wu_in, wu), (wv_in, wv)))]

    def put(tile, i, src, dst):
        rows = pl.ds(pl.multiple_of(SUB * tile, SUB), SUB)
        return pltpu.make_async_copy(src.at[:, rows, :], dst.at[:, rows, :], store_sem.at[i, tile])

    for part in (slice(0, 2), slice(2, 4)):
        for tile in range(TILES):
            for copy in fetch(tile)[part]:
                copy.start()
    lane = lane_index()
    at_first, at_last = lane == 0, lane == LANES - 1
    five = range(STRIPS + 1)
    dt_fast = TIME_STEP / n_sub
    total = ROWS * n_row
    zero = jnp.zeros((SUB, LANES), F32)

    def page(tile, c, offset=0):
        return pl.ds(c * PAGE + SUB + SUB * tile + offset, SUB)

    def gather(f, own, north, south, side, tile, c):
        if c == STRIPS:
            return side[f, SUB * tile:SUB * tile + SUB, :]
        lanes = slice(c * LANES, (c + 1) * LANES)
        if tile < REACH // SUB:
            return south[f, SUB * tile:SUB * tile + SUB, lanes]
        if tile < (REACH + ROWS) // SUB:
            return own[SUB * tile - REACH:SUB * tile - REACH + SUB, lanes]
        start = SUB * tile - REACH - ROWS
        return north[f, start:start + SUB, lanes]

    for ref in (e_s, u_s, v_s, b_s, d_s):
        for c in five:
            ref[page(-1, c), :] = zero
            ref[page(EXT_TILES, c), :] = zero
    for tile in range(EXT_TILES):
        for c in five:
            at = page(tile, c)
            e_s[at, :] = gather(0, eta, wide_north, wide_south, wide_side, tile, c)
            u_s[at, :] = dt_fast * gather(1, tu, wide_north, wide_south, wide_side, tile, c)
            v_s[at, :] = dt_fast * gather(2, tv, wide_north, wide_south, wide_side, tile, c)
            d_s[at, :] = gather(3, depth, wide_north, wide_south, wide_side, tile, c)
            bu_s[at, :] = gather(0, force.at[0], force_north, force_south, force_side, tile, c)
            bv_s[at, :] = gather(1, force.at[1], force_north, force_south, force_side, tile, c)
    for tile in range(EXT_TILES):
        place = row * ROWS + (SUB * tile - REACH) + lax.broadcasted_iota(jnp.int32, (SUB, LANES), 0)
        inside = jnp.logical_and(place >= 0, place < total)
        inside_v = jnp.logical_and(place >= 0, place < total - 1)
        row_pos = place.astype(F32)
        fu = (0.25 * dt_fast) * (CORIO_F0 + CORIO_BETA * ((row_pos + 0.5) / total - 0.5))
        fv = (0.25 * dt_fast) * (CORIO_F0 + CORIO_BETA * ((row_pos + 1.0) / total - 0.5))
        fu_s[SUB * tile:SUB * tile + SUB, :] = jnp.where(inside, fu, 0.0)
        fv_s[SUB * tile:SUB * tile + SUB, :] = jnp.where(inside_v, fv, 0.0)
        deep = [d_s[page(tile, c), :] for c in five]
        deep_e = east_of(deep, deep[0], at_first)
        for c in five:
            at = page(tile, c)
            hu = jnp.where(inside, 0.5 * (deep[c] + deep_e[c]), 0.0)
            hv = jnp.where(inside_v, 0.5 * (deep[c] + d_s[page(tile, c, 1), :]), 0.0)
            cu_s[at, :] = (dt_fast * dt_fast * GRAVITY) * hu
            cv_s[at, :] = (dt_fast * dt_fast * GRAVITY) * hv
            bu_s[at, :] = (dt_fast * dt_fast / TIME_STEP) * hu * bu_s[at, :]
            bv_s[at, :] = (dt_fast * dt_fast / TIME_STEP) * hv * bv_s[at, :]
    bar_u[...] = jnp.zeros_like(bar_u)
    bar_v[...] = jnp.zeros_like(bar_v)

    def subcycle(n, low, high):
        weight = weights[n]
        for tile in range(high - 1, low - 1, -1):
            uu = [u_s[page(tile, c), :] for c in five]
            vv = [v_s[page(tile, c), :] for c in five]
            v_south = [v_s[page(tile, c, -1), :] for c in five]
            part = [e_s[page(tile, c), :] - (uu[c] + (vv[c] - v_south[c])) for c in five]
            pair_v = [vv[c] + v_south[c] for c in five]
            u_west = west_of(uu, uu[-1], at_last)
            part_e = east_of(part, part[0], at_first)
            pair_ve = east_of(pair_v, pair_v[0], at_first)
            fu = fu_s[SUB * tile:SUB * tile + SUB, :]
            fv = fv_s[SUB * tile:SUB * tile + SUB, :]
            for c in five:
                at, up = page(tile, c), page(tile, c, 1)
                new = part[c] + u_west[c]
                pair_u = uu[c] + u_west[c]
                e_s[at, :] = new
                b_s[at, :] = pair_u
                u_next = uu[c] + ((fu * (pair_v[c] + pair_ve[c]) + bu_s[at, :]) - cu_s[at, :] * ((part_e[c] + uu[c]) - new))
                v_next = vv[c] + ((bv_s[at, :] - fv * (pair_u + b_s[up, :])) - cv_s[at, :] * (e_s[up, :] - new))
                u_s[at, :] = u_next
                v_s[at, :] = v_next
                if c < STRIPS and REACH // SUB <= tile < (REACH + ROWS) // SUB:
                    own = tile - REACH // SUB
                    bar_u[own, c] += weight * u_next
                    bar_v[own, c] += weight * v_next

    def wall_row():
        for tile in range(EXT_TILES):
            place = row * ROWS + (SUB * tile - REACH) + lax.broadcasted_iota(jnp.int32, (SUB, LANES), 0)
            wet = jnp.logical_and(place >= 0, place < total - 1)
            for c in five:
                at = page(tile, c)
                v_s[at, :] = jnp.where(wet, v_s[at, :], 0.0)
                if c < STRIPS and REACH // SUB <= tile < (REACH + ROWS) // SUB:
                    own = tile - REACH // SUB
                    bar_v[own, c] = jnp.where(wet, bar_v[own, c], 0.0)

    four = range(STRIPS)
    inner, _ = tables(DIFF_R)

    def tracers(tile, _):
        for copy in fetch(tile)[:2]:
            copy.wait()
        mid = [counts[c, pl.ds(pl.multiple_of(SUB * tile + SUB, SUB), SUB), :] for c in four]
        out_rows = pl.ds(pl.multiple_of(SUB * tile, SUB), SUB)
        xt, xs = [zero] * STRIPS, [zero] * STRIPS
        for k in range(LEV - 1, -1, -1):
            for c in four:
                on = mid[c] > k
                lanes = pl.ds(LANES * c, LANES)

                def solve(w, x, out):
                    value = w[tile, k, c]
                    full = value + (DIFF_R / inner[k]) * x[c]
                    out[k, out_rows, lanes] = jnp.where(on, full, value)
                    x[c] = jnp.where(on, full, 0.0)

                solve(wt, xt, t_new)
                solve(ws, xs, s_new)
        put(tile, 2, t_new, t_out).start()
        put(tile, 3, s_new, s_out).start()
        return 0

    n = 0
    while n < n_sub:
        spread = -(-(n_sub - n) // SUB)
        stop = n_sub - SUB * (spread - 1)
        low, high = REACH // SUB - spread, (REACH + ROWS) // SUB + spread

        def some(i, _, low=low, high=high, first=(n == 0)):
            subcycle(i, low, high)
            if first:
                pl.when(i == 0)(wall_row)
            return 0

        lax.fori_loop(n, stop, some, 0)
        if n == 0:
            lax.fori_loop(0, TILES, tracers, 0)
        n = stop

    pivot, final = tables(VISC_R)
    for tile in range(TILES):
        for c in four:
            at = page(tile + REACH // SUB, c)
            rows, lanes = pl.ds(SUB * tile, SUB), pl.ds(LANES * c, LANES)
            eta_out[rows, lanes] = e_s[at, :]
            tu_out[rows, lanes] = u_s[at, :] * (1.0 / dt_fast)
            tv_out[rows, lanes] = v_s[at, :] * (1.0 / dt_fast)

    def tile_step(tile, _):
        for copy in fetch(tile)[2:]:
            copy.wait()
        _, nu, nv = face_counts(counts, side_cols, tile)
        out_rows = pl.ds(pl.multiple_of(SUB * tile, SUB), SUB)
        add_u, add_v = [], []
        for c in four:
            at = pl.ds(c * PAGE + SUB + REACH + SUB * tile, SUB)
            lanes = pl.ds(LANES * c, LANES)
            deep_u = cu_s[at, :] * (1.0 / (dt_fast * GRAVITY))
            deep_v = cv_s[at, :] * (1.0 / (dt_fast * GRAVITY))
            deep_v = jnp.where(nv[c] > 0, deep_v, 1.0)
            add_u.append(bar_u[tile, c] / deep_u - level_mean[0, out_rows, lanes])
            add_v.append(bar_v[tile, c] / deep_v - level_mean[1, out_rows, lanes])
        xu, xv = [zero] * STRIPS, [zero] * STRIPS
        for k in range(LEV - 1, -1, -1):
            ratio, bottom = VISC_R / pivot[k], pivot[k] / final[k]
            for c in four:
                lanes = pl.ds(LANES * c, LANES)

                def solve(w, x, n, add, out):
                    value = w[tile, k, c]
                    last = value * bottom
                    if k < LEV - 1:
                        x[c] = jnp.where(n[c] > k + 1, value + ratio * x[c], last)
                    else:
                        x[c] = last
                    out[k, out_rows, lanes] = jnp.where(n[c] > k, x[c] + add[c], 0.0)

                solve(wu, xu, nu, add_u, u_new)
                solve(wv, xv, nv, add_v, v_new)
        put(tile, 0, u_new, u_out).start()
        put(tile, 1, v_new, v_out).start()
        return 0

    lax.fori_loop(0, TILES, tile_step, 0)
    for tile in range(TILES):
        for i, (src, dst) in enumerate(((u_new, u_out), (v_new, v_out), (t_new, t_out), (s_new, s_out))):
            put(tile, i, src, dst).wait()


def solution(mesh):
    n_row = mesh.shape['row']
    hbm = pl.BlockSpec(memory_space=pltpu.HBM)
    vmem = pl.BlockSpec(memory_space=pltpu.VMEM)
    smem = pl.BlockSpec(memory_space=pltpu.SMEM)
    dma = pltpu.SemaphoreType.DMA
    strip = pltpu.VMEM((STRIPS, LEV + 1, PITCH, LANES), F32)
    whole = pltpu.VMEM((LEV, ROWS, COLS), F32)
    column = pltpu.VMEM((TILES, LEV, STRIPS, SUB, LANES), F32)
    extended = pltpu.VMEM(((STRIPS + 1) * PAGE, LANES), F32)

    def shape(*dims):
        return jax.ShapeDtypeStruct(dims, F32)

    def call(body, ins, outs, shapes, scratch, **params):
        return pl.pallas_call(body, out_shape=shapes, in_specs=ins, out_specs=outs, scratch_shapes=scratch,
                              compiler_params=pltpu.CompilerParams(vmem_limit_bytes=VMEM_LIMIT, **params))

    def step(vel_u, vel_v, temp, salt, eta, tu, tv, depth, count, weights):
        n_sub = weights.shape[0]
        (wu, wv, wt, ws, force, level_mean, side_cols, counts, wide_north, wide_south, wide_side,
         force_north, force_south, force_side) = call(
            functools.partial(step_kernel, n_row), [hbm] * 4 + [vmem] * 5, [hbm] * 4 + [vmem] * 10,
            [shape(TILES, LEV, STRIPS, SUB, LANES)] * 4 + [shape(2, ROWS, COLS)] * 2
            + [shape(4, ROWS + 2 * SUB, LANES), shape(STRIPS, ROWS + 2 * SUB, LANES)]
            + [shape(4, REACH, COLS), shape(4, REACH, COLS), shape(4, EXT, LANES)]
            + [shape(2, REACH, COLS), shape(2, REACH, COLS), shape(2, EXT, LANES)],
            [strip] * 6 + [pltpu.VMEM((7, LEV, ROWS + SUB, LANES), F32)] + [column] * 4
            + [pltpu.VMEM((4, ROWS, LANES), F32)] * 2 + [pltpu.VMEM((2, ROWS, LANES), F32)]
            + [dma((4, STRIPS)), dma((64,)), dma((64,)), dma((4, TILES))],
            collective_id=0, has_side_effects=True)(vel_u, vel_v, temp, salt, eta, tu, tv, depth, count)
        return call(
            functools.partial(fast_kernel, n_row, n_sub), [smem] + [hbm] * 4 + [vmem] * 14, [vmem] * 3 + [hbm] * 4,
            [shape(ROWS, COLS)] * 3 + [shape(LEV, ROWS, COLS)] * 4,
            [extended] * 9 + [pltpu.VMEM((EXT, LANES), F32)] * 2 + [pltpu.VMEM((TILES, STRIPS, SUB, LANES), F32)] * 2
            + [column] * 4 + [whole] * 4 + [dma((4, TILES)), dma((4, TILES))],
        )(weights, wu, wv, wt, ws, eta, tu, tv, depth, wide_north, wide_south, wide_side,
          force, force_north, force_south, force_side, level_mean, counts, side_cols)

    cube = P(None, 'row', 'col')
    flat = P('row', 'col')
    return jax.shard_map(step, mesh=mesh, in_specs=(cube, cube, cube, cube, flat, flat, flat, flat, flat, P()),
                         out_specs=(flat, flat, flat, cube, cube, cube, cube), check_vma=False)
```

```python
import functools

import jax
import jax.numpy as jnp
from jax import lax
from jax.experimental import pallas as pl
from jax.experimental.pallas import tpu as pltpu
from jax.sharding import PartitionSpec as P

TIME_STEP = 1.0
GRAVITY = 16.0
BC_GRAVITY = 4.0
EXPAND_T = 0.2
CONTRACT_S = 0.6
CORIO_F0 = 0.4
CORIO_BETA = 0.4
VISC_R = 2.0
DIFF_R = 0.5

LEV = 41
ROWS = 48
SUB = 8
COLS = 512
LANES = 128
STRIPS = COLS // LANES
TILES = ROWS // SUB
PITCH = 56
REACH = 32
EXT = ROWS + 2 * REACH
EXT_TILES = EXT // SUB
PAGE = EXT + 16
MESH = pl.DeviceIdType.MESH
F32 = jnp.float32
VMEM_LIMIT = 62 * 1024 * 1024


def tables(strength):
    inner, last, ratio = [], [], 0.0
    for level in range(LEV):
        low = strength if level else 0.0
        pivot = 1.0 + low + strength - low * ratio
        inner.append(pivot)
        last.append(1.0 + low - low * ratio)
        ratio = strength / pivot
    return inner, last


def lane_index():
    return lax.broadcasted_iota(jnp.int32, (SUB, LANES), 1)


def west_of(strips, edge, at_last):
    mixed = [jnp.where(at_last, edge if c == 0 else strips[c - 1], strips[c]) for c in range(len(strips))]
    return [pltpu.roll(x, 1, 1) for x in mixed]


def east_of(strips, edge, at_first):
    n = len(strips)
    mixed = [jnp.where(at_first, edge if c == n - 1 else strips[c + 1], strips[c]) for c in range(n)]
    return [pltpu.roll(x, LANES - 1, 1) for x in mixed]


def places(n_row):
    row = lax.axis_index('row')
    col = lax.axis_index('col')
    other = 1 - col
    has_north = row < n_row - 1
    has_south = row > 0
    return dict(
        row=row, has_north=has_north, has_south=has_south,
        side={'col': other, 'row': row},
        north={'col': col, 'row': row + 1}, south={'col': col, 'row': row - 1},
        north_side={'col': other, 'row': row + 1}, south_side={'col': other, 'row': row - 1})


def meet(at):
    barrier = pltpu.get_barrier_semaphore()
    pl.semaphore_signal(barrier, inc=1, device_id=at['side'], device_id_type=MESH)

    @pl.when(at['has_north'])
    def _():
        pl.semaphore_signal(barrier, inc=1, device_id=at['north'], device_id_type=MESH)
        pl.semaphore_signal(barrier, inc=1, device_id=at['north_side'], device_id_type=MESH)

    @pl.when(at['has_south'])
    def _():
        pl.semaphore_signal(barrier, inc=1, device_id=at['south'], device_id_type=MESH)
        pl.semaphore_signal(barrier, inc=1, device_id=at['south_side'], device_id_type=MESH)

    return barrier


def await_meet(barrier, at):
    pl.semaphore_wait(barrier, 1 + 2 * at['has_north'].astype(jnp.int32) + 2 * at['has_south'].astype(jnp.int32))


def remote(src, dst, send, recv, where):
    return pltpu.make_async_remote_copy(src_ref=src, dst_ref=dst, send_sem=send, recv_sem=recv, device_id=where, device_id_type=MESH)


def level_rows(tile, k, offset=0):
    return pl.ds(SUB * tile + (PITCH * (k + 1) + offset), SUB)


def west_stack(strips, edge, at_last):
    return pltpu.roll(jnp.where(at_last, jnp.concatenate([edge[None], strips[:-1]], axis=0), strips), 1, 2)


def east_stack(strips, edge, at_first):
    return pltpu.roll(jnp.where(at_first, jnp.concatenate([strips[1:], edge[None]], axis=0), strips), LANES - 1, 2)


def face_counts(counts, side_cols, tile):
    rows = SUB * tile + SUB
    mid = counts[:, pl.ds(rows, SUB), :]
    north = counts[:, pl.ds(rows + 1, SUB), :]
    edge = pltpu.roll(side_cols[0, pl.ds(rows, SUB), :], LANES - 1 - 2 * LEV, 1)
    at_first = lax.broadcasted_iota(jnp.int32, mid.shape, 2) == 0
    return mid, jnp.minimum(mid, east_stack(mid, edge, at_first)), jnp.minimum(mid, north)


def unpack(packed, edges, f, rows):
    for k in range(LEV):
        edges[f, k, rows, :] = pltpu.roll(packed[f, rows, :], LANES - 1 - 2 * k, 1)


def step_kernel(n_row, u, v, t, s, eta, tu, tv, depth, count,
                wu_out, wv_out, wt_out, ws_out, force, level_mean, side_cols, counts,
                wide_north, wide_south, wide_side, force_north, force_south, force_side,
                cube, one_s, two_s, edges, wu, wv, wt, ws, own_cols, fold, force_fold,
                load_sem, send_sem, recv_sem, store_sem):
    at = places(n_row)
    fields = (u, v, t, s)
    four = range(STRIPS)

    def load(f, c, sem):
        return pltpu.make_async_copy(fields[f].at[:, :, pl.ds(LANES * c, LANES)], cube.at[f, c, pl.ds(1, LEV), pl.ds(0, ROWS), :], sem)

    outer = [[load(f, c, load_sem.at[2 * f + e]) for e, c in enumerate((0, STRIPS - 1))] for f in four]
    inner_sem = load_sem.at[2 * STRIPS]
    for pair in outer:
        for copy in pair:
            copy.start()
    for f in four:
        for c in range(1, STRIPS - 1):
            load(f, c, inner_sem).start()
    barrier = meet(at)
    lane = lane_index()
    at_first = lane == 0
    zero = jnp.zeros((SUB, LANES), F32)
    line = jnp.zeros((1, LANES), F32)
    for c in four:
        counts[c, SUB:SUB + ROWS, :] = count[:, c * LANES:(c + 1) * LANES].astype(F32)
    fast = (eta, tu, tv, depth)
    low_half = lax.broadcasted_iota(jnp.int32, (ROWS, LANES), 1) < LANES // 2
    for f in four:
        fold[f] = jnp.where(low_half, fast[f][:, :LANES], fast[f][:, COLS - LANES:])
    await_meet(barrier, at)
    slot = iter(range(LANES))

    def plan(where, region, *pairs):
        i = next(slot)
        copies = [remote(src, dst, send_sem.at[i], recv_sem.at[i], at[where]) for src, dst in pairs]
        return copies, remote(region, region, send_sem.at[i], recv_sem.at[i], at[where])

    def begin(plans):
        for copies, _ in plans:
            for copy in copies:
                copy.start()

    def start(north, south, side=()):
        pl.when(at['has_north'])(lambda: begin(north))
        pl.when(at['has_south'])(lambda: begin(south))
        begin(side)

    def received(plans):
        for _, waiter in plans:
            waiter.wait_recv()

    def sent(plans):
        for _, waiter in plans:
            waiter.wait_send()

    def arrive(north, south, side=()):
        received(side)
        pl.when(at['has_north'])(lambda: received(south))
        pl.when(at['has_south'])(lambda: received(north))

    def leave(north, south, side=()):
        sent(side)
        pl.when(at['has_north'])(lambda: sent(north))
        pl.when(at['has_south'])(lambda: sent(south))

    def row_region(level, row):
        return cube.at[:, :, pl.ds(level, LEV), pl.ds(row, 1), :]

    def row_pairs(source, level, row):
        return [(fields[f].at[:, pl.ds(source, 1), pl.ds(LANES * c, LANES)], cube.at[f, c, pl.ds(level, LEV), pl.ds(row, 1), :])
                for f in four for c in four]

    rows_north = [plan('north', row_region(0, PITCH - 1), *row_pairs(ROWS - 1, 0, PITCH - 1))]
    rows_south = [plan('south', row_region(1, ROWS), *row_pairs(0, 1, ROWS))]
    low_tile, high_tile = counts.at[:, pl.ds(0, SUB), :], counts.at[:, pl.ds(SUB + ROWS, SUB), :]
    count_north = [plan('north', low_tile, (counts.at[:, pl.ds(ROWS, SUB), :], low_tile))]
    count_south = [plan('south', high_tile, (counts.at[:, pl.ds(SUB, SUB), :], high_tile))]
    start(count_north + rows_north, count_south + rows_south)

    half_lane = lane >> 1
    sides = []
    for f in four:
        for copy in outer[f]:
            copy.wait()

        def pack(tile, _):
            rows = pl.ds(pl.multiple_of(SUB * tile, SUB), SUB)
            packed = zero
            for k in range(LEV + 1 if f == 0 else LEV):
                if k < LEV:
                    first, last = cube[f, 0, k + 1, rows, :], cube[f, STRIPS - 1, k + 1, rows, :]
                else:
                    lower = pl.ds(pl.multiple_of(SUB * tile + SUB, SUB), SUB)
                    first, last = counts[0, lower, :], counts[STRIPS - 1, lower, :]
                both = pltpu.roll(jnp.where(at_first, first, last), 2 * k + 1, 1)
                packed = jnp.where(half_lane == k, both, packed)
            own_cols[f, rows, :] = packed
            return 0

        lax.fori_loop(0, TILES, pack, 0)
        target = side_cols.at[f, pl.ds(SUB, ROWS), :]
        sides.append(plan('side', target, (own_cols.at[f], target)))
        begin(sides[-1:])
    high_u, low_v = side_cols.at[0, pl.ds(SUB + ROWS, SUB), :], side_cols.at[1, pl.ds(0, SUB), :]
    corner_south = [plan('south_side', high_u, (own_cols.at[0, pl.ds(0, SUB), :], high_u))]
    corner_north = [plan('north_side', low_v, (own_cols.at[1, pl.ds(ROWS - SUB, SUB), :], low_v))]
    start(corner_north, corner_south)

    def clear(level, row):
        def body(k, _):
            for f in four:
                for c in four:
                    cube[f, c, k + level, pl.ds(row, 1), :] = line
            return 0

        lax.fori_loop(0, LEV, body, 0)

    @pl.when(jnp.logical_not(at['has_north']))
    def _():
        clear(1, ROWS)
        counts[:, SUB + ROWS:, :] = jnp.zeros((STRIPS, SUB, LANES), F32)
        side_cols[:, SUB + ROWS:, :] = jnp.zeros((STRIPS, SUB, LANES), F32)
        wide_north[...] = jnp.zeros_like(wide_north)
        force_north[...] = jnp.zeros_like(force_north)
        wide_side[:, REACH + ROWS:, :] = jnp.zeros((STRIPS, REACH, LANES), F32)
        force_side[:, REACH + ROWS:, :] = jnp.zeros((2, REACH, LANES), F32)

    @pl.when(jnp.logical_not(at['has_south']))
    def _():
        clear(0, PITCH - 1)
        counts[:, :SUB, :] = jnp.zeros((STRIPS, SUB, LANES), F32)
        side_cols[:, :SUB, :] = jnp.zeros((STRIPS, SUB, LANES), F32)
        wide_south[...] = jnp.zeros_like(wide_south)
        force_south[...] = jnp.zeros_like(force_south)
        wide_side[:, :REACH, :] = jnp.zeros((STRIPS, REACH, LANES), F32)
        force_side[:, :REACH, :] = jnp.zeros((2, REACH, LANES), F32)

    half_scale = 0.5 * BC_GRAVITY / LEV
    scale = 0.5 * TIME_STEP

    def density(sal, tem):
        return (half_scale * CONTRACT_S) * sal - (half_scale * EXPAND_T) * tem

    for f in four:
        received(sides[f:f + 1])

        def spread(tile, _):
            unpack(side_cols, edges, f, pl.ds(pl.multiple_of(SUB * tile, SUB), SUB))
            return 0

        lax.fori_loop(1, TILES + 1, spread, 0)
    arrive(count_north + corner_north, count_south + corner_south)
    unpack(side_cols, edges, 0, pl.ds(SUB + ROWS, SUB))
    unpack(side_cols, edges, 1, pl.ds(0, SUB))
    pltpu.make_async_copy(cube.at[:, pl.ds(1, STRIPS - 2), pl.ds(1, LEV), pl.ds(0, ROWS), :],
                          cube.at[:, pl.ds(1, STRIPS - 2), pl.ds(1, LEV), pl.ds(0, ROWS), :], inner_sem).wait()
    arrive(rows_north, rows_south)
    leave(rows_north, rows_south)
    low_rows, high_rows = pl.ds(0, REACH), pl.ds(ROWS - REACH, REACH)
    side_low, side_high = wide_side.at[:, low_rows, :], wide_side.at[:, pl.ds(REACH + ROWS, REACH), :]
    side_mid = wide_side.at[:, pl.ds(REACH, ROWS), :]
    wide_up = [plan('north', wide_south, *[(fast[f].at[high_rows, :], wide_south.at[f]) for f in four]),
               plan('north_side', side_low, (fold.at[:, high_rows, :], side_low))]
    wide_down = [plan('south', wide_north, *[(fast[f].at[low_rows, :], wide_north.at[f]) for f in four]),
                 plan('south_side', side_high, (fold.at[:, low_rows, :], side_high))]
    wide_across = [plan('side', side_mid, (fold, side_mid))]
    start(wide_up, wide_down, wide_across)
    rows_flat = (LEV + 1) * PITCH
    uf, vf, tf, sf = [cube.at[f].reshape(STRIPS, rows_flat, LANES) for f in four]
    pf, bf = [ref.reshape(STRIPS, rows_flat, LANES) for ref in (one_s, two_s)]
    stack = lax.broadcasted_iota(jnp.int32, (STRIPS, SUB, LANES), 2)
    first_lanes, last_lanes = stack == 0, stack == LANES - 1
    none = jnp.zeros((STRIPS, SUB, LANES), F32)
    pivot, _ = tables(VISC_R)
    acc = none
    for k in range(LEV):
        spot = level_rows(TILES, k)
        uu = uf[:, spot, :]
        bf[:, spot, :] = uu + west_stack(uu, edges[0, k, pl.ds(SUB + ROWS, SUB), :], last_lanes)
        rho = density(sf[:, spot, :], tf[:, spot, :])
        pf[:, spot, :] = acc + rho
        acc = (acc + rho) + rho

    def momentum(step, _):
        tile = TILES - 1 - step
        _, nu, nv = face_counts(counts, side_cols, tile)
        row_pos = (at['row'] * ROWS + SUB * tile + lax.broadcasted_iota(jnp.int32, (STRIPS, SUB, LANES), 1)).astype(F32)
        fu = 0.25 * (CORIO_F0 + CORIO_BETA * ((row_pos + 0.5) / (ROWS * n_row) - 0.5))
        fv = 0.25 * (CORIO_F0 + CORIO_BETA * ((row_pos + 1.0) / (ROWS * n_row) - 0.5))
        out_rows = pl.ds(pl.multiple_of(SUB * tile, SUB), SUB)
        mid_rows = pl.ds(pl.multiple_of(SUB * tile + SUB, SUB), SUB)
        acc, acc_e = none, zero
        xu, xv, sum_du, sum_dv, sum_su, sum_sv = (none,) * 6
        for k in range(LEV):
            here, up, below = [level_rows(tile, k, step) for step in (0, 1, -1)]
            uu, vv = uf[:, here, :], vf[:, here, :]
            v_south = vf[:, below, :]
            edge_u, edge_v = edges[0, k, mid_rows, :], edges[1, k, mid_rows, :]
            u_west = west_stack(uu, edge_u, last_lanes)
            u_east = east_stack(uu, edge_u, first_lanes)
            v_west = west_stack(vv, edge_v, last_lanes)
            v_east = east_stack(vv, edge_v, first_lanes)
            pair_v = vv + v_south
            pair_ve = east_stack(pair_v, edge_v + edges[1, k, pl.ds(SUB * tile + SUB - 1, SUB), :], first_lanes)
            rho_e = density(edges[3, k, mid_rows, :], edges[2, k, mid_rows, :])
            p_edge = acc_e + rho_e
            acc_e = p_edge + rho_e
            rho = density(sf[:, here, :], tf[:, here, :])
            pp = acc + rho
            acc = pp + rho
            pf[:, here, :] = pp
            p_east = east_stack(pp, p_edge, first_lanes)
            pair_u = uu + u_west
            bf[:, here, :] = pair_u
            v4 = pair_v + pair_ve
            u4 = pair_u + bf[:, up, :]
            du = v4 * (fu - 0.125 * (uf[:, up, :] - uf[:, below, :])) - 0.5 * uu * (u_east - u_west) + (pp - p_east)
            dv = (pp - pf[:, up, :]) - u4 * (fv + 0.125 * (v_east - v_west)) - 0.5 * vv * (vf[:, up, :] - v_south)
            us, vs = uu + du, vv + dv
            on_u, on_v = nu > k, nv > k
            sum_du += jnp.where(on_u, du, 0.0)
            sum_dv += jnp.where(on_v, dv, 0.0)
            sum_su += jnp.where(on_u, us, 0.0)
            sum_sv += jnp.where(on_v, vs, 0.0)
            xu = us * (1.0 / pivot[k]) + xu * (VISC_R / pivot[k])
            xv = vs * (1.0 / pivot[k]) + xv * (VISC_R / pivot[k])
            wu[tile, k] = xu
            wv[tile, k] = xv
        inv_u = 1.0 / jnp.maximum(nu, 1.0)
        inv_v = 1.0 / jnp.maximum(nv, 1.0)
        for c in four:
            lanes = pl.ds(LANES * c, LANES)
            force[0, out_rows, lanes] = (sum_du * inv_u)[c]
            force[1, out_rows, lanes] = (sum_dv * inv_v)[c]
            level_mean[0, out_rows, lanes] = (sum_su * inv_u)[c]
            level_mean[1, out_rows, lanes] = (sum_sv * inv_v)[c]
        pltpu.make_async_copy(wu.at[tile], wu_out.at[tile], store_sem.at[0]).start()
        pltpu.make_async_copy(wv.at[tile], wv_out.at[tile], store_sem.at[1]).start()
        return 0

    lax.fori_loop(0, TILES, momentum, 0)

    for f in range(2):
        force_fold[f] = jnp.where(low_half, force[f, :, :LANES], force[f, :, COLS - LANES:])
    side_low, side_high = force_side.at[:, low_rows, :], force_side.at[:, pl.ds(REACH + ROWS, REACH), :]
    side_mid = force_side.at[:, pl.ds(REACH, ROWS), :]
    force_up = [plan('north', force_south, (force.at[:, high_rows, :], force_south)),
                plan('north_side', side_low, (force_fold.at[:, high_rows, :], side_low))]
    force_down = [plan('south', force_north, (force.at[:, low_rows, :], force_north)),
                  plan('south_side', side_high, (force_fold.at[:, low_rows, :], side_high))]
    force_across = [plan('side', side_mid, (force_fold, side_mid))]
    start(force_up, force_down, force_across)

    ftf, fsf = pf, bf
    pivot, final = tables(DIFF_R)

    south_count = jnp.minimum(counts[:, pl.ds(0, SUB), :], counts[:, pl.ds(1, SUB), :])
    for k in range(LEV):
        here, up = level_rows(-1, k), level_rows(-1, k, 1)
        hv = jnp.where(south_count > k, scale * vf[:, here, :], 0.0)
        ftf[:, here, :] = hv * (tf[:, here, :] + tf[:, up, :])
        fsf[:, here, :] = hv * (sf[:, here, :] + sf[:, up, :])

    def tracers(tile, _):
        mid, nu, nv = face_counts(counts, side_cols, tile)
        out_rows = pl.ds(pl.multiple_of(SUB * tile, SUB), SUB)
        mid_rows = pl.ds(pl.multiple_of(SUB * tile + SUB, SUB), SUB)
        west_count = jnp.minimum(pltpu.roll(side_cols[0, mid_rows, :], LANES - 1 - 2 * LEV, 1), pltpu.roll(counts[0, mid_rows, :], LANES - 1, 1))
        xt, xs = none, none
        for k in range(LEV):
            here, up, below = [level_rows(tile, k, step) for step in (0, 1, -1)]
            hu = jnp.where(nu > k, scale * uf[:, here, :], 0.0)
            hv = jnp.where(nv > k, scale * vf[:, here, :], 0.0)
            hw = west_stack(hu, jnp.where(west_count > k, scale * edges[0, k, mid_rows, :], 0.0), last_lanes)
            inverse = jnp.where(mid > k + 1, 1.0 / pivot[k], 1.0 / final[k]) if k < LEV - 1 else 1.0 / final[k]

            def advance(flat, flux, which, x, w):
                q = flat[:, here, :]
                edge = edges[which, k, mid_rows, :]
                flux_e = hu * (q + east_stack(q, edge, first_lanes))
                flux_w = hw * (q + west_stack(q, edge, last_lanes))
                flux_n = hv * (q + flat[:, up, :])
                flux[:, here, :] = flux_n
                new = q - ((flux_e - flux_w) + (flux_n - flux[:, below, :]))
                x = (new + DIFF_R * x) * inverse
                w[tile, k] = jnp.where(mid > k, x, new)
                return x

            xt = advance(tf, ftf, 2, xt, wt)
            xs = advance(sf, fsf, 3, xs, ws)
        pltpu.make_async_copy(wt.at[tile], wt_out.at[tile], store_sem.at[2]).start()
        pltpu.make_async_copy(ws.at[tile], ws_out.at[tile], store_sem.at[3]).start()
        return 0

    lax.fori_loop(0, TILES, tracers, 0)
    for i, (src, dst) in enumerate(((wu, wu_out), (wv, wv_out), (wt, wt_out), (ws, ws_out))):
        pltpu.make_async_copy(src, dst, store_sem.at[i]).wait()
    leave(count_north + corner_north, count_south + corner_south, sides)
    for group in ((wide_up, wide_down, wide_across), (force_up, force_down, force_across)):
        arrive(*group)
        leave(*group)


def fast_kernel(n_row, n_sub, weights, wu_in, wv_in, wt_in, ws_in, eta, tu, tv, depth, wide_north, wide_south, wide_side,
                force, force_north, force_south, force_side, level_mean, counts, side_cols,
                eta_out, tu_out, tv_out, u_out, v_out, t_out, s_out,
                e_s, u_s, v_s, b_s, d_s, cu_s, cv_s, bu_s, bv_s, fu_s, fv_s, bar_u, bar_v, wu, wv, wt, ws, u_new, v_new, t_new, s_new, load_sem, store_sem):
    row = lax.axis_index('row')
    def fetch(tile):
        return [pltpu.make_async_copy(src.at[tile], dst.at[tile], load_sem.at[i, tile])
                for i, (src, dst) in enumerate(((wt_in, wt), (ws_in, ws), (wu_in, wu), (wv_in, wv)))]

    def put(tile, i, src, dst):
        rows = pl.ds(pl.multiple_of(SUB * tile, SUB), SUB)
        return pltpu.make_async_copy(src.at[:, rows, :], dst.at[:, rows, :], store_sem.at[i, tile])

    for part in (slice(0, 2), slice(2, 4)):
        for tile in range(TILES):
            for copy in fetch(tile)[part]:
                copy.start()
    lane = lane_index()
    at_first, at_last = lane == 0, lane == LANES - 1
    five = range(STRIPS + 1)
    dt_fast = TIME_STEP / n_sub
    total = ROWS * n_row
    zero = jnp.zeros((SUB, LANES), F32)

    def page(tile, c, offset=0):
        return pl.ds(c * PAGE + SUB + SUB * tile + offset, SUB)

    def gather(f, own, north, south, side, tile, c):
        if c == STRIPS:
            return side[f, SUB * tile:SUB * tile + SUB, :]
        lanes = slice(c * LANES, (c + 1) * LANES)
        if tile < REACH // SUB:
            return south[f, SUB * tile:SUB * tile + SUB, lanes]
        if tile < (REACH + ROWS) // SUB:
            return own[SUB * tile - REACH:SUB * tile - REACH + SUB, lanes]
        start = SUB * tile - REACH - ROWS
        return north[f, start:start + SUB, lanes]

    for ref in (e_s, u_s, v_s, b_s, d_s):
        for c in five:
            ref[page(-1, c), :] = zero
            ref[page(EXT_TILES, c), :] = zero
    for tile in range(EXT_TILES):
        for c in five:
            at = page(tile, c)
            e_s[at, :] = gather(0, eta, wide_north, wide_south, wide_side, tile, c)
            u_s[at, :] = dt_fast * gather(1, tu, wide_north, wide_south, wide_side, tile, c)
            v_s[at, :] = dt_fast * gather(2, tv, wide_north, wide_south, wide_side, tile, c)
            d_s[at, :] = gather(3, depth, wide_north, wide_south, wide_side, tile, c)
            bu_s[at, :] = gather(0, force.at[0], force_north, force_south, force_side, tile, c)
            bv_s[at, :] = gather(1, force.at[1], force_north, force_south, force_side, tile, c)
    for tile in range(EXT_TILES):
        place = row * ROWS + (SUB * tile - REACH) + lax.broadcasted_iota(jnp.int32, (SUB, LANES), 0)
        inside = jnp.logical_and(place >= 0, place < total)
        inside_v = jnp.logical_and(place >= 0, place < total - 1)
        row_pos = place.astype(F32)
        fu = (0.25 * dt_fast) * (CORIO_F0 + CORIO_BETA * ((row_pos + 0.5) / total - 0.5))
        fv = (0.25 * dt_fast) * (CORIO_F0 + CORIO_BETA * ((row_pos + 1.0) / total - 0.5))
        fu_s[SUB * tile:SUB * tile + SUB, :] = jnp.where(inside, fu, 0.0)
        fv_s[SUB * tile:SUB * tile + SUB, :] = jnp.where(inside_v, fv, 0.0)
        deep = [d_s[page(tile, c), :] for c in five]
        deep_e = east_of(deep, deep[0], at_first)
        for c in five:
            at = page(tile, c)
            hu = jnp.where(inside, 0.5 * (deep[c] + deep_e[c]), 0.0)
            hv = jnp.where(inside_v, 0.5 * (deep[c] + d_s[page(tile, c, 1), :]), 0.0)
            cu_s[at, :] = (dt_fast * dt_fast * GRAVITY) * hu
            cv_s[at, :] = (dt_fast * dt_fast * GRAVITY) * hv
            bu_s[at, :] = (dt_fast * dt_fast / TIME_STEP) * hu * bu_s[at, :]
            bv_s[at, :] = (dt_fast * dt_fast / TIME_STEP) * hv * bv_s[at, :]
    bar_u[...] = jnp.zeros_like(bar_u)
    bar_v[...] = jnp.zeros_like(bar_v)

    def subcycle(n, low, high):
        weight = weights[n]
        for tile in range(high - 1, low - 1, -1):
            uu = [u_s[page(tile, c), :] for c in five]
            vv = [v_s[page(tile, c), :] for c in five]
            v_south = [v_s[page(tile, c, -1), :] for c in five]
            part = [e_s[page(tile, c), :] - (uu[c] + (vv[c] - v_south[c])) for c in five]
            pair_v = [vv[c] + v_south[c] for c in five]
            u_west = west_of(uu, uu[-1], at_last)
            part_e = east_of(part, part[0], at_first)
            pair_ve = east_of(pair_v, pair_v[0], at_first)
            fu = fu_s[SUB * tile:SUB * tile + SUB, :]
            fv = fv_s[SUB * tile:SUB * tile + SUB, :]
            for c in five:
                at, up = page(tile, c), page(tile, c, 1)
                new = part[c] + u_west[c]
                pair_u = uu[c] + u_west[c]
                e_s[at, :] = new
                b_s[at, :] = pair_u
                u_next = uu[c] + ((fu * (pair_v[c] + pair_ve[c]) + bu_s[at, :]) - cu_s[at, :] * ((part_e[c] + uu[c]) - new))
                v_next = vv[c] + ((bv_s[at, :] - fv * (pair_u + b_s[up, :])) - cv_s[at, :] * (e_s[up, :] - new))
                u_s[at, :] = u_next
                v_s[at, :] = v_next
                if c < STRIPS and REACH // SUB <= tile < (REACH + ROWS) // SUB:
                    own = tile - REACH // SUB
                    bar_u[own, c] += weight * u_next
                    bar_v[own, c] += weight * v_next

    def wall_row():
        for tile in range(EXT_TILES):
            place = row * ROWS + (SUB * tile - REACH) + lax.broadcasted_iota(jnp.int32, (SUB, LANES), 0)
            wet = jnp.logical_and(place >= 0, place < total - 1)
            for c in five:
                at = page(tile, c)
                v_s[at, :] = jnp.where(wet, v_s[at, :], 0.0)
                if c < STRIPS and REACH // SUB <= tile < (REACH + ROWS) // SUB:
                    own = tile - REACH // SUB
                    bar_v[own, c] = jnp.where(wet, bar_v[own, c], 0.0)

    four = range(STRIPS)
    inner, _ = tables(DIFF_R)

    def tracers(tile, _):
        for copy in fetch(tile)[:2]:
            copy.wait()
        mid = [counts[c, pl.ds(pl.multiple_of(SUB * tile + SUB, SUB), SUB), :] for c in four]
        out_rows = pl.ds(pl.multiple_of(SUB * tile, SUB), SUB)
        xt, xs = [zero] * STRIPS, [zero] * STRIPS
        for k in range(LEV - 1, -1, -1):
            for c in four:
                on = mid[c] > k
                lanes = pl.ds(LANES * c, LANES)

                def solve(w, x, out):
                    value = w[tile, k, c]
                    full = value + (DIFF_R / inner[k]) * x[c]
                    out[k, out_rows, lanes] = jnp.where(on, full, value)
                    x[c] = jnp.where(on, full, 0.0)

                solve(wt, xt, t_new)
                solve(ws, xs, s_new)
        put(tile, 2, t_new, t_out).start()
        put(tile, 3, s_new, s_out).start()
        return 0

    n = 0
    while n < n_sub:
        spread = -(-(n_sub - n) // SUB)
        stop = n_sub - SUB * (spread - 1)
        low, high = REACH // SUB - spread, (REACH + ROWS) // SUB + spread

        def some(i, _, low=low, high=high, first=(n == 0)):
            subcycle(i, low, high)
            if first:
                pl.when(i == 0)(wall_row)
            return 0

        lax.fori_loop(n, stop, some, 0)
        if n == 0:
            lax.fori_loop(0, TILES, tracers, 0)
        n = stop

    pivot, final = tables(VISC_R)
    for tile in range(TILES):
        for c in four:
            at = page(tile + REACH // SUB, c)
            rows, lanes = pl.ds(SUB * tile, SUB), pl.ds(LANES * c, LANES)
            eta_out[rows, lanes] = e_s[at, :]
            tu_out[rows, lanes] = u_s[at, :] * (1.0 / dt_fast)
            tv_out[rows, lanes] = v_s[at, :] * (1.0 / dt_fast)

    def tile_step(tile, _):
        for copy in fetch(tile)[2:]:
            copy.wait()
        _, nu, nv = face_counts(counts, side_cols, tile)
        out_rows = pl.ds(pl.multiple_of(SUB * tile, SUB), SUB)
        add_u, add_v = [], []
        for c in four:
            at = pl.ds(c * PAGE + SUB + REACH + SUB * tile, SUB)
            lanes = pl.ds(LANES * c, LANES)
            deep_u = cu_s[at, :] * (1.0 / (dt_fast * GRAVITY))
            deep_v = cv_s[at, :] * (1.0 / (dt_fast * GRAVITY))
            deep_v = jnp.where(nv[c] > 0, deep_v, 1.0)
            add_u.append(bar_u[tile, c] / deep_u - level_mean[0, out_rows, lanes])
            add_v.append(bar_v[tile, c] / deep_v - level_mean[1, out_rows, lanes])
        xu, xv = [zero] * STRIPS, [zero] * STRIPS
        for k in range(LEV - 1, -1, -1):
            ratio, bottom = VISC_R / pivot[k], pivot[k] / final[k]
            for c in four:
                lanes = pl.ds(LANES * c, LANES)

                def solve(w, x, n, add, out):
                    value = w[tile, k, c]
                    last = value * bottom
                    if k < LEV - 1:
                        x[c] = jnp.where(n[c] > k + 1, value + ratio * x[c], last)
                    else:
                        x[c] = last
                    out[k, out_rows, lanes] = jnp.where(n[c] > k, x[c] + add[c], 0.0)

                solve(wu, xu, nu, add_u, u_new)
                solve(wv, xv, nv, add_v, v_new)
        put(tile, 0, u_new, u_out).start()
        put(tile, 1, v_new, v_out).start()
        return 0

    lax.fori_loop(0, TILES, tile_step, 0)
    for tile in range(TILES):
        for i, (src, dst) in enumerate(((u_new, u_out), (v_new, v_out), (t_new, t_out), (s_new, s_out))):
            put(tile, i, src, dst).wait()


def solution(mesh):
    n_row = mesh.shape['row']
    hbm = pl.BlockSpec(memory_space=pltpu.HBM)
    vmem = pl.BlockSpec(memory_space=pltpu.VMEM)
    smem = pl.BlockSpec(memory_space=pltpu.SMEM)
    dma = pltpu.SemaphoreType.DMA
    strip = pltpu.VMEM((STRIPS, LEV + 1, PITCH, LANES), F32)
    whole = pltpu.VMEM((LEV, ROWS, COLS), F32)
    column = pltpu.VMEM((TILES, LEV, STRIPS, SUB, LANES), F32)
    extended = pltpu.VMEM(((STRIPS + 1) * PAGE, LANES), F32)

    def shape(*dims):
        return jax.ShapeDtypeStruct(dims, F32)

    def call(body, ins, outs, shapes, scratch, **params):
        return pl.pallas_call(body, out_shape=shapes, in_specs=ins, out_specs=outs, scratch_shapes=scratch,
                              compiler_params=pltpu.CompilerParams(vmem_limit_bytes=VMEM_LIMIT, **params))

    def step(vel_u, vel_v, temp, salt, eta, tu, tv, depth, count, weights):
        n_sub = weights.shape[0]
        (wu, wv, wt, ws, force, level_mean, side_cols, counts, wide_north, wide_south, wide_side,
         force_north, force_south, force_side) = call(
            functools.partial(step_kernel, n_row), [hbm] * 4 + [vmem] * 5, [hbm] * 4 + [vmem] * 10,
            [shape(TILES, LEV, STRIPS, SUB, LANES)] * 4 + [shape(2, ROWS, COLS)] * 2
            + [shape(4, ROWS + 2 * SUB, LANES), shape(STRIPS, ROWS + 2 * SUB, LANES)]
            + [shape(4, REACH, COLS), shape(4, REACH, COLS), shape(4, EXT, LANES)]
            + [shape(2, REACH, COLS), shape(2, REACH, COLS), shape(2, EXT, LANES)],
            [pltpu.VMEM((4, STRIPS, LEV + 1, PITCH, LANES), F32)] + [strip] * 2 + [pltpu.VMEM((4, LEV, ROWS + 2 * SUB, LANES), F32)] + [column] * 4
            + [pltpu.VMEM((4, ROWS, LANES), F32)] * 2 + [pltpu.VMEM((2, ROWS, LANES), F32)]
            + [dma((9,)), dma((20,)), dma((20,)), dma((4,))],
            collective_id=0, has_side_effects=True)(vel_u, vel_v, temp, salt, eta, tu, tv, depth, count)
        return call(
            functools.partial(fast_kernel, n_row, n_sub), [smem] + [hbm] * 4 + [vmem] * 14, [vmem] * 3 + [hbm] * 4,
            [shape(ROWS, COLS)] * 3 + [shape(LEV, ROWS, COLS)] * 4,
            [extended] * 9 + [pltpu.VMEM((EXT, LANES), F32)] * 2 + [pltpu.VMEM((TILES, STRIPS, SUB, LANES), F32)] * 2
            + [column] * 4 + [whole] * 4 + [dma((4, TILES)), dma((4, TILES))],
        )(weights, wu, wv, wt, ws, eta, tu, tv, depth, wide_north, wide_south, wide_side,
          force, force_north, force_south, force_side, level_mean, counts, side_cols)

    cube = P(None, 'row', 'col')
    flat = P('row', 'col')
    return jax.shard_map(step, mesh=mesh, in_specs=(cube, cube, cube, cube, flat, flat, flat, flat, flat, P()),
                         out_specs=(flat, flat, flat, cube, cube, cube, cube), check_vma=False)
```

```python
import functools

import jax
import jax.numpy as jnp
from jax import lax
from jax.experimental import pallas as pl
from jax.experimental.pallas import tpu as pltpu
from jax.sharding import PartitionSpec as P

TIME_STEP = 1.0
GRAVITY = 16.0
BC_GRAVITY = 4.0
EXPAND_T = 0.2
CONTRACT_S = 0.6
CORIO_F0 = 0.4
CORIO_BETA = 0.4
VISC_R = 2.0
DIFF_R = 0.5

LEV = 41
ROWS = 48
SUB = 8
COLS = 512
LANES = 128
STRIPS = COLS // LANES
TILES = ROWS // SUB
PITCH = 56
REACH = 32
EXT = ROWS + 2 * REACH
EXT_TILES = EXT // SUB
PAGE = EXT + 16
MESH = pl.DeviceIdType.MESH
F32 = jnp.float32
VMEM_LIMIT = 62 * 1024 * 1024


def tables(strength):
    inner, last, ratio = [], [], 0.0
    for level in range(LEV):
        low = strength if level else 0.0
        pivot = 1.0 + low + strength - low * ratio
        inner.append(pivot)
        last.append(1.0 + low - low * ratio)
        ratio = strength / pivot
    return inner, last


def lane_index():
    return lax.broadcasted_iota(jnp.int32, (SUB, LANES), 1)


def west_of(strips, edge, at_last):
    mixed = [jnp.where(at_last, edge if c == 0 else strips[c - 1], strips[c]) for c in range(len(strips))]
    return [pltpu.roll(x, 1, 1) for x in mixed]


def east_of(strips, edge, at_first):
    n = len(strips)
    mixed = [jnp.where(at_first, edge if c == n - 1 else strips[c + 1], strips[c]) for c in range(n)]
    return [pltpu.roll(x, LANES - 1, 1) for x in mixed]


def places(n_row):
    row = lax.axis_index('row')
    col = lax.axis_index('col')
    other = 1 - col
    has_north = row < n_row - 1
    has_south = row > 0
    return dict(
        row=row, has_north=has_north, has_south=has_south,
        side={'col': other, 'row': row},
        north={'col': col, 'row': row + 1}, south={'col': col, 'row': row - 1},
        north_side={'col': other, 'row': row + 1}, south_side={'col': other, 'row': row - 1})


def meet(at):
    barrier = pltpu.get_barrier_semaphore()
    pl.semaphore_signal(barrier, inc=1, device_id=at['side'], device_id_type=MESH)

    @pl.when(at['has_north'])
    def _():
        pl.semaphore_signal(barrier, inc=1, device_id=at['north'], device_id_type=MESH)
        pl.semaphore_signal(barrier, inc=1, device_id=at['north_side'], device_id_type=MESH)

    @pl.when(at['has_south'])
    def _():
        pl.semaphore_signal(barrier, inc=1, device_id=at['south'], device_id_type=MESH)
        pl.semaphore_signal(barrier, inc=1, device_id=at['south_side'], device_id_type=MESH)

    return barrier


def await_meet(barrier, at):
    pl.semaphore_wait(barrier, 1 + 2 * at['has_north'].astype(jnp.int32) + 2 * at['has_south'].astype(jnp.int32))


def remote(src, dst, send, recv, where):
    return pltpu.make_async_remote_copy(src_ref=src, dst_ref=dst, send_sem=send, recv_sem=recv, device_id=where, device_id_type=MESH)


def level_rows(tile, k, offset=0):
    return pl.ds(SUB * tile + (PITCH * (k + 1) + offset), SUB)


def west_stack(strips, edge, at_last):
    return pltpu.roll(jnp.where(at_last, jnp.concatenate([edge[None], strips[:-1]], axis=0), strips), 1, 2)


def east_stack(strips, edge, at_first):
    return pltpu.roll(jnp.where(at_first, jnp.concatenate([strips[1:], edge[None]], axis=0), strips), LANES - 1, 2)


def face_counts(counts, side, tile):
    rows = SUB * tile + SUB
    mid = counts[:, pl.ds(rows, SUB), :]
    north = counts[:, pl.ds(rows + 1, SUB), :]
    edge = pltpu.roll(side[pl.ds(rows, SUB), :], LANES - 1 - 2 * LEV, 1)
    at_first = lax.broadcasted_iota(jnp.int32, mid.shape, 2) == 0
    return mid, jnp.minimum(mid, east_stack(mid, edge, at_first)), jnp.minimum(mid, north)


def unpack(packed, edges, f, rows):
    for k in range(LEV):
        edges[f, k, rows, :] = pltpu.roll(packed[f, rows, :], LANES - 1 - 2 * k, 1)


def step_kernel(n_row, u, v, t, s, eta, tu, tv, depth, count,
                wu_out, wv_out, wt_out, ws_out, force_out, mean_out, side_out, counts_out,
                wide_north, wide_south, wide_side, force_north, force_south, force_side,
                cube, one_s, two_s, slope, edges, wu, wv, wt, ws, own_cols, fold, force_fold,
                flat_in, count_in, force, level_mean, side_cols, counts, blank,
                load_sem, send_sem, recv_sem, store_sem):
    at = places(n_row)
    fields = (u, v, t, s)
    four = range(STRIPS)

    def load(f, c, sem):
        return pltpu.make_async_copy(fields[f].at[:, :, pl.ds(LANES * c, LANES)], cube.at[f, c, pl.ds(1, LEV), pl.ds(0, ROWS), :], sem)

    outer = [[load(f, c, load_sem.at[2 * f + e]) for e, c in enumerate((0, STRIPS - 1))] for f in four]
    inner_sem, flat_sem, count_sem = load_sem.at[9], load_sem.at[10], load_sem.at[11]
    fetch_count = pltpu.make_async_copy(count, count_in, count_sem)
    fetch_count.start()
    for pair in outer:
        for copy in pair:
            copy.start()
    for f in (2, 3, 0, 1):
        for c in range(1, STRIPS - 1):
            load(f, c, load_sem.at[8 + (f < 2)]).start()
    for f, src in enumerate((eta, tu, tv, depth)):
        pltpu.make_async_copy(src, flat_in.at[f], flat_sem).start()
    barrier = meet(at)
    lane = lane_index()
    at_first, at_last = lane == 0, lane == LANES - 1
    zero = jnp.zeros((SUB, LANES), F32)
    line = jnp.zeros((1, LANES), F32)
    fetch_count.wait()
    for c in four:
        counts[c, SUB:SUB + ROWS, :] = count_in[:, c * LANES:(c + 1) * LANES].astype(F32)
    await_meet(barrier, at)
    slot = iter(range(LANES))

    def plan(where, region, *pairs):
        i = next(slot)
        copies = [remote(src, dst, send_sem.at[i], recv_sem.at[i], at[where]) for src, dst in pairs]
        return copies, remote(region, region, send_sem.at[i], recv_sem.at[i], at[where])

    def begin(plans):
        for copies, _ in plans:
            for copy in copies:
                copy.start()

    def start(north, south, side=()):
        pl.when(at['has_north'])(lambda: begin(north))
        pl.when(at['has_south'])(lambda: begin(south))
        begin(side)

    def received(plans):
        for _, waiter in plans:
            waiter.wait_recv()

    def sent(plans):
        for _, waiter in plans:
            waiter.wait_send()

    def arrive(north, south, side=()):
        received(side)
        pl.when(at['has_north'])(lambda: received(south))
        pl.when(at['has_south'])(lambda: received(north))

    def leave(north, south, side=()):
        sent(side)
        pl.when(at['has_north'])(lambda: sent(north))
        pl.when(at['has_south'])(lambda: sent(south))

    def row_region(level, row):
        return cube.at[:, :, pl.ds(level, LEV), pl.ds(row, 1), :]

    def row_pairs(source, level, row):
        return [(fields[f].at[:, pl.ds(source, 1), pl.ds(LANES * c, LANES)], cube.at[f, c, pl.ds(level, LEV), pl.ds(row, 1), :])
                for f in four for c in four]

    rows_north = [plan('north', row_region(0, PITCH - 1), *row_pairs(ROWS - 1, 0, PITCH - 1))]
    rows_south = [plan('south', row_region(1, ROWS), *row_pairs(0, 1, ROWS))]
    low_tile, high_tile = counts.at[:, pl.ds(0, SUB), :], counts.at[:, pl.ds(SUB + ROWS, SUB), :]
    count_north = [plan('north', low_tile, (counts.at[:, pl.ds(ROWS, SUB), :], low_tile))]
    count_south = [plan('south', high_tile, (counts.at[:, pl.ds(SUB, SUB), :], high_tile))]
    start(count_north + rows_north, count_south + rows_south)

    half_lane = lane >> 1
    sides = []
    for f in four:
        for copy in outer[f]:
            copy.wait()

        def pack(tile, _):
            rows = pl.ds(pl.multiple_of(SUB * tile, SUB), SUB)
            packed = zero
            for k in range(LEV + 1 if f == 0 else LEV):
                if k < LEV:
                    first, last = cube[f, 0, k + 1, rows, :], cube[f, STRIPS - 1, k + 1, rows, :]
                else:
                    lower = pl.ds(pl.multiple_of(SUB * tile + SUB, SUB), SUB)
                    first, last = counts[0, lower, :], counts[STRIPS - 1, lower, :]
                both = pltpu.roll(jnp.where(at_first, first, last), 2 * k + 1, 1)
                packed = jnp.where(half_lane == k, both, packed)
            own_cols[f, rows, :] = packed
            return 0

        lax.fori_loop(0, TILES, pack, 0)
        target = side_cols.at[f, pl.ds(SUB, ROWS), :]
        sides.append(plan('side', target, (own_cols.at[f], target)))
        begin(sides[-1:])
    high_u, low_v = side_cols.at[0, pl.ds(SUB + ROWS, SUB), :], side_cols.at[1, pl.ds(0, SUB), :]
    corner_south = [plan('south_side', high_u, (own_cols.at[0, pl.ds(0, SUB), :], high_u))]
    corner_north = [plan('north_side', low_v, (own_cols.at[1, pl.ds(ROWS - SUB, SUB), :], low_v))]
    start(corner_north, corner_south)

    def clear(level, row):
        def body(k, _):
            for f in four:
                for c in four:
                    cube[f, c, k + level, pl.ds(row, 1), :] = line
            return 0

        lax.fori_loop(0, LEV, body, 0)

    narrow = blank.at[:, :, pl.ds(0, LANES)]
    pair = pl.ds(0, 2)
    low_rows, high_rows = pl.ds(0, REACH), pl.ds(ROWS - REACH, REACH)
    far_rows = pl.ds(REACH + ROWS, REACH)

    def blanks(wide, forced, rows):
        targets = ((blank, wide), (narrow, wide_side.at[:, rows, :]), (blank.at[pair], forced), (blank.at[pair, :, pl.ds(0, LANES)], force_side.at[:, rows, :]))
        return [pltpu.make_async_copy(src, dst, load_sem.at[12 + i]) for i, (src, dst) in enumerate(targets)]

    @pl.when(jnp.logical_not(at['has_north']))
    def _():
        clear(1, ROWS)
        counts[:, SUB + ROWS:, :] = jnp.zeros((STRIPS, SUB, LANES), F32)
        side_cols[:, SUB + ROWS:, :] = jnp.zeros((STRIPS, SUB, LANES), F32)
        blank[...] = jnp.zeros_like(blank)
        for copy in blanks(wide_north, force_north, far_rows):
            copy.start()

    @pl.when(jnp.logical_not(at['has_south']))
    def _():
        clear(0, PITCH - 1)
        counts[:, :SUB, :] = jnp.zeros((STRIPS, SUB, LANES), F32)
        side_cols[:, :SUB, :] = jnp.zeros((STRIPS, SUB, LANES), F32)
        blank[...] = jnp.zeros_like(blank)
        for copy in blanks(wide_south, force_south, low_rows):
            copy.start()

    half_scale = 0.5 * BC_GRAVITY / LEV
    scale = 0.5 * TIME_STEP

    def density(sal, tem):
        return (half_scale * CONTRACT_S) * sal - (half_scale * EXPAND_T) * tem

    def interior(f, sem):
        region = cube.at[pl.ds(f, 2), pl.ds(1, STRIPS - 2), pl.ds(1, LEV), pl.ds(0, ROWS), :]
        return pltpu.make_async_copy(region, region, sem)

    rows_flat = (LEV + 1) * PITCH
    uf, vf, tf, sf = [cube.at[f].reshape(STRIPS, rows_flat, LANES) for f in four]
    pf, bf = [ref.reshape(STRIPS, rows_flat, LANES) for ref in (one_s, two_s)]
    stack = lax.broadcasted_iota(jnp.int32, (STRIPS, SUB, LANES), 2)
    first_lanes, last_lanes = stack == 0, stack == LANES - 1
    none = jnp.zeros((STRIPS, SUB, LANES), F32)
    interior(2, load_sem.at[8]).wait()

    def pressure(tile, _):
        acc = none
        for k in range(LEV):
            here = level_rows(tile, k)
            rho = density(sf[:, here, :], tf[:, here, :])
            pp = acc + rho
            acc = pp + rho
            pf[:, here, :] = pp
            slope[tile, k] = pp - east_stack(pp, zero, first_lanes)
        return 0

    lax.fori_loop(0, TILES, pressure, 0)

    for f in four:
        received(sides[f:f + 1])

        def spread(tile, _):
            unpack(side_cols, edges, f, pl.ds(pl.multiple_of(SUB * tile, SUB), SUB))
            return 0

        lax.fori_loop(1, TILES + 1, spread, 0)
    arrive(count_north + corner_north, count_south + corner_south)
    unpack(side_cols, edges, 0, pl.ds(SUB + ROWS, SUB))
    unpack(side_cols, edges, 1, pl.ds(0, SUB))
    interior(0, inner_sem).wait()
    low_half = lax.broadcasted_iota(jnp.int32, (ROWS, LANES), 1) < LANES // 2
    pltpu.make_async_copy(flat_in, flat_in, flat_sem).wait()
    for f in four:
        fold[f] = jnp.where(low_half, flat_in[f, :, :LANES], flat_in[f, :, COLS - LANES:])
    arrive(rows_north, rows_south)
    leave(rows_north, rows_south)
    side_low, side_high = wide_side.at[:, low_rows, :], wide_side.at[:, far_rows, :]
    side_mid = wide_side.at[:, pl.ds(REACH, ROWS), :]
    wide_up = [plan('north', wide_south, (flat_in.at[:, high_rows, :], wide_south)),
               plan('north_side', side_low, (fold.at[:, high_rows, :], side_low))]
    wide_down = [plan('south', wide_north, (flat_in.at[:, low_rows, :], wide_north)),
                 plan('south_side', side_high, (fold.at[:, low_rows, :], side_high))]
    wide_across = [plan('side', side_mid, (fold, side_mid))]
    start(wide_up, wide_down, wide_across)
    pivot, _ = tables(VISC_R)
    acc = none
    for k in range(LEV):
        spot = level_rows(TILES, k)
        uu = uf[:, spot, :]
        bf[:, spot, :] = uu + west_stack(uu, edges[0, k, pl.ds(SUB + ROWS, SUB), :], last_lanes)
        rho = density(sf[:, spot, :], tf[:, spot, :])
        pf[:, spot, :] = acc + rho
        acc = (acc + rho) + rho

    def momentum(step, _):
        tile = TILES - 1 - step
        _, nu, nv = face_counts(counts, side_cols.at[0], tile)
        row_pos = (at['row'] * ROWS + SUB * tile + lax.broadcasted_iota(jnp.int32, (STRIPS, SUB, LANES), 1)).astype(F32)
        fu = 0.25 * (CORIO_F0 + CORIO_BETA * ((row_pos + 0.5) / (ROWS * n_row) - 0.5))
        fv = 0.25 * (CORIO_F0 + CORIO_BETA * ((row_pos + 1.0) / (ROWS * n_row) - 0.5))
        out_rows = pl.ds(pl.multiple_of(SUB * tile, SUB), SUB)
        mid_rows = pl.ds(pl.multiple_of(SUB * tile + SUB, SUB), SUB)
        acc_e = zero
        xu, xv, sum_du, sum_dv, sum_su, sum_sv = (none,) * 6
        for k in range(LEV):
            here, up, below = [level_rows(tile, k, step) for step in (0, 1, -1)]
            uu, vv = uf[:, here, :], vf[:, here, :]
            v_south = vf[:, below, :]
            edge_u, edge_v = edges[0, k, mid_rows, :], edges[1, k, mid_rows, :]
            u_west = west_stack(uu, edge_u, last_lanes)
            u_east = east_stack(uu, edge_u, first_lanes)
            v_west = west_stack(vv, edge_v, last_lanes)
            v_east = east_stack(vv, edge_v, first_lanes)
            pair_v = vv + v_south
            pair_ve = east_stack(pair_v, edge_v + edges[1, k, pl.ds(SUB * tile + SUB - 1, SUB), :], first_lanes)
            rho_e = pltpu.roll(density(edges[3, k, mid_rows, :], edges[2, k, mid_rows, :]), LANES - 1, 1)
            p_edge = acc_e + rho_e
            acc_e = p_edge + rho_e
            pp = pf[:, here, :]
            fall = slope[tile, k]
            fall = jnp.concatenate([fall[:-1], jnp.where(at_last, pp[-1] - p_edge, fall[-1])[None]], axis=0)
            pair_u = uu + u_west
            bf[:, here, :] = pair_u
            v4 = pair_v + pair_ve
            u4 = pair_u + bf[:, up, :]
            du = v4 * (fu - 0.125 * (uf[:, up, :] - uf[:, below, :])) - 0.5 * uu * (u_east - u_west) + fall
            dv = (pp - pf[:, up, :]) - u4 * (fv + 0.125 * (v_east - v_west)) - 0.5 * vv * (vf[:, up, :] - v_south)
            us, vs = uu + du, vv + dv
            on_u, on_v = nu > k, nv > k
            sum_du += jnp.where(on_u, du, 0.0)
            sum_dv += jnp.where(on_v, dv, 0.0)
            sum_su += jnp.where(on_u, us, 0.0)
            sum_sv += jnp.where(on_v, vs, 0.0)
            xu = us * (1.0 / pivot[k]) + xu * (VISC_R / pivot[k])
            xv = vs * (1.0 / pivot[k]) + xv * (VISC_R / pivot[k])
            wu[tile, k] = xu
            wv[tile, k] = xv
        inv_u = 1.0 / jnp.maximum(nu, 1.0)
        inv_v = 1.0 / jnp.maximum(nv, 1.0)
        for c in four:
            lanes = pl.ds(LANES * c, LANES)
            force[0, out_rows, lanes] = (sum_du * inv_u)[c]
            force[1, out_rows, lanes] = (sum_dv * inv_v)[c]
            level_mean[0, out_rows, lanes] = (sum_su * inv_u)[c]
            level_mean[1, out_rows, lanes] = (sum_sv * inv_v)[c]
        pltpu.make_async_copy(wu.at[tile], wu_out.at[tile], store_sem.at[0]).start()
        pltpu.make_async_copy(wv.at[tile], wv_out.at[tile], store_sem.at[1]).start()
        return 0

    lax.fori_loop(0, TILES, momentum, 0)

    for f in range(2):
        force_fold[f] = jnp.where(low_half, force[f, :, :LANES], force[f, :, COLS - LANES:])
    side_low, side_high = force_side.at[:, low_rows, :], force_side.at[:, far_rows, :]
    side_mid = force_side.at[:, pl.ds(REACH, ROWS), :]
    force_up = [plan('north', force_south, (force.at[:, high_rows, :], force_south)),
                plan('north_side', side_low, (force_fold.at[:, high_rows, :], side_low))]
    force_down = [plan('south', force_north, (force.at[:, low_rows, :], force_north)),
                  plan('south_side', side_high, (force_fold.at[:, low_rows, :], side_high))]
    force_across = [plan('side', side_mid, (force_fold, side_mid))]
    start(force_up, force_down, force_across)
    extras = [pltpu.make_async_copy(src, dst, store_sem.at[4 + i])
              for i, (src, dst) in enumerate(((force, force_out), (level_mean, mean_out), (side_cols.at[0], side_out), (counts, counts_out)))]
    for copy in extras:
        copy.start()

    ftf, fsf = pf, bf
    pivot, final = tables(DIFF_R)

    south_count = jnp.minimum(counts[:, pl.ds(0, SUB), :], counts[:, pl.ds(1, SUB), :])
    for k in range(LEV):
        here, up = level_rows(-1, k), level_rows(-1, k, 1)
        hv = jnp.where(south_count > k, scale * vf[:, here, :], 0.0)
        ftf[:, here, :] = hv * (tf[:, here, :] + tf[:, up, :])
        fsf[:, here, :] = hv * (sf[:, here, :] + sf[:, up, :])

    def tracers(tile, _):
        mid, nu, nv = face_counts(counts, side_cols.at[0], tile)
        out_rows = pl.ds(pl.multiple_of(SUB * tile, SUB), SUB)
        mid_rows = pl.ds(pl.multiple_of(SUB * tile + SUB, SUB), SUB)
        west_count = jnp.minimum(pltpu.roll(side_cols[0, mid_rows, :], LANES - 1 - 2 * LEV, 1), pltpu.roll(counts[0, mid_rows, :], LANES - 1, 1))
        xt, xs = none, none
        for k in range(LEV):
            here, up, below = [level_rows(tile, k, step) for step in (0, 1, -1)]
            hu = jnp.where(nu > k, scale * uf[:, here, :], 0.0)
            hv = jnp.where(nv > k, scale * vf[:, here, :], 0.0)
            hw = west_stack(hu, jnp.where(west_count > k, scale * edges[0, k, mid_rows, :], 0.0), last_lanes)
            inverse = jnp.where(mid > k + 1, 1.0 / pivot[k], 1.0 / final[k]) if k < LEV - 1 else 1.0 / final[k]

            def advance(flat, flux, which, x, w):
                q = flat[:, here, :]
                edge = edges[which, k, mid_rows, :]
                flux_e = hu * (q + east_stack(q, edge, first_lanes))
                flux_w = hw * (q + west_stack(q, edge, last_lanes))
                flux_n = hv * (q + flat[:, up, :])
                flux[:, here, :] = flux_n
                new = q - ((flux_e - flux_w) + (flux_n - flux[:, below, :]))
                x = (new + DIFF_R * x) * inverse
                w[tile, k] = jnp.where(mid > k, x, new)
                return x

            xt = advance(tf, ftf, 2, xt, wt)
            xs = advance(sf, fsf, 3, xs, ws)
        pltpu.make_async_copy(wt.at[tile], wt_out.at[tile], store_sem.at[2]).start()
        pltpu.make_async_copy(ws.at[tile], ws_out.at[tile], store_sem.at[3]).start()
        return 0

    lax.fori_loop(0, TILES, tracers, 0)
    for i, (src, dst) in enumerate(((wu, wu_out), (wv, wv_out), (wt, wt_out), (ws, ws_out))):
        pltpu.make_async_copy(src, dst, store_sem.at[i]).wait()
    for copy in extras:
        copy.wait()
    leave(count_north + corner_north, count_south + corner_south, sides)
    for group in ((wide_up, wide_down, wide_across), (force_up, force_down, force_across)):
        arrive(*group)
        leave(*group)

    @pl.when(jnp.logical_not(at['has_north']))
    def _():
        for copy in blanks(wide_north, force_north, far_rows):
            copy.wait()

    @pl.when(jnp.logical_not(at['has_south']))
    def _():
        for copy in blanks(wide_south, force_south, low_rows):
            copy.wait()


def fast_kernel(n_row, n_sub, weights, wu_in, wv_in, wt_in, ws_in, eta, tu, tv, depth, wide_north, wide_south, wide_side,
                force, force_north, force_south, force_side, level_mean, counts, side_cols,
                eta_out, tu_out, tv_out, u_out, v_out, t_out, s_out,
                e_s, u_s, v_s, b_s, d_s, cu_s, cv_s, bu_s, bv_s, fu_s, fv_s, bar_u, bar_v, wu, wv, wt, ws, u_new, v_new, t_new, s_new, load_sem, store_sem):
    row = lax.axis_index('row')
    def fetch(tile):
        return [pltpu.make_async_copy(src.at[tile], dst.at[tile], load_sem.at[i, tile])
                for i, (src, dst) in enumerate(((wt_in, wt), (ws_in, ws), (wu_in, wu), (wv_in, wv)))]

    def put(tile, i, src, dst):
        rows = pl.ds(pl.multiple_of(SUB * tile, SUB), SUB)
        return pltpu.make_async_copy(src.at[:, rows, :], dst.at[:, rows, :], store_sem.at[i, tile])

    for part in (slice(0, 2), slice(2, 4)):
        for tile in range(TILES):
            for copy in fetch(tile)[part]:
                copy.start()
    lane = lane_index()
    at_first, at_last = lane == 0, lane == LANES - 1
    five = range(STRIPS + 1)
    dt_fast = TIME_STEP / n_sub
    total = ROWS * n_row
    zero = jnp.zeros((SUB, LANES), F32)

    def page(tile, c, offset=0):
        return pl.ds(c * PAGE + SUB + SUB * tile + offset, SUB)

    def gather(f, own, north, south, side, tile, c):
        if c == STRIPS:
            return side[f, SUB * tile:SUB * tile + SUB, :]
        lanes = slice(c * LANES, (c + 1) * LANES)
        if tile < REACH // SUB:
            return south[f, SUB * tile:SUB * tile + SUB, lanes]
        if tile < (REACH + ROWS) // SUB:
            return own[SUB * tile - REACH:SUB * tile - REACH + SUB, lanes]
        start = SUB * tile - REACH - ROWS
        return north[f, start:start + SUB, lanes]

    for ref in (e_s, u_s, v_s, b_s, d_s):
        for c in five:
            ref[page(-1, c), :] = zero
            ref[page(EXT_TILES, c), :] = zero
    for tile in range(EXT_TILES):
        for c in five:
            at = page(tile, c)
            e_s[at, :] = gather(0, eta, wide_north, wide_south, wide_side, tile, c)
            u_s[at, :] = dt_fast * gather(1, tu, wide_north, wide_south, wide_side, tile, c)
            v_s[at, :] = dt_fast * gather(2, tv, wide_north, wide_south, wide_side, tile, c)
            d_s[at, :] = gather(3, depth, wide_north, wide_south, wide_side, tile, c)
            bu_s[at, :] = gather(0, force.at[0], force_north, force_south, force_side, tile, c)
            bv_s[at, :] = gather(1, force.at[1], force_north, force_south, force_side, tile, c)
    for tile in range(EXT_TILES):
        place = row * ROWS + (SUB * tile - REACH) + lax.broadcasted_iota(jnp.int32, (SUB, LANES), 0)
        inside = jnp.logical_and(place >= 0, place < total)
        inside_v = jnp.logical_and(place >= 0, place < total - 1)
        row_pos = place.astype(F32)
        fu = (0.25 * dt_fast) * (CORIO_F0 + CORIO_BETA * ((row_pos + 0.5) / total - 0.5))
        fv = (0.25 * dt_fast) * (CORIO_F0 + CORIO_BETA * ((row_pos + 1.0) / total - 0.5))
        fu_s[SUB * tile:SUB * tile + SUB, :] = jnp.where(inside, fu, 0.0)
        fv_s[SUB * tile:SUB * tile + SUB, :] = jnp.where(inside_v, fv, 0.0)
        deep = [d_s[page(tile, c), :] for c in five]
        deep_e = east_of(deep, deep[0], at_first)
        for c in five:
            at = page(tile, c)
            hu = jnp.where(inside, 0.5 * (deep[c] + deep_e[c]), 0.0)
            hv = jnp.where(inside_v, 0.5 * (deep[c] + d_s[page(tile, c, 1), :]), 0.0)
            cu_s[at, :] = (dt_fast * dt_fast * GRAVITY) * hu
            cv_s[at, :] = (dt_fast * dt_fast * GRAVITY) * hv
            bu_s[at, :] = (dt_fast * dt_fast / TIME_STEP) * hu * bu_s[at, :]
            bv_s[at, :] = (dt_fast * dt_fast / TIME_STEP) * hv * bv_s[at, :]
    bar_u[...] = jnp.zeros_like(bar_u)
    bar_v[...] = jnp.zeros_like(bar_v)

    def subcycle(n, low, high):
        weight = weights[n]
        for tile in range(high - 1, low - 1, -1):
            uu = [u_s[page(tile, c), :] for c in five]
            vv = [v_s[page(tile, c), :] for c in five]
            v_south = [v_s[page(tile, c, -1), :] for c in five]
            part = [e_s[page(tile, c), :] - (uu[c] + (vv[c] - v_south[c])) for c in five]
            pair_v = [vv[c] + v_south[c] for c in five]
            u_west = west_of(uu, uu[-1], at_last)
            part_e = east_of(part, part[0], at_first)
            pair_ve = east_of(pair_v, pair_v[0], at_first)
            fu = fu_s[SUB * tile:SUB * tile + SUB, :]
            fv = fv_s[SUB * tile:SUB * tile + SUB, :]
            for c in five:
                at, up = page(tile, c), page(tile, c, 1)
                new = part[c] + u_west[c]
                pair_u = uu[c] + u_west[c]
                e_s[at, :] = new
                b_s[at, :] = pair_u
                u_next = uu[c] + ((fu * (pair_v[c] + pair_ve[c]) + bu_s[at, :]) - cu_s[at, :] * ((part_e[c] + uu[c]) - new))
                v_next = vv[c] + ((bv_s[at, :] - fv * (pair_u + b_s[up, :])) - cv_s[at, :] * (e_s[up, :] - new))
                u_s[at, :] = u_next
                v_s[at, :] = v_next
                if c < STRIPS and REACH // SUB <= tile < (REACH + ROWS) // SUB:
                    own = tile - REACH // SUB
                    bar_u[own, c] += weight * u_next
                    bar_v[own, c] += weight * v_next

    def wall_row():
        for tile in range(EXT_TILES):
            place = row * ROWS + (SUB * tile - REACH) + lax.broadcasted_iota(jnp.int32, (SUB, LANES), 0)
            wet = jnp.logical_and(place >= 0, place < total - 1)
            for c in five:
                at = page(tile, c)
                v_s[at, :] = jnp.where(wet, v_s[at, :], 0.0)
                if c < STRIPS and REACH // SUB <= tile < (REACH + ROWS) // SUB:
                    own = tile - REACH // SUB
                    bar_v[own, c] = jnp.where(wet, bar_v[own, c], 0.0)

    four = range(STRIPS)
    inner, _ = tables(DIFF_R)

    def tracers(tile, _):
        for copy in fetch(tile)[:2]:
            copy.wait()
        mid = [counts[c, pl.ds(pl.multiple_of(SUB * tile + SUB, SUB), SUB), :] for c in four]
        out_rows = pl.ds(pl.multiple_of(SUB * tile, SUB), SUB)
        xt, xs = [zero] * STRIPS, [zero] * STRIPS
        for k in range(LEV - 1, -1, -1):
            for c in four:
                on = mid[c] > k
                lanes = pl.ds(LANES * c, LANES)

                def solve(w, x, out):
                    value = w[tile, k, c]
                    full = value + (DIFF_R / inner[k]) * x[c]
                    out[k, out_rows, lanes] = jnp.where(on, full, value)
                    x[c] = jnp.where(on, full, 0.0)

                solve(wt, xt, t_new)
                solve(ws, xs, s_new)
        put(tile, 2, t_new, t_out).start()
        put(tile, 3, s_new, s_out).start()
        return 0

    n = 0
    while n < n_sub:
        spread = -(-(n_sub - n) // SUB)
        stop = n_sub - SUB * (spread - 1)
        low, high = REACH // SUB - spread, (REACH + ROWS) // SUB + spread

        def some(i, _, low=low, high=high, first=(n == 0)):
            subcycle(i, low, high)
            if first:
                pl.when(i == 0)(wall_row)
            return 0

        lax.fori_loop(n, stop, some, 0)
        if n == 0:
            lax.fori_loop(0, TILES, tracers, 0)
        n = stop

    pivot, final = tables(VISC_R)
    for tile in range(TILES):
        for c in four:
            at = page(tile + REACH // SUB, c)
            rows, lanes = pl.ds(SUB * tile, SUB), pl.ds(LANES * c, LANES)
            eta_out[rows, lanes] = e_s[at, :]
            tu_out[rows, lanes] = u_s[at, :] * (1.0 / dt_fast)
            tv_out[rows, lanes] = v_s[at, :] * (1.0 / dt_fast)

    def tile_step(tile, _):
        for copy in fetch(tile)[2:]:
            copy.wait()
        _, nu, nv = face_counts(counts, side_cols, tile)
        out_rows = pl.ds(pl.multiple_of(SUB * tile, SUB), SUB)
        add_u, add_v = [], []
        for c in four:
            at = pl.ds(c * PAGE + SUB + REACH + SUB * tile, SUB)
            lanes = pl.ds(LANES * c, LANES)
            deep_u = cu_s[at, :] * (1.0 / (dt_fast * GRAVITY))
            deep_v = cv_s[at, :] * (1.0 / (dt_fast * GRAVITY))
            deep_v = jnp.where(nv[c] > 0, deep_v, 1.0)
            add_u.append(bar_u[tile, c] / deep_u - level_mean[0, out_rows, lanes])
            add_v.append(bar_v[tile, c] / deep_v - level_mean[1, out_rows, lanes])
        xu, xv = [zero] * STRIPS, [zero] * STRIPS
        for k in range(LEV - 1, -1, -1):
            ratio, bottom = VISC_R / pivot[k], pivot[k] / final[k]
            for c in four:
                lanes = pl.ds(LANES * c, LANES)

                def solve(w, x, n, add, out):
                    value = w[tile, k, c]
                    last = value * bottom
                    if k < LEV - 1:
                        x[c] = jnp.where(n[c] > k + 1, value + ratio * x[c], last)
                    else:
                        x[c] = last
                    out[k, out_rows, lanes] = jnp.where(n[c] > k, x[c] + add[c], 0.0)

                solve(wu, xu, nu, add_u, u_new)
                solve(wv, xv, nv, add_v, v_new)
        put(tile, 0, u_new, u_out).start()
        put(tile, 1, v_new, v_out).start()
        return 0

    lax.fori_loop(0, TILES, tile_step, 0)
    for tile in range(TILES):
        for i, (src, dst) in enumerate(((u_new, u_out), (v_new, v_out), (t_new, t_out), (s_new, s_out))):
            put(tile, i, src, dst).wait()


def solution(mesh):
    n_row = mesh.shape['row']
    hbm = pl.BlockSpec(memory_space=pltpu.HBM)
    vmem = pl.BlockSpec(memory_space=pltpu.VMEM)
    smem = pl.BlockSpec(memory_space=pltpu.SMEM)
    dma = pltpu.SemaphoreType.DMA
    strip = pltpu.VMEM((STRIPS, LEV + 1, PITCH, LANES), F32)
    whole = pltpu.VMEM((LEV, ROWS, COLS), F32)
    column = pltpu.VMEM((TILES, LEV, STRIPS, SUB, LANES), F32)
    extended = pltpu.VMEM(((STRIPS + 1) * PAGE, LANES), F32)

    def shape(*dims):
        return jax.ShapeDtypeStruct(dims, F32)

    def call(body, ins, outs, shapes, scratch, **params):
        return pl.pallas_call(body, out_shape=shapes, in_specs=ins, out_specs=outs, scratch_shapes=scratch,
                              compiler_params=pltpu.CompilerParams(vmem_limit_bytes=VMEM_LIMIT, **params))

    def step(vel_u, vel_v, temp, salt, eta, tu, tv, depth, count, weights):
        n_sub = weights.shape[0]
        (wu, wv, wt, ws, force, level_mean, side_cols, counts, wide_north, wide_south, wide_side,
         force_north, force_south, force_side) = call(
            functools.partial(step_kernel, n_row), [hbm] * 9, [hbm] * 14,
            [shape(TILES, LEV, STRIPS, SUB, LANES)] * 4 + [shape(2, ROWS, COLS)] * 2
            + [shape(ROWS + 2 * SUB, LANES), shape(STRIPS, ROWS + 2 * SUB, LANES)]
            + [shape(4, REACH, COLS), shape(4, REACH, COLS), shape(4, EXT, LANES)]
            + [shape(2, REACH, COLS), shape(2, REACH, COLS), shape(2, EXT, LANES)],
            [pltpu.VMEM((4, STRIPS, LEV + 1, PITCH, LANES), F32)] + [strip] * 2 + [column] + [pltpu.VMEM((4, LEV, ROWS + 2 * SUB, LANES), F32)] + [column] * 4
            + [pltpu.VMEM((4, ROWS, LANES), F32)] * 2 + [pltpu.VMEM((2, ROWS, LANES), F32)]
            + [pltpu.VMEM((4, ROWS, COLS), F32), pltpu.VMEM((ROWS, COLS), jnp.int32)] + [pltpu.VMEM((2, ROWS, COLS), F32)] * 2
            + [pltpu.VMEM((4, ROWS + 2 * SUB, LANES), F32), pltpu.VMEM((STRIPS, ROWS + 2 * SUB, LANES), F32), pltpu.VMEM((4, REACH, COLS), F32)]
            + [dma((16,)), dma((20,)), dma((20,)), dma((8,))],
            collective_id=0, has_side_effects=True)(vel_u, vel_v, temp, salt, eta, tu, tv, depth, count)
        return call(
            functools.partial(fast_kernel, n_row, n_sub), [smem] + [hbm] * 4 + [vmem] * 14, [vmem] * 3 + [hbm] * 4,
            [shape(ROWS, COLS)] * 3 + [shape(LEV, ROWS, COLS)] * 4,
            [extended] * 9 + [pltpu.VMEM((EXT, LANES), F32)] * 2 + [pltpu.VMEM((TILES, STRIPS, SUB, LANES), F32)] * 2
            + [column] * 4 + [whole] * 4 + [dma((4, TILES)), dma((4, TILES))],
        )(weights, wu, wv, wt, ws, eta, tu, tv, depth, wide_north, wide_south, wide_side,
          force, force_north, force_south, force_side, level_mean, counts, side_cols)

    cube = P(None, 'row', 'col')
    flat = P('row', 'col')
    return jax.shard_map(step, mesh=mesh, in_specs=(cube, cube, cube, cube, flat, flat, flat, flat, flat, P()),
                         out_specs=(flat, flat, flat, cube, cube, cube, cube), check_vma=False)
```

```python
import functools

import jax
import jax.numpy as jnp
from jax import lax
from jax.experimental import pallas as pl
from jax.experimental.pallas import tpu as pltpu
from jax.sharding import PartitionSpec as P

TIME_STEP = 1.0
GRAVITY = 16.0
BC_GRAVITY = 4.0
EXPAND_T = 0.2
CONTRACT_S = 0.6
CORIO_F0 = 0.4
CORIO_BETA = 0.4
VISC_R = 2.0
DIFF_R = 0.5

LEV = 41
ROWS = 48
SUB = 8
COLS = 512
LANES = 128
STRIPS = COLS // LANES
TILES = ROWS // SUB
PITCH = 56
REACH = 32
EXT = ROWS + 2 * REACH
EXT_TILES = EXT // SUB
PAGE = EXT + 16
MESH = pl.DeviceIdType.MESH
F32 = jnp.float32
STEP_MIB, FAST_MIB = 35, 36


def tables(strength):
    inner, last, ratio = [], [], 0.0
    for level in range(LEV):
        low = strength if level else 0.0
        pivot = 1.0 + low + strength - low * ratio
        inner.append(pivot)
        last.append(1.0 + low - low * ratio)
        ratio = strength / pivot
    return inner, last


def lane_index():
    return lax.broadcasted_iota(jnp.int32, (SUB, LANES), 1)


def west_of(strips, edge, at_last):
    mixed = [jnp.where(at_last, edge if c == 0 else strips[c - 1], strips[c]) for c in range(len(strips))]
    return [pltpu.roll(x, 1, 1) for x in mixed]


def east_of(strips, edge, at_first):
    n = len(strips)
    mixed = [jnp.where(at_first, edge if c == n - 1 else strips[c + 1], strips[c]) for c in range(n)]
    return [pltpu.roll(x, LANES - 1, 1) for x in mixed]


def places(n_row):
    row = lax.axis_index('row')
    col = lax.axis_index('col')
    other = 1 - col
    has_north = row < n_row - 1
    has_south = row > 0
    return dict(
        row=row, has_north=has_north, has_south=has_south,
        side={'col': other, 'row': row},
        north={'col': col, 'row': row + 1}, south={'col': col, 'row': row - 1},
        north_side={'col': other, 'row': row + 1}, south_side={'col': other, 'row': row - 1})


def meet(at):
    barrier = pltpu.get_barrier_semaphore()
    pl.semaphore_signal(barrier, inc=1, device_id=at['side'], device_id_type=MESH)

    @pl.when(at['has_north'])
    def _():
        pl.semaphore_signal(barrier, inc=1, device_id=at['north'], device_id_type=MESH)
        pl.semaphore_signal(barrier, inc=1, device_id=at['north_side'], device_id_type=MESH)

    @pl.when(at['has_south'])
    def _():
        pl.semaphore_signal(barrier, inc=1, device_id=at['south'], device_id_type=MESH)
        pl.semaphore_signal(barrier, inc=1, device_id=at['south_side'], device_id_type=MESH)

    return barrier


def await_meet(barrier, at):
    pl.semaphore_wait(barrier, 1 + 2 * at['has_north'].astype(jnp.int32) + 2 * at['has_south'].astype(jnp.int32))


def remote(src, dst, send, recv, where):
    return pltpu.make_async_remote_copy(src_ref=src, dst_ref=dst, send_sem=send, recv_sem=recv, device_id=where, device_id_type=MESH)


def level_rows(tile, k, offset=0):
    return pl.ds(SUB * tile + (PITCH * (k + 1) + offset), SUB)


def west_stack(strips, edge, at_last):
    return pltpu.roll(jnp.where(at_last, jnp.concatenate([edge[None], strips[:-1]], axis=0), strips), 1, 2)


def east_stack(strips, edge, at_first):
    return pltpu.roll(jnp.where(at_first, jnp.concatenate([strips[1:], edge[None]], axis=0), strips), LANES - 1, 2)


def face_counts(counts, side, tile):
    rows = SUB * tile + SUB
    mid = counts[:, pl.ds(rows, SUB), :]
    north = counts[:, pl.ds(rows + 1, SUB), :]
    edge = pltpu.roll(side[pl.ds(rows, SUB), :], LANES - 1 - 2 * LEV, 1)
    at_first = lax.broadcasted_iota(jnp.int32, mid.shape, 2) == 0
    return mid, jnp.minimum(mid, east_stack(mid, edge, at_first)), jnp.minimum(mid, north)


def unpack(packed, edges, f, rows):
    for k in range(LEV):
        edges[f, k, rows, :] = pltpu.roll(packed[f, rows, :], LANES - 1 - 2 * k, 1)


def step_kernel(n_row, u, v, t, s, flat_in,
                wu, wv, wt, ws, force, level_mean, side_cols, counts,
                wide_north, wide_south, wide_side, force_north, force_south, force_side,
                cube, one_s, two_s, edges, own_cols, fold, force_fold,
                load_sem, send_sem, recv_sem):
    at = places(n_row)
    fields = (u, v, t, s)
    four = range(STRIPS)

    def load(f, c, sem):
        return pltpu.make_async_copy(fields[f].at[:, :, pl.ds(LANES * c, LANES)], cube.at[f, c, pl.ds(1, LEV), pl.ds(0, ROWS), :], sem)

    outer = [[load(f, c, load_sem.at[2 * f + e]) for e, c in enumerate((0, STRIPS - 1))] for f in four]
    inner_sem = load_sem.at[9]
    for pair in outer:
        for copy in pair:
            copy.start()
    barrier = meet(at)
    lane = lane_index()
    at_first, at_last = lane == 0, lane == LANES - 1
    zero = jnp.zeros((SUB, LANES), F32)
    line = jnp.zeros((1, LANES), F32)
    for c in four:
        counts[c, SUB:SUB + ROWS, :] = flat_in[4, :, c * LANES:(c + 1) * LANES]
    await_meet(barrier, at)
    slot = iter(range(LANES))

    def plan(where, region, *pairs):
        i = next(slot)
        copies = [remote(src, dst, send_sem.at[i], recv_sem.at[i], at[where]) for src, dst in pairs]
        return copies, remote(region, region, send_sem.at[i], recv_sem.at[i], at[where])

    def begin(plans):
        for copies, _ in plans:
            for copy in copies:
                copy.start()

    def start(north, south, side=()):
        pl.when(at['has_north'])(lambda: begin(north))
        pl.when(at['has_south'])(lambda: begin(south))
        begin(side)

    def received(plans):
        for _, waiter in plans:
            waiter.wait_recv()

    def sent(plans):
        for _, waiter in plans:
            waiter.wait_send()

    def arrive(north, south, side=()):
        received(side)
        pl.when(at['has_north'])(lambda: received(south))
        pl.when(at['has_south'])(lambda: received(north))

    def leave(north, south, side=()):
        sent(side)
        pl.when(at['has_north'])(lambda: sent(north))
        pl.when(at['has_south'])(lambda: sent(south))

    def row_region(level, row):
        return cube.at[:, :, pl.ds(level, LEV), pl.ds(row, 1), :]

    def row_pairs(source, level, row):
        return [(fields[f].at[:, pl.ds(source, 1), pl.ds(LANES * c, LANES)], cube.at[f, c, pl.ds(level, LEV), pl.ds(row, 1), :])
                for f in four for c in four]

    rows_north = [plan('north', row_region(0, PITCH - 1), *row_pairs(ROWS - 1, 0, PITCH - 1))]
    rows_south = [plan('south', row_region(1, ROWS), *row_pairs(0, 1, ROWS))]
    low_tile, high_tile = counts.at[:, pl.ds(0, SUB), :], counts.at[:, pl.ds(SUB + ROWS, SUB), :]
    count_north = [plan('north', low_tile, (counts.at[:, pl.ds(ROWS, SUB), :], low_tile))]
    count_south = [plan('south', high_tile, (counts.at[:, pl.ds(SUB, SUB), :], high_tile))]
    start(count_north + rows_north, count_south + rows_south)

    half_lane = lane >> 1
    sides = []
    for f in four:
        for copy in outer[f]:
            copy.wait()
        later = (f + 2) % 4
        for c in range(1, STRIPS - 1):
            load(later, c, load_sem.at[8 + (later < 2)]).start()

        def pack(tile, _):
            rows = pl.ds(pl.multiple_of(SUB * tile, SUB), SUB)
            packed = zero
            for k in range(LEV + 1 if f == 0 else LEV):
                if k < LEV:
                    first, last = cube[f, 0, k + 1, rows, :], cube[f, STRIPS - 1, k + 1, rows, :]
                else:
                    lower = pl.ds(pl.multiple_of(SUB * tile + SUB, SUB), SUB)
                    first, last = counts[0, lower, :], counts[STRIPS - 1, lower, :]
                both = pltpu.roll(jnp.where(at_first, first, last), 2 * k + 1, 1)
                packed = jnp.where(half_lane == k, both, packed)
            own_cols[f, rows, :] = packed
            return 0

        lax.fori_loop(0, TILES, pack, 0)
        target = side_cols.at[f, pl.ds(SUB, ROWS), :]
        sides.append(plan('side', target, (own_cols.at[f], target)))
        begin(sides[-1:])
    high_u, low_v = side_cols.at[0, pl.ds(SUB + ROWS, SUB), :], side_cols.at[1, pl.ds(0, SUB), :]
    corner_south = [plan('south_side', high_u, (own_cols.at[0, pl.ds(0, SUB), :], high_u))]
    corner_north = [plan('north_side', low_v, (own_cols.at[1, pl.ds(ROWS - SUB, SUB), :], low_v))]
    start(corner_north, corner_south)

    def clear(level, row):
        def body(k, _):
            for f in four:
                for c in four:
                    cube[f, c, k + level, pl.ds(row, 1), :] = line
            return 0

        lax.fori_loop(0, LEV, body, 0)

    low_rows, high_rows = pl.ds(0, REACH), pl.ds(ROWS - REACH, REACH)
    far_rows = pl.ds(REACH + ROWS, REACH)

    def walled(level, row, tile, wide, forced, rows):
        clear(level, row)
        counts[:, pl.ds(tile, SUB), :] = jnp.zeros((STRIPS, SUB, LANES), F32)
        side_cols[:, pl.ds(tile, SUB), :] = jnp.zeros((STRIPS, SUB, LANES), F32)
        wide[...] = jnp.zeros_like(wide)
        forced[...] = jnp.zeros_like(forced)
        wide_side[:, rows, :] = jnp.zeros((STRIPS, REACH, LANES), F32)
        force_side[:, rows, :] = jnp.zeros((2, REACH, LANES), F32)

    pl.when(jnp.logical_not(at['has_north']))(lambda: walled(1, ROWS, SUB + ROWS, wide_north, force_north, far_rows))
    pl.when(jnp.logical_not(at['has_south']))(lambda: walled(0, PITCH - 1, 0, wide_south, force_south, low_rows))
    half_scale = 0.5 * BC_GRAVITY / LEV
    scale = 0.5 * TIME_STEP

    def density(sal, tem):
        return (half_scale * CONTRACT_S) * sal - (half_scale * EXPAND_T) * tem

    def interior(f, sem):
        region = cube.at[pl.ds(f, 2), pl.ds(1, STRIPS - 2), pl.ds(1, LEV), pl.ds(0, ROWS), :]
        return pltpu.make_async_copy(region, region, sem)

    rows_flat = (LEV + 1) * PITCH
    uf, vf, tf, sf = [cube.at[f].reshape(STRIPS, rows_flat, LANES) for f in four]
    pf, bf = [ref.reshape(STRIPS, rows_flat, LANES) for ref in (one_s, two_s)]
    stack = lax.broadcasted_iota(jnp.int32, (STRIPS, SUB, LANES), 2)
    first_lanes, last_lanes = stack == 0, stack == LANES - 1
    none = jnp.zeros((STRIPS, SUB, LANES), F32)
    interior(2, load_sem.at[8]).wait()

    slope = wt

    def pressure(tile, _):
        acc = none
        for k in range(LEV):
            here = level_rows(tile, k)
            rho = density(sf[:, here, :], tf[:, here, :])
            pp = acc + rho
            acc = pp + rho
            pf[:, here, :] = pp
            slope[tile, k] = pp - east_stack(pp, zero, first_lanes)
        return 0

    lax.fori_loop(0, TILES, pressure, 0)

    for f in four:
        received(sides[f:f + 1])

        def spread(tile, _):
            unpack(side_cols, edges, f, pl.ds(pl.multiple_of(SUB * tile, SUB), SUB))
            return 0

        lax.fori_loop(1, TILES + 1, spread, 0)
    arrive(count_north + corner_north, count_south + corner_south)
    unpack(side_cols, edges, 0, pl.ds(SUB + ROWS, SUB))
    unpack(side_cols, edges, 1, pl.ds(0, SUB))
    interior(0, inner_sem).wait()
    low_half = lax.broadcasted_iota(jnp.int32, (ROWS, LANES), 1) < LANES // 2
    for f in four:
        fold[f] = jnp.where(low_half, flat_in[f, :, :LANES], flat_in[f, :, COLS - LANES:])
    side_low, side_high = wide_side.at[:, low_rows, :], wide_side.at[:, far_rows, :]
    side_mid = wide_side.at[:, pl.ds(REACH, ROWS), :]
    wide_up = [plan('north', wide_south, (flat_in.at[pl.ds(0, 4), high_rows, :], wide_south)),
               plan('north_side', side_low, (fold.at[:, high_rows, :], side_low))]
    wide_down = [plan('south', wide_north, (flat_in.at[pl.ds(0, 4), low_rows, :], wide_north)),
                 plan('south_side', side_high, (fold.at[:, low_rows, :], side_high))]
    wide_across = [plan('side', side_mid, (fold, side_mid))]
    start(wide_up, wide_down, wide_across)
    pivot, _ = tables(VISC_R)
    for k in range(LEV):
        spot = level_rows(TILES - 1, k)
        uu = uf[:, spot, :]
        bf[:, spot, :] = uu + west_stack(uu, edges[0, k, pl.ds(ROWS, SUB), :], last_lanes)

    def border_rows():
        arrive(rows_north, rows_south)
        acc = none
        for k in range(LEV):
            spot = level_rows(TILES, k)
            uu = uf[:, spot, :]
            bf[:, spot, :] = uu + west_stack(uu, edges[0, k, pl.ds(SUB + ROWS, SUB), :], last_lanes)
            rho = density(sf[:, spot, :], tf[:, spot, :])
            pf[:, spot, :] = acc + rho
            acc = (acc + rho) + rho

    def momentum(step, _):
        tile = (2 * TILES - 2 - step) % TILES
        pl.when(step == TILES - 2)(border_rows)
        _, nu, nv = face_counts(counts, side_cols.at[0], tile)
        row_pos = (at['row'] * ROWS + SUB * tile + lax.broadcasted_iota(jnp.int32, (STRIPS, SUB, LANES), 1)).astype(F32)
        fu = 0.25 * (CORIO_F0 + CORIO_BETA * ((row_pos + 0.5) / (ROWS * n_row) - 0.5))
        fv = 0.25 * (CORIO_F0 + CORIO_BETA * ((row_pos + 1.0) / (ROWS * n_row) - 0.5))
        out_rows = pl.ds(pl.multiple_of(SUB * tile, SUB), SUB)
        mid_rows = pl.ds(pl.multiple_of(SUB * tile + SUB, SUB), SUB)
        acc_e = zero
        xu, xv, sum_du, sum_dv, sum_su, sum_sv = (none,) * 6
        for k in range(LEV):
            here, up, below = [level_rows(tile, k, step) for step in (0, 1, -1)]
            uu, vv = uf[:, here, :], vf[:, here, :]
            v_south = vf[:, below, :]
            edge_u, edge_v = edges[0, k, mid_rows, :], edges[1, k, mid_rows, :]
            u_west = west_stack(uu, edge_u, last_lanes)
            u_east = east_stack(uu, edge_u, first_lanes)
            v_west = west_stack(vv, edge_v, last_lanes)
            v_east = east_stack(vv, edge_v, first_lanes)
            pair_v = vv + v_south
            pair_ve = east_stack(pair_v, edge_v + edges[1, k, pl.ds(SUB * tile + SUB - 1, SUB), :], first_lanes)
            rho_e = pltpu.roll(density(edges[3, k, mid_rows, :], edges[2, k, mid_rows, :]), LANES - 1, 1)
            p_edge = acc_e + rho_e
            acc_e = p_edge + rho_e
            pp = pf[:, here, :]
            fall = slope[tile, k]
            fall = jnp.concatenate([fall[:-1], jnp.where(at_last, pp[-1] - p_edge, fall[-1])[None]], axis=0)
            pair_u = uu + u_west
            bf[:, here, :] = pair_u
            v4 = pair_v + pair_ve
            u4 = pair_u + bf[:, up, :]
            du = v4 * (fu - 0.125 * (uf[:, up, :] - uf[:, below, :])) - 0.5 * uu * (u_east - u_west) + fall
            dv = (pp - pf[:, up, :]) - u4 * (fv + 0.125 * (v_east - v_west)) - 0.5 * vv * (vf[:, up, :] - v_south)
            us, vs = uu + du, vv + dv
            on_u, on_v = nu > k, nv > k
            sum_du += jnp.where(on_u, du, 0.0)
            sum_dv += jnp.where(on_v, dv, 0.0)
            sum_su += jnp.where(on_u, us, 0.0)
            sum_sv += jnp.where(on_v, vs, 0.0)
            xu = us * (1.0 / pivot[k]) + xu * (VISC_R / pivot[k])
            xv = vs * (1.0 / pivot[k]) + xv * (VISC_R / pivot[k])
            wu[tile, k] = xu
            wv[tile, k] = xv
        inv_u = 1.0 / jnp.maximum(nu, 1.0)
        inv_v = 1.0 / jnp.maximum(nv, 1.0)
        for c in four:
            lanes = pl.ds(LANES * c, LANES)
            force[0, out_rows, lanes] = (sum_du * inv_u)[c]
            force[1, out_rows, lanes] = (sum_dv * inv_v)[c]
            level_mean[0, out_rows, lanes] = (sum_su * inv_u)[c]
            level_mean[1, out_rows, lanes] = (sum_sv * inv_v)[c]
        return 0

    lax.fori_loop(0, TILES, momentum, 0)

    for f in range(2):
        force_fold[f] = jnp.where(low_half, force[f, :, :LANES], force[f, :, COLS - LANES:])
    side_low, side_high = force_side.at[:, low_rows, :], force_side.at[:, far_rows, :]
    side_mid = force_side.at[:, pl.ds(REACH, ROWS), :]
    force_up = [plan('north', force_south, (force.at[:, high_rows, :], force_south)),
                plan('north_side', side_low, (force_fold.at[:, high_rows, :], side_low))]
    force_down = [plan('south', force_north, (force.at[:, low_rows, :], force_north)),
                  plan('south_side', side_high, (force_fold.at[:, low_rows, :], side_high))]
    force_across = [plan('side', side_mid, (force_fold, side_mid))]
    start(force_up, force_down, force_across)
    ftf, fsf = pf, bf
    pivot, final = tables(DIFF_R)

    south_count = jnp.minimum(counts[:, pl.ds(0, SUB), :], counts[:, pl.ds(1, SUB), :])
    for k in range(LEV):
        here, up = level_rows(-1, k), level_rows(-1, k, 1)
        hv = jnp.where(south_count > k, scale * vf[:, here, :], 0.0)
        ftf[:, here, :] = hv * (tf[:, here, :] + tf[:, up, :])
        fsf[:, here, :] = hv * (sf[:, here, :] + sf[:, up, :])

    def tracers(tile, _):
        mid, nu, nv = face_counts(counts, side_cols.at[0], tile)
        out_rows = pl.ds(pl.multiple_of(SUB * tile, SUB), SUB)
        mid_rows = pl.ds(pl.multiple_of(SUB * tile + SUB, SUB), SUB)
        west_count = jnp.minimum(pltpu.roll(side_cols[0, mid_rows, :], LANES - 1 - 2 * LEV, 1), pltpu.roll(counts[0, mid_rows, :], LANES - 1, 1))
        xt, xs = none, none
        for k in range(LEV):
            here, up, below = [level_rows(tile, k, step) for step in (0, 1, -1)]
            hu = jnp.where(nu > k, scale * uf[:, here, :], 0.0)
            hv = jnp.where(nv > k, scale * vf[:, here, :], 0.0)
            hw = west_stack(hu, jnp.where(west_count > k, scale * edges[0, k, mid_rows, :], 0.0), last_lanes)
            inverse = jnp.where(mid > k + 1, 1.0 / pivot[k], 1.0 / final[k]) if k < LEV - 1 else 1.0 / final[k]

            def advance(flat, flux, which, x, w):
                q = flat[:, here, :]
                edge = edges[which, k, mid_rows, :]
                flux_e = hu * (q + east_stack(q, edge, first_lanes))
                flux_w = hw * (q + west_stack(q, edge, last_lanes))
                flux_n = hv * (q + flat[:, up, :])
                flux[:, here, :] = flux_n
                new = q - ((flux_e - flux_w) + (flux_n - flux[:, below, :]))
                x = (new + DIFF_R * x) * inverse
                w[tile, k] = jnp.where(mid > k, x, new)
                return x

            xt = advance(tf, ftf, 2, xt, wt)
            xs = advance(sf, fsf, 3, xs, ws)
        return 0

    lax.fori_loop(0, TILES, tracers, 0)
    leave(count_north + corner_north + rows_north, count_south + corner_south + rows_south, sides)
    for group in ((wide_up, wide_down, wide_across), (force_up, force_down, force_across)):
        arrive(*group)
        leave(*group)


def fast_kernel(n_row, n_sub, weights, flat_in, wu, wv, wt, ws, force, level_mean, side_cols, counts,
                wide_north, wide_south, wide_side, force_north, force_south, force_side,
                eta_out, tu_out, tv_out, u_out, v_out, t_out, s_out,
                flat_out, small_sem, e_s, u_s, v_s, b_s, d_s, cu_s, cv_s, bu_s, bv_s, fu_s, fv_s, bar_u, bar_v,
                u_new, v_new, t_new, s_new, store_sem):
    row = lax.axis_index('row')
    def put(tile, i, src, dst):
        rows = pl.ds(pl.multiple_of(SUB * tile, SUB), SUB)
        return pltpu.make_async_copy(src.at[:, rows, :], dst.at[:, rows, :], store_sem.at[i, tile])

    lane = lane_index()
    at_first, at_last = lane == 0, lane == LANES - 1
    five = range(STRIPS + 1)
    dt_fast = TIME_STEP / n_sub
    total = ROWS * n_row
    zero = jnp.zeros((SUB, LANES), F32)

    def page(tile, c, offset=0):
        return pl.ds(c * PAGE + SUB + SUB * tile + offset, SUB)

    def gather(f, own, north, south, side, tile, c):
        if c == STRIPS:
            return side[f, SUB * tile:SUB * tile + SUB, :]
        lanes = slice(c * LANES, (c + 1) * LANES)
        if tile < REACH // SUB:
            return south[f, SUB * tile:SUB * tile + SUB, lanes]
        if tile < (REACH + ROWS) // SUB:
            return own[SUB * tile - REACH:SUB * tile - REACH + SUB, lanes]
        start = SUB * tile - REACH - ROWS
        return north[f, start:start + SUB, lanes]

    for ref in (e_s, u_s, v_s, b_s, d_s):
        for c in five:
            ref[page(-1, c), :] = zero
            ref[page(EXT_TILES, c), :] = zero
    for tile in range(EXT_TILES):
        for c in five:
            at = page(tile, c)
            e_s[at, :] = gather(0, flat_in.at[0], wide_north, wide_south, wide_side, tile, c)
            u_s[at, :] = dt_fast * gather(1, flat_in.at[1], wide_north, wide_south, wide_side, tile, c)
            v_s[at, :] = dt_fast * gather(2, flat_in.at[2], wide_north, wide_south, wide_side, tile, c)
            d_s[at, :] = gather(3, flat_in.at[3], wide_north, wide_south, wide_side, tile, c)
            bu_s[at, :] = gather(0, force.at[0], force_north, force_south, force_side, tile, c)
            bv_s[at, :] = gather(1, force.at[1], force_north, force_south, force_side, tile, c)
    for tile in range(EXT_TILES):
        place = row * ROWS + (SUB * tile - REACH) + lax.broadcasted_iota(jnp.int32, (SUB, LANES), 0)
        inside = jnp.logical_and(place >= 0, place < total)
        inside_v = jnp.logical_and(place >= 0, place < total - 1)
        row_pos = place.astype(F32)
        fu = (0.25 * dt_fast) * (CORIO_F0 + CORIO_BETA * ((row_pos + 0.5) / total - 0.5))
        fv = (0.25 * dt_fast) * (CORIO_F0 + CORIO_BETA * ((row_pos + 1.0) / total - 0.5))
        fu_s[SUB * tile:SUB * tile + SUB, :] = jnp.where(inside, fu, 0.0)
        fv_s[SUB * tile:SUB * tile + SUB, :] = jnp.where(inside_v, fv, 0.0)
        deep = [d_s[page(tile, c), :] for c in five]
        deep_e = east_of(deep, deep[0], at_first)
        for c in five:
            at = page(tile, c)
            hu = jnp.where(inside, 0.5 * (deep[c] + deep_e[c]), 0.0)
            hv = jnp.where(inside_v, 0.5 * (deep[c] + d_s[page(tile, c, 1), :]), 0.0)
            cu_s[at, :] = (dt_fast * dt_fast * GRAVITY) * hu
            cv_s[at, :] = (dt_fast * dt_fast * GRAVITY) * hv
            bu_s[at, :] = (dt_fast * dt_fast / TIME_STEP) * hu * bu_s[at, :]
            bv_s[at, :] = (dt_fast * dt_fast / TIME_STEP) * hv * bv_s[at, :]
    bar_u[...] = jnp.zeros_like(bar_u)
    bar_v[...] = jnp.zeros_like(bar_v)

    def subcycle(n, low, high):
        weight = weights[n]
        for tile in range(high - 1, low - 1, -1):
            uu = [u_s[page(tile, c), :] for c in five]
            vv = [v_s[page(tile, c), :] for c in five]
            v_south = [v_s[page(tile, c, -1), :] for c in five]
            part = [e_s[page(tile, c), :] - (uu[c] + (vv[c] - v_south[c])) for c in five]
            pair_v = [vv[c] + v_south[c] for c in five]
            u_west = west_of(uu, uu[-1], at_last)
            part_e = east_of(part, part[0], at_first)
            pair_ve = east_of(pair_v, pair_v[0], at_first)
            fu = fu_s[SUB * tile:SUB * tile + SUB, :]
            fv = fv_s[SUB * tile:SUB * tile + SUB, :]
            for c in five:
                at, up = page(tile, c), page(tile, c, 1)
                new = part[c] + u_west[c]
                pair_u = uu[c] + u_west[c]
                e_s[at, :] = new
                b_s[at, :] = pair_u
                u_next = uu[c] + ((fu * (pair_v[c] + pair_ve[c]) + bu_s[at, :]) - cu_s[at, :] * ((part_e[c] + uu[c]) - new))
                v_next = vv[c] + ((bv_s[at, :] - fv * (pair_u + b_s[up, :])) - cv_s[at, :] * (e_s[up, :] - new))
                u_s[at, :] = u_next
                v_s[at, :] = v_next
                if c < STRIPS and REACH // SUB <= tile < (REACH + ROWS) // SUB:
                    own = tile - REACH // SUB
                    bar_u[own, c] += weight * u_next
                    bar_v[own, c] += weight * v_next

    def wall_row():
        for tile in range(EXT_TILES):
            place = row * ROWS + (SUB * tile - REACH) + lax.broadcasted_iota(jnp.int32, (SUB, LANES), 0)
            wet = jnp.logical_and(place >= 0, place < total - 1)
            for c in five:
                at = page(tile, c)
                v_s[at, :] = jnp.where(wet, v_s[at, :], 0.0)
                if c < STRIPS and REACH // SUB <= tile < (REACH + ROWS) // SUB:
                    own = tile - REACH // SUB
                    bar_v[own, c] = jnp.where(wet, bar_v[own, c], 0.0)

    four = range(STRIPS)
    inner, _ = tables(DIFF_R)

    def tracers(tile, _):
        mid = [counts[c, pl.ds(pl.multiple_of(SUB * tile + SUB, SUB), SUB), :] for c in four]
        out_rows = pl.ds(pl.multiple_of(SUB * tile, SUB), SUB)
        xt, xs = [zero] * STRIPS, [zero] * STRIPS
        for k in range(LEV - 1, -1, -1):
            for c in four:
                on = mid[c] > k
                lanes = pl.ds(LANES * c, LANES)

                def solve(w, x, out):
                    value = w[tile, k, c]
                    full = value + (DIFF_R / inner[k]) * x[c]
                    out[k, out_rows, lanes] = jnp.where(on, full, value)
                    x[c] = jnp.where(on, full, 0.0)

                solve(wt, xt, t_new)
                solve(ws, xs, s_new)
        put(tile, 2, t_new, t_out).start()
        put(tile, 3, s_new, s_out).start()
        return 0

    n = 0
    while n < n_sub:
        spread = -(-(n_sub - n) // SUB)
        stop = n_sub - SUB * (spread - 1)
        low, high = REACH // SUB - spread, (REACH + ROWS) // SUB + spread

        def some(i, _, low=low, high=high, first=(n == 0)):
            subcycle(i, low, high)
            if first:
                pl.when(i == 0)(wall_row)
            return 0

        lax.fori_loop(n, stop, some, 0)
        if n == 0:
            lax.fori_loop(0, TILES, tracers, 0)
        n = stop

    pivot, final = tables(VISC_R)
    for tile in range(TILES):
        for c in four:
            at = page(tile + REACH // SUB, c)
            rows, lanes = pl.ds(SUB * tile, SUB), pl.ds(LANES * c, LANES)
            flat_out[0, rows, lanes] = e_s[at, :]
            flat_out[1, rows, lanes] = u_s[at, :] * (1.0 / dt_fast)
            flat_out[2, rows, lanes] = v_s[at, :] * (1.0 / dt_fast)

    results = [pltpu.make_async_copy(flat_out.at[i], dst, small_sem.at[i]) for i, dst in enumerate((eta_out, tu_out, tv_out))]
    for copy in results:
        copy.start()

    def tile_step(tile, _):
        _, nu, nv = face_counts(counts, side_cols.at[0], tile)
        out_rows = pl.ds(pl.multiple_of(SUB * tile, SUB), SUB)
        add_u, add_v = [], []
        for c in four:
            at = pl.ds(c * PAGE + SUB + REACH + SUB * tile, SUB)
            lanes = pl.ds(LANES * c, LANES)
            deep_u = cu_s[at, :] * (1.0 / (dt_fast * GRAVITY))
            deep_v = cv_s[at, :] * (1.0 / (dt_fast * GRAVITY))
            deep_v = jnp.where(nv[c] > 0, deep_v, 1.0)
            add_u.append(bar_u[tile, c] / deep_u - level_mean[0, out_rows, lanes])
            add_v.append(bar_v[tile, c] / deep_v - level_mean[1, out_rows, lanes])
        xu, xv = [zero] * STRIPS, [zero] * STRIPS
        for k in range(LEV - 1, -1, -1):
            ratio, bottom = VISC_R / pivot[k], pivot[k] / final[k]
            for c in four:
                lanes = pl.ds(LANES * c, LANES)

                def solve(w, x, n, add, out):
                    value = w[tile, k, c]
                    last = value * bottom
                    if k < LEV - 1:
                        x[c] = jnp.where(n[c] > k + 1, value + ratio * x[c], last)
                    else:
                        x[c] = last
                    out[k, out_rows, lanes] = jnp.where(n[c] > k, x[c] + add[c], 0.0)

                solve(wu, xu, nu, add_u, u_new)
                solve(wv, xv, nv, add_v, v_new)
        put(tile, 0, u_new, u_out).start()
        put(tile, 1, v_new, v_out).start()
        return 0

    lax.fori_loop(0, TILES, tile_step, 0)
    for tile in range(TILES):
        for i, (src, dst) in enumerate(((u_new, u_out), (v_new, v_out), (t_new, t_out), (s_new, s_out))):
            put(tile, i, src, dst).wait()
    for copy in results:
        copy.wait()


def solution(mesh):
    n_row = mesh.shape['row']
    hbm = pl.BlockSpec(memory_space=pltpu.HBM)
    vmem = pl.BlockSpec(memory_space=pltpu.VMEM)
    smem = pl.BlockSpec(memory_space=pltpu.SMEM)
    dma = pltpu.SemaphoreType.DMA
    strip = pltpu.VMEM((STRIPS, LEV + 1, PITCH, LANES), F32)
    whole = pltpu.VMEM((LEV, ROWS, COLS), F32)
    extended = pltpu.VMEM(((STRIPS + 1) * PAGE, LANES), F32)

    def shape(*dims):
        return jax.ShapeDtypeStruct(dims, F32)

    def call(limit, body, ins, outs, shapes, scratch, **params):
        return pl.pallas_call(body, out_shape=shapes, in_specs=ins, out_specs=outs, scratch_shapes=scratch,
                              compiler_params=pltpu.CompilerParams(vmem_limit_bytes=limit * 1024 * 1024, **params))

    def step(vel_u, vel_v, temp, salt, eta, tu, tv, depth, count, weights):
        n_sub = weights.shape[0]
        part = lax.broadcasted_iota(jnp.int32, (5, ROWS, COLS), 0)
        flat_in = jnp.where(part == 4, count, part).astype(F32)
        for f, field in enumerate((eta, tu, tv, depth)):
            flat_in = jnp.where(part == f, field, flat_in)
        kept = call(
            STEP_MIB, functools.partial(step_kernel, n_row), [hbm] * 4 + [vmem], [vmem] * 14,
            [shape(TILES, LEV, STRIPS, SUB, LANES)] * 4 + [shape(2, ROWS, COLS)] * 2
            + [shape(4, ROWS + 2 * SUB, LANES), shape(STRIPS, ROWS + 2 * SUB, LANES)]
            + [shape(4, REACH, COLS), shape(4, REACH, COLS), shape(4, EXT, LANES)]
            + [shape(2, REACH, COLS), shape(2, REACH, COLS), shape(2, EXT, LANES)],
            [pltpu.VMEM((4, STRIPS, LEV + 1, PITCH, LANES), F32)] + [strip] * 2
            + [pltpu.VMEM((4, LEV, ROWS + 2 * SUB, LANES), F32)] + [pltpu.VMEM((4, ROWS, LANES), F32)] * 2
            + [pltpu.VMEM((2, ROWS, LANES), F32)]
            + [dma((10,)), dma((20,)), dma((20,))],
            collective_id=0, has_side_effects=True)(vel_u, vel_v, temp, salt, flat_in)
        return call(
            FAST_MIB, functools.partial(fast_kernel, n_row, n_sub), [smem] + [vmem] * 15, [hbm] * 7,
            [shape(ROWS, COLS)] * 3 + [shape(LEV, ROWS, COLS)] * 4,
            [pltpu.VMEM((3, ROWS, COLS), F32), dma((3,))]
            + [extended] * 9 + [pltpu.VMEM((EXT, LANES), F32)] * 2 + [pltpu.VMEM((TILES, STRIPS, SUB, LANES), F32)] * 2
            + [whole] * 4 + [dma((4, TILES))],
        )(weights, flat_in, *kept)

    cube = P(None, 'row', 'col')
    flat = P('row', 'col')
    return jax.shard_map(step, mesh=mesh, in_specs=(cube, cube, cube, cube, flat, flat, flat, flat, flat, P()),
                         out_specs=(flat, flat, flat, cube, cube, cube, cube), check_vma=False)
```

```python
import functools

import jax
import jax.numpy as jnp
from jax import lax
from jax.experimental import pallas as pl
from jax.experimental.pallas import tpu as pltpu
from jax.sharding import PartitionSpec as P

TIME_STEP = 1.0
GRAVITY = 16.0
BC_GRAVITY = 4.0
EXPAND_T = 0.2
CONTRACT_S = 0.6
CORIO_F0 = 0.4
CORIO_BETA = 0.4
VISC_R = 2.0
DIFF_R = 0.5

LEV = 41
ROWS = 48
SUB = 8
COLS = 512
LANES = 128
STRIPS = COLS // LANES
TILES = ROWS // SUB
PITCH = 56
REACH = 32
EXT = ROWS + 2 * REACH
EXT_TILES = EXT // SUB
PAGE = EXT + 16
MESH = pl.DeviceIdType.MESH
F32 = jnp.float32
STEP_MIB, FAST_MIB = 35, 36


def tables(strength):
    inner, last, ratio = [], [], 0.0
    for level in range(LEV):
        low = strength if level else 0.0
        pivot = 1.0 + low + strength - low * ratio
        inner.append(pivot)
        last.append(1.0 + low - low * ratio)
        ratio = strength / pivot
    return inner, last


def lane_index():
    return lax.broadcasted_iota(jnp.int32, (SUB, LANES), 1)


def west_of(strips, edge, at_last):
    mixed = [jnp.where(at_last, edge if c == 0 else strips[c - 1], strips[c]) for c in range(len(strips))]
    return [pltpu.roll(x, 1, 1) for x in mixed]


def east_of(strips, edge, at_first):
    n = len(strips)
    mixed = [jnp.where(at_first, edge if c == n - 1 else strips[c + 1], strips[c]) for c in range(n)]
    return [pltpu.roll(x, LANES - 1, 1) for x in mixed]


def places(n_row):
    row = lax.axis_index('row')
    col = lax.axis_index('col')
    other = 1 - col
    has_north = row < n_row - 1
    has_south = row > 0
    return dict(
        row=row, has_north=has_north, has_south=has_south,
        side={'col': other, 'row': row},
        north={'col': col, 'row': row + 1}, south={'col': col, 'row': row - 1},
        north_side={'col': other, 'row': row + 1}, south_side={'col': other, 'row': row - 1})


def meet(at):
    barrier = pltpu.get_barrier_semaphore()
    pl.semaphore_signal(barrier, inc=1, device_id=at['side'], device_id_type=MESH)

    @pl.when(at['has_north'])
    def _():
        pl.semaphore_signal(barrier, inc=1, device_id=at['north'], device_id_type=MESH)
        pl.semaphore_signal(barrier, inc=1, device_id=at['north_side'], device_id_type=MESH)

    @pl.when(at['has_south'])
    def _():
        pl.semaphore_signal(barrier, inc=1, device_id=at['south'], device_id_type=MESH)
        pl.semaphore_signal(barrier, inc=1, device_id=at['south_side'], device_id_type=MESH)

    return barrier


def await_meet(barrier, at):
    pl.semaphore_wait(barrier, 1 + 2 * at['has_north'].astype(jnp.int32) + 2 * at['has_south'].astype(jnp.int32))


def remote(src, dst, send, recv, where):
    return pltpu.make_async_remote_copy(src_ref=src, dst_ref=dst, send_sem=send, recv_sem=recv, device_id=where, device_id_type=MESH)


def level_rows(tile, k, offset=0):
    return pl.ds(SUB * tile + (PITCH * (k + 1) + offset), SUB)


def west_stack(strips, edge, at_last):
    return pltpu.roll(jnp.where(at_last, jnp.concatenate([edge[None], strips[:-1]], axis=0), strips), 1, 2)


def east_stack(strips, edge, at_first):
    return pltpu.roll(jnp.where(at_first, jnp.concatenate([strips[1:], edge[None]], axis=0), strips), LANES - 1, 2)


def face_counts(counts, side, tile):
    rows = SUB * tile + SUB
    mid = counts[:, pl.ds(rows, SUB), :]
    north = counts[:, pl.ds(rows + 1, SUB), :]
    edge = pltpu.roll(side[pl.ds(rows, SUB), :], LANES - 1 - 2 * LEV, 1)
    at_first = lax.broadcasted_iota(jnp.int32, mid.shape, 2) == 0
    return mid, jnp.minimum(mid, east_stack(mid, edge, at_first)), jnp.minimum(mid, north)


def unpack(packed, edges, f, rows):
    for k in range(LEV):
        edges[f, k, rows, :] = pltpu.roll(packed[f, rows, :], LANES - 1 - 2 * k, 1)


def step_kernel(n_row, u, v, t, s, flat_in,
                wu, wv, wt, ws, force, level_mean, side_cols, counts,
                wide_north, wide_south, wide_side, force_north, force_south, force_side,
                cube, one_s, two_s, edges, own_cols, fold, force_fold,
                load_sem, send_sem, recv_sem):
    at = places(n_row)
    fields = (u, v, t, s)
    four = range(STRIPS)

    def load(f, c, sem):
        return pltpu.make_async_copy(fields[f].at[:, :, pl.ds(LANES * c, LANES)], cube.at[f, c, pl.ds(1, LEV), pl.ds(0, ROWS), :], sem)

    outer = [[load(f, c, load_sem.at[2 * f + e]) for e, c in enumerate((0, STRIPS - 1))] for f in four]
    inner_sem = load_sem.at[9]
    for pair in outer:
        for copy in pair:
            copy.start()
    barrier = meet(at)
    lane = lane_index()
    at_first, at_last = lane == 0, lane == LANES - 1
    zero = jnp.zeros((SUB, LANES), F32)
    line = jnp.zeros((1, LANES), F32)
    for c in four:
        counts[c, SUB:SUB + ROWS, :] = flat_in[4, :, c * LANES:(c + 1) * LANES]
    await_meet(barrier, at)
    slot = iter(range(LANES))

    def plan(where, region, *pairs):
        i = next(slot)
        copies = [remote(src, dst, send_sem.at[i], recv_sem.at[i], at[where]) for src, dst in pairs]
        return copies, remote(region, region, send_sem.at[i], recv_sem.at[i], at[where])

    def begin(plans):
        for copies, _ in plans:
            for copy in copies:
                copy.start()

    def start(north, south, side=()):
        pl.when(at['has_north'])(lambda: begin(north))
        pl.when(at['has_south'])(lambda: begin(south))
        begin(side)

    def received(plans):
        for _, waiter in plans:
            waiter.wait_recv()

    def sent(plans):
        for _, waiter in plans:
            waiter.wait_send()

    def arrive(north, south, side=()):
        received(side)
        pl.when(at['has_north'])(lambda: received(south))
        pl.when(at['has_south'])(lambda: received(north))

    def leave(north, south, side=()):
        sent(side)
        pl.when(at['has_north'])(lambda: sent(north))
        pl.when(at['has_south'])(lambda: sent(south))

    def row_region(level, row):
        return cube.at[:, :, pl.ds(level, LEV), pl.ds(row, 1), :]

    def row_pairs(source, level, row):
        return [(fields[f].at[:, pl.ds(source, 1), pl.ds(LANES * c, LANES)], cube.at[f, c, pl.ds(level, LEV), pl.ds(row, 1), :])
                for f in four for c in four]

    rows_north = [plan('north', row_region(0, PITCH - 1), *row_pairs(ROWS - 1, 0, PITCH - 1))]
    rows_south = [plan('south', row_region(1, ROWS), *row_pairs(0, 1, ROWS))]
    low_tile, high_tile = counts.at[:, pl.ds(0, SUB), :], counts.at[:, pl.ds(SUB + ROWS, SUB), :]
    count_north = [plan('north', low_tile, (counts.at[:, pl.ds(ROWS, SUB), :], low_tile))]
    count_south = [plan('south', high_tile, (counts.at[:, pl.ds(SUB, SUB), :], high_tile))]
    start(count_north + rows_north, count_south + rows_south)

    half_lane = lane >> 1
    sides = []
    for f in four:
        for copy in outer[f]:
            copy.wait()
        later = (f + 2) % 4
        for c in range(1, STRIPS - 1):
            load(later, c, load_sem.at[8 + (later < 2)]).start()

        def pack(tile):
            rows = pl.ds(pl.multiple_of(SUB * tile, SUB), SUB)
            packed = zero
            for k in range(LEV + 1 if f == 0 else LEV):
                if k < LEV:
                    first, last = cube[f, 0, k + 1, rows, :], cube[f, STRIPS - 1, k + 1, rows, :]
                else:
                    lower = pl.ds(pl.multiple_of(SUB * tile + SUB, SUB), SUB)
                    first, last = counts[0, lower, :], counts[STRIPS - 1, lower, :]
                both = pltpu.roll(jnp.where(at_first, first, last), 2 * k + 1, 1)
                packed = jnp.where(half_lane == k, both, packed)
            own_cols[f, rows, :] = packed

        def pack_two(pair, _):
            pack(2 * pair)
            pack(2 * pair + 1)
            return 0

        lax.fori_loop(0, TILES // 2, pack_two, 0)
        target = side_cols.at[f, pl.ds(SUB, ROWS), :]
        sides.append(plan('side', target, (own_cols.at[f], target)))
        begin(sides[-1:])
    high_u, low_v = side_cols.at[0, pl.ds(SUB + ROWS, SUB), :], side_cols.at[1, pl.ds(0, SUB), :]
    corner_south = [plan('south_side', high_u, (own_cols.at[0, pl.ds(0, SUB), :], high_u))]
    corner_north = [plan('north_side', low_v, (own_cols.at[1, pl.ds(ROWS - SUB, SUB), :], low_v))]
    start(corner_north, corner_south)

    def clear(level, row):
        def body(k, _):
            for f in four:
                for c in four:
                    cube[f, c, k + level, pl.ds(row, 1), :] = line
            return 0

        lax.fori_loop(0, LEV, body, 0)

    low_rows, high_rows = pl.ds(0, REACH), pl.ds(ROWS - REACH, REACH)
    far_rows = pl.ds(REACH + ROWS, REACH)

    def walled(level, row, tile, wide, forced, rows):
        clear(level, row)
        counts[:, pl.ds(tile, SUB), :] = jnp.zeros((STRIPS, SUB, LANES), F32)
        side_cols[:, pl.ds(tile, SUB), :] = jnp.zeros((STRIPS, SUB, LANES), F32)
        wide[...] = jnp.zeros_like(wide)
        forced[...] = jnp.zeros_like(forced)
        wide_side[:, rows, :] = jnp.zeros((STRIPS, REACH, LANES), F32)
        force_side[:, rows, :] = jnp.zeros((2, REACH, LANES), F32)

    pl.when(jnp.logical_not(at['has_north']))(lambda: walled(1, ROWS, SUB + ROWS, wide_north, force_north, far_rows))
    pl.when(jnp.logical_not(at['has_south']))(lambda: walled(0, PITCH - 1, 0, wide_south, force_south, low_rows))
    half_scale = 0.5 * BC_GRAVITY / LEV
    scale = 0.5 * TIME_STEP

    def density(sal, tem):
        return (half_scale * CONTRACT_S) * sal - (half_scale * EXPAND_T) * tem

    def interior(f, sem):
        region = cube.at[pl.ds(f, 2), pl.ds(1, STRIPS - 2), pl.ds(1, LEV), pl.ds(0, ROWS), :]
        return pltpu.make_async_copy(region, region, sem)

    rows_flat = (LEV + 1) * PITCH
    uf, vf, tf, sf = [cube.at[f].reshape(STRIPS, rows_flat, LANES) for f in four]
    pf, bf = [ref.reshape(STRIPS, rows_flat, LANES) for ref in (one_s, two_s)]
    stack = lax.broadcasted_iota(jnp.int32, (STRIPS, SUB, LANES), 2)
    first_lanes, last_lanes = stack == 0, stack == LANES - 1
    none = jnp.zeros((STRIPS, SUB, LANES), F32)
    interior(2, load_sem.at[8]).wait()

    slope = wt

    def pressure(tile, _):
        acc = none
        for k in range(LEV):
            here = level_rows(tile, k)
            rho = density(sf[:, here, :], tf[:, here, :])
            pp = acc + rho
            acc = pp + rho
            pf[:, here, :] = pp
            slope[tile, k] = pp - east_stack(pp, zero, first_lanes)
        return 0

    lax.fori_loop(0, TILES, pressure, 0)

    for f in four:
        received(sides[f:f + 1])

        def spread(group, _):
            for part in range(3):
                unpack(side_cols, edges, f, pl.ds(pl.multiple_of(SUB * (3 * group + part + 1), SUB), SUB))
            return 0

        lax.fori_loop(0, TILES // 3, spread, 0)
    arrive(count_north + corner_north, count_south + corner_south)
    unpack(side_cols, edges, 0, pl.ds(SUB + ROWS, SUB))
    unpack(side_cols, edges, 1, pl.ds(0, SUB))
    interior(0, inner_sem).wait()
    low_half = lax.broadcasted_iota(jnp.int32, (ROWS, LANES), 1) < LANES // 2
    for f in four:
        fold[f] = jnp.where(low_half, flat_in[f, :, :LANES], flat_in[f, :, COLS - LANES:])
    side_low, side_high = wide_side.at[:, low_rows, :], wide_side.at[:, far_rows, :]
    side_mid = wide_side.at[:, pl.ds(REACH, ROWS), :]
    wide_up = [plan('north', wide_south, (flat_in.at[pl.ds(0, 4), high_rows, :], wide_south)),
               plan('north_side', side_low, (fold.at[:, high_rows, :], side_low))]
    wide_down = [plan('south', wide_north, (flat_in.at[pl.ds(0, 4), low_rows, :], wide_north)),
                 plan('south_side', side_high, (fold.at[:, low_rows, :], side_high))]
    wide_across = [plan('side', side_mid, (fold, side_mid))]
    start(wide_up, wide_down, wide_across)
    pivot, _ = tables(VISC_R)
    for k in range(LEV):
        spot = level_rows(TILES - 1, k)
        uu = uf[:, spot, :]
        bf[:, spot, :] = uu + west_stack(uu, edges[0, k, pl.ds(ROWS, SUB), :], last_lanes)

    def border_rows():
        arrive(rows_north, rows_south)
        acc = none
        for k in range(LEV):
            spot = level_rows(TILES, k)
            uu = uf[:, spot, :]
            bf[:, spot, :] = uu + west_stack(uu, edges[0, k, pl.ds(SUB + ROWS, SUB), :], last_lanes)
            rho = density(sf[:, spot, :], tf[:, spot, :])
            pf[:, spot, :] = acc + rho
            acc = (acc + rho) + rho

    def momentum(step, _):
        tile = (2 * TILES - 2 - step) % TILES
        pl.when(step == TILES - 2)(border_rows)
        _, nu, nv = face_counts(counts, side_cols.at[0], tile)
        row_pos = (at['row'] * ROWS + SUB * tile + lax.broadcasted_iota(jnp.int32, (STRIPS, SUB, LANES), 1)).astype(F32)
        fu = 0.25 * (CORIO_F0 + CORIO_BETA * ((row_pos + 0.5) / (ROWS * n_row) - 0.5))
        fv = 0.25 * (CORIO_F0 + CORIO_BETA * ((row_pos + 1.0) / (ROWS * n_row) - 0.5))
        out_rows = pl.ds(pl.multiple_of(SUB * tile, SUB), SUB)
        mid_rows = pl.ds(pl.multiple_of(SUB * tile + SUB, SUB), SUB)
        acc_e = zero
        xu, xv, sum_du, sum_dv, sum_su, sum_sv = (none,) * 6
        for k in range(LEV):
            here, up, below = [level_rows(tile, k, step) for step in (0, 1, -1)]
            uu, vv = uf[:, here, :], vf[:, here, :]
            v_south = vf[:, below, :]
            edge_u, edge_v = edges[0, k, mid_rows, :], edges[1, k, mid_rows, :]
            u_west = west_stack(uu, edge_u, last_lanes)
            u_east = east_stack(uu, edge_u, first_lanes)
            v_west = west_stack(vv, edge_v, last_lanes)
            v_east = east_stack(vv, edge_v, first_lanes)
            pair_v = vv + v_south
            pair_ve = east_stack(pair_v, edge_v + edges[1, k, pl.ds(SUB * tile + SUB - 1, SUB), :], first_lanes)
            rho_e = pltpu.roll(density(edges[3, k, mid_rows, :], edges[2, k, mid_rows, :]), LANES - 1, 1)
            p_edge = acc_e + rho_e
            acc_e = p_edge + rho_e
            pp = pf[:, here, :]
            fall = slope[tile, k]
            fall = jnp.concatenate([fall[:-1], jnp.where(at_last, pp[-1] - p_edge, fall[-1])[None]], axis=0)
            pair_u = uu + u_west
            bf[:, here, :] = pair_u
            v4 = pair_v + pair_ve
            u4 = pair_u + bf[:, up, :]
            du = v4 * (fu - 0.125 * (uf[:, up, :] - uf[:, below, :])) - 0.5 * uu * (u_east - u_west) + fall
            dv = (pp - pf[:, up, :]) - u4 * (fv + 0.125 * (v_east - v_west)) - 0.5 * vv * (vf[:, up, :] - v_south)
            us, vs = uu + du, vv + dv
            on_u, on_v = nu > k, nv > k
            sum_du += jnp.where(on_u, du, 0.0)
            sum_dv += jnp.where(on_v, dv, 0.0)
            sum_su += jnp.where(on_u, us, 0.0)
            sum_sv += jnp.where(on_v, vs, 0.0)
            xu = us * (1.0 / pivot[k]) + xu * (VISC_R / pivot[k])
            xv = vs * (1.0 / pivot[k]) + xv * (VISC_R / pivot[k])
            wu[tile, k] = xu
            wv[tile, k] = xv
        inv_u = 1.0 / jnp.maximum(nu, 1.0)
        inv_v = 1.0 / jnp.maximum(nv, 1.0)
        for c in four:
            lanes = pl.ds(LANES * c, LANES)
            force[0, out_rows, lanes] = (sum_du * inv_u)[c]
            force[1, out_rows, lanes] = (sum_dv * inv_v)[c]
            level_mean[0, out_rows, lanes] = (sum_su * inv_u)[c]
            level_mean[1, out_rows, lanes] = (sum_sv * inv_v)[c]
        return 0

    lax.fori_loop(0, TILES, momentum, 0)

    for f in range(2):
        force_fold[f] = jnp.where(low_half, force[f, :, :LANES], force[f, :, COLS - LANES:])
    side_low, side_high = force_side.at[:, low_rows, :], force_side.at[:, far_rows, :]
    side_mid = force_side.at[:, pl.ds(REACH, ROWS), :]
    force_up = [plan('north', force_south, (force.at[:, high_rows, :], force_south)),
                plan('north_side', side_low, (force_fold.at[:, high_rows, :], side_low))]
    force_down = [plan('south', force_north, (force.at[:, low_rows, :], force_north)),
                  plan('south_side', side_high, (force_fold.at[:, low_rows, :], side_high))]
    force_across = [plan('side', side_mid, (force_fold, side_mid))]
    start(force_up, force_down, force_across)
    ftf, fsf = pf, bf
    pivot, final = tables(DIFF_R)

    south_count = jnp.minimum(counts[:, pl.ds(0, SUB), :], counts[:, pl.ds(1, SUB), :])
    for k in range(LEV):
        here, up = level_rows(-1, k), level_rows(-1, k, 1)
        hv = jnp.where(south_count > k, scale * vf[:, here, :], 0.0)
        ftf[:, here, :] = hv * (tf[:, here, :] + tf[:, up, :])
        fsf[:, here, :] = hv * (sf[:, here, :] + sf[:, up, :])

    def tracers(tile, _):
        mid, nu, nv = face_counts(counts, side_cols.at[0], tile)
        out_rows = pl.ds(pl.multiple_of(SUB * tile, SUB), SUB)
        mid_rows = pl.ds(pl.multiple_of(SUB * tile + SUB, SUB), SUB)
        west_count = jnp.minimum(pltpu.roll(side_cols[0, mid_rows, :], LANES - 1 - 2 * LEV, 1), pltpu.roll(counts[0, mid_rows, :], LANES - 1, 1))
        xt, xs = none, none
        for k in range(LEV):
            here, up, below = [level_rows(tile, k, step) for step in (0, 1, -1)]
            hu = jnp.where(nu > k, scale * uf[:, here, :], 0.0)
            hv = jnp.where(nv > k, scale * vf[:, here, :], 0.0)
            hw = west_stack(hu, jnp.where(west_count > k, scale * edges[0, k, mid_rows, :], 0.0), last_lanes)
            inverse = jnp.where(mid > k + 1, 1.0 / pivot[k], 1.0 / final[k]) if k < LEV - 1 else 1.0 / final[k]

            def advance(flat, flux, which, x, w):
                q = flat[:, here, :]
                edge = edges[which, k, mid_rows, :]
                flux_e = hu * (q + east_stack(q, edge, first_lanes))
                flux_w = hw * (q + west_stack(q, edge, last_lanes))
                flux_n = hv * (q + flat[:, up, :])
                flux[:, here, :] = flux_n
                new = q - ((flux_e - flux_w) + (flux_n - flux[:, below, :]))
                x = (new + DIFF_R * x) * inverse
                w[tile, k] = jnp.where(mid > k, x, new)
                return x

            xt = advance(tf, ftf, 2, xt, wt)
            xs = advance(sf, fsf, 3, xs, ws)
        return 0

    lax.fori_loop(0, TILES, tracers, 0)
    leave(count_north + corner_north + rows_north, count_south + corner_south + rows_south, sides)
    for group in ((wide_up, wide_down, wide_across), (force_up, force_down, force_across)):
        arrive(*group)
        leave(*group)


def fast_kernel(n_row, n_sub, weights, flat_in, wu, wv, wt, ws, force, level_mean, side_cols, counts,
                wide_north, wide_south, wide_side, force_north, force_south, force_side,
                eta_out, tu_out, tv_out, u_out, v_out, t_out, s_out,
                flat_out, small_sem, e_s, u_s, v_s, b_s, d_s, cu_s, cv_s, bu_s, bv_s, fu_s, fv_s, bar_u, bar_v,
                u_new, v_new, t_new, s_new, store_sem):
    row = lax.axis_index('row')
    def put(tile, i, src, dst):
        rows = pl.ds(pl.multiple_of(SUB * tile, SUB), SUB)
        return pltpu.make_async_copy(src.at[:, rows, :], dst.at[:, rows, :], store_sem.at[i, tile])

    lane = lane_index()
    at_first, at_last = lane == 0, lane == LANES - 1
    five = range(STRIPS + 1)
    dt_fast = TIME_STEP / n_sub
    total = ROWS * n_row
    zero = jnp.zeros((SUB, LANES), F32)

    def page(tile, c, offset=0):
        return pl.ds(c * PAGE + SUB + SUB * tile + offset, SUB)

    def gather(f, own, north, south, side, tile, c):
        if c == STRIPS:
            return side[f, SUB * tile:SUB * tile + SUB, :]
        lanes = slice(c * LANES, (c + 1) * LANES)
        if tile < REACH // SUB:
            return south[f, SUB * tile:SUB * tile + SUB, lanes]
        if tile < (REACH + ROWS) // SUB:
            return own[SUB * tile - REACH:SUB * tile - REACH + SUB, lanes]
        start = SUB * tile - REACH - ROWS
        return north[f, start:start + SUB, lanes]

    for ref in (e_s, u_s, v_s, b_s, d_s):
        for c in five:
            ref[page(-1, c), :] = zero
            ref[page(EXT_TILES, c), :] = zero
    for tile in range(EXT_TILES):
        for c in five:
            at = page(tile, c)
            e_s[at, :] = gather(0, flat_in.at[0], wide_north, wide_south, wide_side, tile, c)
            u_s[at, :] = dt_fast * gather(1, flat_in.at[1], wide_north, wide_south, wide_side, tile, c)
            v_s[at, :] = dt_fast * gather(2, flat_in.at[2], wide_north, wide_south, wide_side, tile, c)
            d_s[at, :] = gather(3, flat_in.at[3], wide_north, wide_south, wide_side, tile, c)
            bu_s[at, :] = gather(0, force.at[0], force_north, force_south, force_side, tile, c)
            bv_s[at, :] = gather(1, force.at[1], force_north, force_south, force_side, tile, c)
    for tile in range(EXT_TILES):
        place = row * ROWS + (SUB * tile - REACH) + lax.broadcasted_iota(jnp.int32, (SUB, LANES), 0)
        inside = jnp.logical_and(place >= 0, place < total)
        inside_v = jnp.logical_and(place >= 0, place < total - 1)
        row_pos = place.astype(F32)
        fu = (0.25 * dt_fast) * (CORIO_F0 + CORIO_BETA * ((row_pos + 0.5) / total - 0.5))
        fv = (0.25 * dt_fast) * (CORIO_F0 + CORIO_BETA * ((row_pos + 1.0) / total - 0.5))
        fu_s[SUB * tile:SUB * tile + SUB, :] = jnp.where(inside, fu, 0.0)
        fv_s[SUB * tile:SUB * tile + SUB, :] = jnp.where(inside_v, fv, 0.0)
        deep = [d_s[page(tile, c), :] for c in five]
        deep_e = east_of(deep, deep[0], at_first)
        for c in five:
            at = page(tile, c)
            hu = jnp.where(inside, 0.5 * (deep[c] + deep_e[c]), 0.0)
            hv = jnp.where(inside_v, 0.5 * (deep[c] + d_s[page(tile, c, 1), :]), 0.0)
            cu_s[at, :] = (dt_fast * dt_fast * GRAVITY) * hu
            cv_s[at, :] = (dt_fast * dt_fast * GRAVITY) * hv
            bu_s[at, :] = (dt_fast * dt_fast / TIME_STEP) * hu * bu_s[at, :]
            bv_s[at, :] = (dt_fast * dt_fast / TIME_STEP) * hv * bv_s[at, :]
    bar_u[...] = jnp.zeros_like(bar_u)
    bar_v[...] = jnp.zeros_like(bar_v)

    def subcycle(n, low, high):
        weight = weights[n]
        for tile in range(high - 1, low - 1, -1):
            uu = [u_s[page(tile, c), :] for c in five]
            vv = [v_s[page(tile, c), :] for c in five]
            v_south = [v_s[page(tile, c, -1), :] for c in five]
            part = [e_s[page(tile, c), :] - (uu[c] + (vv[c] - v_south[c])) for c in five]
            pair_v = [vv[c] + v_south[c] for c in five]
            u_west = west_of(uu, uu[-1], at_last)
            part_e = east_of(part, part[0], at_first)
            pair_ve = east_of(pair_v, pair_v[0], at_first)
            fu = fu_s[SUB * tile:SUB * tile + SUB, :]
            fv = fv_s[SUB * tile:SUB * tile + SUB, :]
            for c in five:
                at, up = page(tile, c), page(tile, c, 1)
                new = part[c] + u_west[c]
                pair_u = uu[c] + u_west[c]
                e_s[at, :] = new
                b_s[at, :] = pair_u
                u_next = uu[c] + ((fu * (pair_v[c] + pair_ve[c]) + bu_s[at, :]) - cu_s[at, :] * ((part_e[c] + uu[c]) - new))
                v_next = vv[c] + ((bv_s[at, :] - fv * (pair_u + b_s[up, :])) - cv_s[at, :] * (e_s[up, :] - new))
                u_s[at, :] = u_next
                v_s[at, :] = v_next
                if c < STRIPS and REACH // SUB <= tile < (REACH + ROWS) // SUB:
                    own = tile - REACH // SUB
                    bar_u[own, c] += weight * u_next
                    bar_v[own, c] += weight * v_next

    def wall_row():
        for tile in range(EXT_TILES):
            place = row * ROWS + (SUB * tile - REACH) + lax.broadcasted_iota(jnp.int32, (SUB, LANES), 0)
            wet = jnp.logical_and(place >= 0, place < total - 1)
            for c in five:
                at = page(tile, c)
                v_s[at, :] = jnp.where(wet, v_s[at, :], 0.0)
                if c < STRIPS and REACH // SUB <= tile < (REACH + ROWS) // SUB:
                    own = tile - REACH // SUB
                    bar_v[own, c] = jnp.where(wet, bar_v[own, c], 0.0)

    four = range(STRIPS)
    inner, _ = tables(DIFF_R)

    def tracers(tile, _):
        mid = [counts[c, pl.ds(pl.multiple_of(SUB * tile + SUB, SUB), SUB), :] for c in four]
        out_rows = pl.ds(pl.multiple_of(SUB * tile, SUB), SUB)
        xt, xs = [zero] * STRIPS, [zero] * STRIPS
        for k in range(LEV - 1, -1, -1):
            for c in four:
                on = mid[c] > k
                lanes = pl.ds(LANES * c, LANES)

                def solve(w, x, out):
                    value = w[tile, k, c]
                    full = value + (DIFF_R / inner[k]) * x[c]
                    out[k, out_rows, lanes] = jnp.where(on, full, value)
                    x[c] = jnp.where(on, full, 0.0)

                solve(wt, xt, t_new)
                solve(ws, xs, s_new)
        put(tile, 2, t_new, t_out).start()
        put(tile, 3, s_new, s_out).start()
        return 0

    n = 0
    while n < n_sub:
        spread = -(-(n_sub - n) // SUB)
        stop = n_sub - SUB * (spread - 1)
        low, high = REACH // SUB - spread, (REACH + ROWS) // SUB + spread

        def some(i, _, low=low, high=high, first=(n == 0)):
            subcycle(i, low, high)
            if first:
                pl.when(i == 0)(wall_row)
            return 0

        lax.fori_loop(n, stop, some, 0)
        if n == 0:
            lax.fori_loop(0, TILES, tracers, 0)
        n = stop

    pivot, final = tables(VISC_R)
    for tile in range(TILES):
        for c in four:
            at = page(tile + REACH // SUB, c)
            rows, lanes = pl.ds(SUB * tile, SUB), pl.ds(LANES * c, LANES)
            flat_out[0, rows, lanes] = e_s[at, :]
            flat_out[1, rows, lanes] = u_s[at, :] * (1.0 / dt_fast)
            flat_out[2, rows, lanes] = v_s[at, :] * (1.0 / dt_fast)

    results = [pltpu.make_async_copy(flat_out.at[i], dst, small_sem.at[i]) for i, dst in enumerate((eta_out, tu_out, tv_out))]
    for copy in results:
        copy.start()

    def tile_step(tile, _):
        _, nu, nv = face_counts(counts, side_cols.at[0], tile)
        out_rows = pl.ds(pl.multiple_of(SUB * tile, SUB), SUB)
        add_u, add_v = [], []
        for c in four:
            at = pl.ds(c * PAGE + SUB + REACH + SUB * tile, SUB)
            lanes = pl.ds(LANES * c, LANES)
            deep_u = cu_s[at, :] * (1.0 / (dt_fast * GRAVITY))
            deep_v = cv_s[at, :] * (1.0 / (dt_fast * GRAVITY))
            deep_v = jnp.where(nv[c] > 0, deep_v, 1.0)
            add_u.append(bar_u[tile, c] / deep_u - level_mean[0, out_rows, lanes])
            add_v.append(bar_v[tile, c] / deep_v - level_mean[1, out_rows, lanes])
        xu, xv = [zero] * STRIPS, [zero] * STRIPS
        for k in range(LEV - 1, -1, -1):
            ratio, bottom = VISC_R / pivot[k], pivot[k] / final[k]
            for c in four:
                lanes = pl.ds(LANES * c, LANES)

                def solve(w, x, n, add, out):
                    value = w[tile, k, c]
                    last = value * bottom
                    if k < LEV - 1:
                        x[c] = jnp.where(n[c] > k + 1, value + ratio * x[c], last)
                    else:
                        x[c] = last
                    out[k, out_rows, lanes] = jnp.where(n[c] > k, x[c] + add[c], 0.0)

                solve(wu, xu, nu, add_u, u_new)
                solve(wv, xv, nv, add_v, v_new)
        put(tile, 0, u_new, u_out).start()
        put(tile, 1, v_new, v_out).start()
        return 0

    lax.fori_loop(0, TILES, tile_step, 0)
    for tile in range(TILES):
        for i, (src, dst) in enumerate(((u_new, u_out), (v_new, v_out), (t_new, t_out), (s_new, s_out))):
            put(tile, i, src, dst).wait()
    for copy in results:
        copy.wait()


def solution(mesh):
    n_row = mesh.shape['row']
    hbm = pl.BlockSpec(memory_space=pltpu.HBM)
    vmem = pl.BlockSpec(memory_space=pltpu.VMEM)
    smem = pl.BlockSpec(memory_space=pltpu.SMEM)
    dma = pltpu.SemaphoreType.DMA
    strip = pltpu.VMEM((STRIPS, LEV + 1, PITCH, LANES), F32)
    whole = pltpu.VMEM((LEV, ROWS, COLS), F32)
    extended = pltpu.VMEM(((STRIPS + 1) * PAGE, LANES), F32)

    def shape(*dims):
        return jax.ShapeDtypeStruct(dims, F32)

    def call(limit, body, ins, outs, shapes, scratch, **params):
        return pl.pallas_call(body, out_shape=shapes, in_specs=ins, out_specs=outs, scratch_shapes=scratch,
                              compiler_params=pltpu.CompilerParams(vmem_limit_bytes=limit * 1024 * 1024, **params))

    def step(vel_u, vel_v, temp, salt, eta, tu, tv, depth, count, weights):
        n_sub = weights.shape[0]
        part = lax.broadcasted_iota(jnp.int32, (5, ROWS, COLS), 0)
        flat_in = jnp.where(part == 4, count, part).astype(F32)
        for f, field in enumerate((eta, tu, tv, depth)):
            flat_in = jnp.where(part == f, field, flat_in)
        kept = call(
            STEP_MIB, functools.partial(step_kernel, n_row), [hbm] * 4 + [vmem], [vmem] * 14,
            [shape(TILES, LEV, STRIPS, SUB, LANES)] * 4 + [shape(2, ROWS, COLS)] * 2
            + [shape(4, ROWS + 2 * SUB, LANES), shape(STRIPS, ROWS + 2 * SUB, LANES)]
            + [shape(4, REACH, COLS), shape(4, REACH, COLS), shape(4, EXT, LANES)]
            + [shape(2, REACH, COLS), shape(2, REACH, COLS), shape(2, EXT, LANES)],
            [pltpu.VMEM((4, STRIPS, LEV + 1, PITCH, LANES), F32)] + [strip] * 2
            + [pltpu.VMEM((4, LEV, ROWS + 2 * SUB, LANES), F32)] + [pltpu.VMEM((4, ROWS, LANES), F32)] * 2
            + [pltpu.VMEM((2, ROWS, LANES), F32)]
            + [dma((10,)), dma((20,)), dma((20,))],
            collective_id=0, has_side_effects=True)(vel_u, vel_v, temp, salt, flat_in)
        return call(
            FAST_MIB, functools.partial(fast_kernel, n_row, n_sub), [smem] + [vmem] * 15, [hbm] * 7,
            [shape(ROWS, COLS)] * 3 + [shape(LEV, ROWS, COLS)] * 4,
            [pltpu.VMEM((3, ROWS, COLS), F32), dma((3,))]
            + [extended] * 9 + [pltpu.VMEM((EXT, LANES), F32)] * 2 + [pltpu.VMEM((TILES, STRIPS, SUB, LANES), F32)] * 2
            + [whole] * 4 + [dma((4, TILES))],
        )(weights, flat_in, *kept)

    cube = P(None, 'row', 'col')
    flat = P('row', 'col')
    return jax.shard_map(step, mesh=mesh, in_specs=(cube, cube, cube, cube, flat, flat, flat, flat, flat, P()),
                         out_specs=(flat, flat, flat, cube, cube, cube, cube), check_vma=False)
```
